512 devices in a mesh: space: 64 (over z, x), level: 8 (over y, core).
Axes of the slice: x: 4, y: 4, z: 16, core: 2. Of those that a mesh axis runs over, the one named last changes fastest.
Arguments:
- velocity: float32 [2, 64, 65536], P(None, 'level', 'space'), may hold values from -3 to 3
- density: float32 [64, 65536], P('level', 'space'), may hold values from -6 to 6
- elevation: float32 [65536], P('space'), may hold values from -3 to 3
- grad_weights: float32 [2, 6, 65536], P(None, None, 'space'), may hold values from -2.4 to 2.4
- lap_weights: float32 [6, 65536], P(None, 'space'), may hold values from 0.02 to 0.2
- coriolis: float32 [65536], P('space'), may hold values from 0.5 to 2
- node_area: float32 [65536], P('space'), may hold values from 1 to 100, as said below
- thickness: float32 [64], P('level'), may hold values from 0.5 to 2
- send_list: int32 [64, 256], P('space'), may hold values from 0 to 1023
- neighbours: int32 [6, 65536], P(None, 'space'), may hold values from 0 to 1279
- bottom: int32 [65536], P('space'), may hold values from 0 to 64, as said below
Outputs:
- velocity_out: float32 [2, 64, 65536], P(None, 'level', 'space')
- density_out: float32 [64, 65536], P('level', 'space')
- elevation_out: float32 [65536], P('space')
- volume_drift: float32 [4], replicated
The draws below stay inside these ranges and needn't reach their ends.
Inputs may be any that keep to these rules, and one draw needn't show every extreme that they name: `send_list`: local node numbers within the sending partition; the first 128 go to the partition one below along space, the other 128 to the one above. `neighbours`: slots below 1024 are the partition's own nodes; the next 128 are halo slots filled from the partition below, the last 128 from the partition above. Levels of a node are wet from the surface down to bottom - 1; a node with 0 is dry. Some partitions are shallower than others. `node_area`: positive areas.
All inputs are finite; a program needn't handle non-finite values.
Results may differ from the reference program's by a relative error of at most 0.00013.
Values sent between devices are 32-bit elements; how exact they have to be, the bound alone decides.
A program may use at most 64 MiB of HBM per device.

```python
import math
import jax
import jax.numpy as jnp
from jax import lax

NODES_DEV = 1024
HALO = 128
K = 6
STEPS = 4
NODES = 65536
LEVELS = 64
N_SPACE = 64


def draw_bottom(key, part):
    key_part = jax.random.fold_in(key, 11)
    key_node = jax.random.fold_in(key, 12)
    partitions = NODES // NODES_DEV
    shallow = jax.random.randint(key_part, (partitions, 1), LEVELS // 4, LEVELS + 1)
    shallow = shallow.at[0].set(LEVELS)
    depths = jax.random.randint(key_node, (partitions, NODES_DEV), 0, LEVELS + 1)
    return jnp.minimum(depths, shallow).reshape(NODES).astype(jnp.int32)


def draw_node_area(key, part):
    key_rough = jax.random.fold_in(key, 21)
    partitions = NODES // NODES_DEV
    owner = (jnp.arange(NODES, dtype=jnp.int32) // NODES_DEV).astype(jnp.float32)
    position = owner / jnp.float32(max(partitions - 1, 1))
    ramp = jnp.exp(jnp.log(jnp.float32(10.0)) * position)
    rough = jnp.exp(jax.random.uniform(key_rough, (NODES,), jnp.float32, 0.0, jnp.log(3.0)))
    return (ramp * rough).astype(jnp.float32)


def plant(values, rng, smallest, high):
    spot = [jax.random.randint(jax.random.fold_in(rng, axis), (), 0, length) for axis, length in enumerate(values.shape)]
    longest = values.shape.index(max(values.shape))
    neighbour = spot[:longest] + [(spot[longest] + 1) % values.shape[longest]] + spot[longest + 1:]
    return values.at[tuple(spot)].set(smallest).at[tuple(neighbour)].set(high)


def block_levels(rng, extent, pieces, smallest, top_value):
    loudness, own = 1.0, jax.random.fold_in(rng, 6)
    for dim, blocks in pieces:
        heights = jnp.exp(jax.random.uniform(jax.random.fold_in(own, dim), (blocks,), jnp.float32, smallest / len(pieces), top_value / len(pieces)))
        loudness = loudness * jnp.repeat(heights, extent[dim] // blocks).reshape([-1 if axis == dim else 1 for axis in range(len(extent))])
    return loudness


def scatter_about(rng, shape, width, most, shards=(), held_as=jnp.bfloat16):
    loudness = block_levels(rng, shape, shards, -0.22, 0.18) if shards else 1.0
    values = jax.random.normal(rng, shape, jnp.float32) * width * loudness
    return jnp.minimum(jnp.maximum(values, -most), most).astype(held_as)


def setup_inputs(seed: int = 0) -> dict:
    key_list = jax.random.split(jax.random.key(seed), 12)
    return {
        "velocity": scatter_about(key_list[0], (2, LEVELS, NODES), 0.5, 3.0, ((1, 8), (2, 64)), jnp.float32),
        "density": scatter_about(key_list[1], (LEVELS, NODES), 1.0, 6.0, ((0, 8), (1, 64)), jnp.float32),
        "elevation": scatter_about(key_list[2], (NODES,), 0.5, 3.0, ((0, 64),), jnp.float32),
        "grad_weights": scatter_about(key_list[3], (2, K, NODES), 0.4, 2.4, ((2, 64),), jnp.float32),
        "lap_weights": jnp.clip(jnp.exp(math.log(0.2) - 2.3025851 * jax.random.uniform(key_list[4], (K, NODES), jnp.float32) ** block_levels(key_list[4], (K, NODES), ((1, 64),), -0.2, 0.2)), 0.02, 0.2),
        "coriolis": jnp.clip(jnp.exp(math.log(2.0) - 1.3862944 * jax.random.uniform(key_list[5], (NODES,), jnp.float32) ** block_levels(key_list[5], (NODES,), ((0, 64),), -0.2, 0.2)), 0.5, 2.0),
        "node_area": draw_node_area(jax.random.fold_in(key_list[11], 71), 0),
        "thickness": jnp.clip(jnp.exp(math.log(2.0) - 1.3862944 * jax.random.uniform(key_list[7], (LEVELS,), jnp.float32) ** block_levels(key_list[7], (LEVELS,), ((0, 8),), -0.2, 0.2)), 0.5, 2.0),
        "send_list": plant(jax.random.randint(key_list[8], (N_SPACE, 2 * HALO), 0, NODES_DEV), jax.random.fold_in(key_list[8], 1), 0, NODES_DEV - 1).astype(jnp.int32),
        "neighbours": plant(jax.random.randint(key_list[9], (K, NODES), 0, NODES_DEV + 2 * HALO), jax.random.fold_in(key_list[9], 1), 0, (NODES_DEV + 2 * HALO) - 1).astype(jnp.int32),
        "bottom": draw_bottom(jax.random.fold_in(key_list[11], 71), 0),
    }


time_step = 0.1
buoyancy = 0.5
drag_rate = 0.5


def neighbour_table(send_list, neighbours):
    node_ids = jnp.arange(NODES, dtype=jnp.int32)
    owner = (node_ids // NODES_DEV)[None, :]
    slot_index = neighbours
    source_below = jnp.clip(owner - 1, 0, N_SPACE - 1)
    source_above = jnp.clip(owner + 1, 0, N_SPACE - 1)
    local_below = send_list[source_below, jnp.clip(HALO + slot_index - NODES_DEV, 0, 2 * HALO - 1)]
    local_above = send_list[source_above, jnp.clip(slot_index - NODES_DEV - HALO, 0, 2 * HALO - 1)]
    global_index = jnp.where(slot_index < NODES_DEV, owner * NODES_DEV + slot_index,
                             jnp.where(slot_index < NODES_DEV + HALO, source_below * NODES_DEV + local_below,
                                       source_above * NODES_DEV + local_above))
    is_valid = jnp.where(slot_index < NODES_DEV, True,
                         jnp.where(slot_index < NODES_DEV + HALO, owner >= 1, owner <= N_SPACE - 2))
    return global_index.astype(jnp.int32), is_valid.astype(jnp.float32)


def stencil(fields, global_index, weight):
    result = jnp.zeros_like(fields)
    for column in range(K):
        nearby = jnp.take(fields, global_index[column], axis=-1)
        result = result + weight[column] * (nearby - fields)
    return result


def reference(velocity, density, elevation, grad_weights, lap_weights, coriolis, node_area, thickness, send_list, neighbours, bottom):
    global_index, valid_float = neighbour_table(send_list, neighbours)
    east_weight = grad_weights[0] * valid_float
    north_weight = grad_weights[1] * valid_float
    smooth_weight = lap_weights * valid_float
    level_ids = jnp.arange(LEVELS, dtype=jnp.int32)[:, None]
    wet_cells = (level_ids < bottom[None, :]).astype(jnp.float32)
    at_floor = (level_ids == bottom[None, :] - 1).astype(jnp.float32)
    wet_nodes = (bottom > 0).astype(jnp.float32)
    area_total = jnp.sum(node_area * wet_nodes)
    velocity = velocity * wet_cells[None]
    drifts = []
    for counter in range(STEPS):
        east_speed = velocity[0]
        north_speed = velocity[1]
        weighted = density * thickness[:, None]
        pressure = buoyancy * (jnp.cumsum(weighted, axis=0) - 0.5 * weighted)
        transport = jnp.einsum('cln,l->cn', velocity, thickness, precision=lax.Precision.HIGHEST)
        diverge = stencil(transport[0], global_index, east_weight) + stencil(transport[1], global_index, north_weight)
        drift = jnp.sum(node_area * wet_nodes * diverge) / area_total
        drifts.append(drift)
        new_elevation = elevation - time_step * wet_nodes * diverge + time_step * drift
        slope_east = stencil(elevation, global_index, east_weight)
        slope_north = stencil(elevation, global_index, north_weight)
        press_east = stencil(pressure, global_index, east_weight)
        press_north = stencil(pressure, global_index, north_weight)
        smooth_speed = stencil(velocity.reshape(2 * LEVELS, NODES), global_index, smooth_weight)
        push_east = (-slope_east[None] - press_east + coriolis[None] * north_speed
                     + smooth_speed[:LEVELS] - drag_rate * at_floor * east_speed)
        push_north = (-slope_north[None] - press_north - coriolis[None] * east_speed
                      + smooth_speed[LEVELS:] - drag_rate * at_floor * north_speed)
        dense_east = stencil(density, global_index, east_weight)
        dense_north = stencil(density, global_index, north_weight)
        dense_smooth = stencil(density, global_index, smooth_weight)
        density = density + time_step * (dense_smooth - east_speed * dense_east - north_speed * dense_north)
        velocity = wet_cells[None] * (velocity + time_step * jnp.stack([push_east, push_north]))
        elevation = new_elevation
    return velocity, density, elevation, jnp.stack(drifts).astype(jnp.float32)
```

```python
import jax
import jax.numpy as jnp
from jax import lax
from jax.experimental import pallas as pl
from jax.experimental.pallas import tpu as pltpu
from jax.sharding import PartitionSpec as P

MESH = pl.DeviceIdType.MESH
STEPS = 4
K = 6
TILES = 8
LANES = 128
X_CHIPS = 4
DT = 0.1
BUOYANCY = 0.5
DRAG = 0.5

_LANE_GATHER = lax.GatherDimensionNumbers(
    offset_dims=(),
    collapsed_slice_dims=(1,),
    start_index_map=(1,),
    operand_batching_dims=(0,),
    start_indices_batching_dims=(0,),
)


def lane_gather(x, idx):
    return lax.gather(
        x, idx[..., None], _LANE_GATHER, (1, 1), mode=lax.GatherScatterMode.PROMISE_IN_BOUNDS
    )


def wide(row):
    return jnp.broadcast_to(row, (8, LANES))


def kernel(
    n_space,
    n_level,
    vel_ref,
    rho_ref,
    eta_ref,
    grad_ref,
    lap_ref,
    cor_ref,
    area_ref,
    thick_ref,
    send_ref,
    nb_ref,
    bot_ref,
    vel_out,
    rho_out,
    eta_out,
    drift_out,
    nbc,
    wts,
    x,
    ploc,
    part,
    near,
    q,
    dq,
    eta,
    etah,
    vv,
    lsend,
    lrecv,
    usend,
    urecv,
    rsend,
    rrecv,
    gsend,
    grecv,
    ssend,
    srecv,
    zsend,
    zrecv,
    xsend,
    xrecv,
    lsem,
    usem,
    rsem,
    gsem,
    ssem,
    zsem,
    tok,
):
    p = lax.axis_index("space")
    g = lax.axis_index("level")
    n_z = n_space // X_CHIPS
    up = lax.rem(p + 1, n_space)
    down = lax.rem(p + n_space - 1, n_space)
    level_peers = [lax.rem(g + d, n_level) for d in range(n_level)]

    def z_peer(d):
        return lax.rem(p + d * X_CHIPS, n_space)

    px = lax.rem(p, X_CHIPS)

    def x_peer(d):
        return p - px + lax.rem(px + d, X_CHIPS)

    barrier = pltpu.get_barrier_semaphore()
    count = 0

    def greet(a, b):
        pl.semaphore_signal(barrier, inc=1, device_id=(a, b), device_id_type=MESH)

    for d in range(n_level):
        greet(up, level_peers[d])
        greet(down, level_peers[d])
        count += 2
        if d:
            greet(p, level_peers[d])
            count += 1
    for d in (1, n_z - 1):
        greet(z_peer(d), g)
        count += 1
    for d in range(1, X_CHIPS):
        greet(x_peer(d), g)
        count += 1

    sub = lax.broadcasted_iota(jnp.int32, (8, LANES), 0)
    lane = lax.broadcasted_iota(jnp.int32, (8, LANES), 1)
    th = jnp.zeros((8, LANES), jnp.float32)
    for l in range(8):
        th = jnp.where(sub == l, thick_ref[l], th)
    level_id = sub + g * 8
    send_idx = [send_ref[:, side * LANES : (side + 1) * LANES] for side in range(2)]
    send_lane = [wide(i & (LANES - 1)) for i in send_idx]
    send_tile = [wide(i >> 7) for i in send_idx]

    def listed_levels(tiles, side):
        out = lane_gather(tiles[0], send_lane[side])
        for t in range(1, TILES):
            out = jnp.where(send_tile[side] == t, lane_gather(tiles[t], send_lane[side]), out)
        return out

    def listed_nodes(compact, side):
        got = lane_gather(compact, send_lane[side])
        return jnp.sum(jnp.where(send_tile[side] == sub, got, 0.0), axis=0, keepdims=True)

    def column(rho_tile):
        weighted = rho_tile * th
        total = weighted
        for shift in (1, 2, 4):
            total = total + jnp.where(sub >= shift, pltpu.roll(total, shift, 0), 0.0)
        return BUOYANCY * (total - 0.5 * weighted), total[7:8]

    def copy(src, dst, sems, i, a, b):
        return pltpu.make_async_remote_copy(
            src_ref=src,
            dst_ref=dst,
            send_sem=sems.at[0, i],
            recv_sem=sems.at[1, i],
            device_id=(a, b),
            device_id_type=MESH,
        )

    def arrived(buf, sems, i):
        pltpu.make_async_copy(buf, buf, sems.at[1, i]).wait()

    def left(buf, sems, i):
        pltpu.make_async_copy(buf, buf, sems.at[0, i]).wait()

    def send_velocity(s):
        for side in range(2):
            for c in range(2):
                usend[s, side, c] = listed_levels([x[c, d] for d in range(TILES)], side)
        copy(usend.at[s, 0], urecv.at[s, 1], usem, s, down, g).start()
        copy(usend.at[s, 1], urecv.at[s, 0], usem, s, up, g).start()

    def send_density(s):
        tiles = [x[2, d] for d in range(TILES)]
        for side in range(2):
            got = listed_levels(tiles, side)
            rsend[s, side] = got
            gsend[s, side, 0:1] = jnp.sum(got * th, axis=0, keepdims=True)
            gsend[s, side, 1:2] = listed_nodes(lsend[s, 1], side)
        copy(rsend.at[s, 0], rrecv.at[s, 1], rsem, s, down, g).start()
        copy(rsend.at[s, 1], rrecv.at[s, 0], rsem, s, up, g).start()
        for d in range(n_level):
            copy(gsend.at[s, 0], grecv.at[s, 1, d], gsem, s, down, level_peers[d]).start()
            copy(gsend.at[s, 1], grecv.at[s, 0, d], gsem, s, up, level_peers[d]).start()
        for d in range(TILES):
            ploc[d], lsend[s, 0, d : d + 1] = column(tiles[d])
        send_level(s)

    def send_level(s):
        for d in range(1, n_level):
            copy(lsend.at[s], lrecv.at[s, d - 1], lsem, s, p, level_peers[d]).start()

    for d in range(TILES):
        cols = slice(d * LANES, (d + 1) * LANES)
        wet = level_id < wide(bot_ref[d : d + 1])
        for c in range(2):
            x[c, d] = jnp.where(wet, vel_ref[c, :, cols], 0.0)
        x[2, d] = rho_ref[:, cols]
    eta[...] = eta_ref[...]
    wet_nodes = (bot_ref[...] > 0).astype(jnp.float32)
    lsend[0, 1] = jnp.zeros((8, LANES), jnp.float32)
    for side in range(2):
        ssend[side, 0:1] = listed_nodes(eta_ref[...], side)
        ssend[side, 1:2] = listed_nodes(wet_nodes, side)

    pl.semaphore_wait(barrier, count)
    for d in (1, n_z - 1):
        pl.semaphore_signal(tok.at[0], inc=1, device_id=(z_peer(d), g), device_id_type=MESH)
    send_velocity(0)
    send_density(0)
    copy(ssend.at[0], srecv.at[1], ssem, 0, down, g).start()
    copy(ssend.at[1], srecv.at[0], ssem, 0, up, g).start()

    for k in range(K):
        for d in range(TILES):
            cols = slice(d * LANES, (d + 1) * LANES)
            row = slice(d, d + 1)
            nbc[k, row] = nb_ref[k : k + 1, cols]
            wts[0, k, row] = grad_ref[0, k : k + 1, cols]
            wts[1, k, row] = grad_ref[1, k : k + 1, cols]
            wts[2, k, row] = lap_ref[k : k + 1, cols]
        tile = nbc[k] >> 7
        below = jnp.where(p > 0, 1.0, 0.0)
        above = jnp.where(p < n_space - 1, 1.0, 0.0)
        valid = jnp.where(tile == TILES, below, jnp.where(tile == TILES + 1, above, 1.0))
        for j in range(3):
            wts[j, k] = wts[j, k] * valid

    def slots(k, d):
        row = wide(nbc[k, d : d + 1])
        return row & (LANES - 1), row >> 7

    def gather_own():
        for d in range(TILES):
            for k in range(K):
                idx, tile = slots(k, d)
                masks = [tile == t for t in range(TILES)]
                for f in range(4):
                    src = [x[f, t] if f < 3 else ploc[t] for t in range(TILES)]
                    out = lane_gather(src[0], idx)
                    for t in range(1, TILES):
                        out = jnp.where(masks[t], lane_gather(src[t], idx), out)
                    near[f, d * K + k] = out

    def level_terms(s):
        arrived(urecv.at[s], usem, s)
        arrived(rrecv.at[s], rsem, s)
        halo = []
        for side in range(2):
            r = rrecv[s, side]
            halo.append([urecv[s, side, 0], urecv[s, side, 1], r, column(r)[0]])
        for d in range(TILES):
            own = [x[0, d], x[1, d], x[2, d], ploc[d]]
            zero = jnp.zeros((8, LANES), jnp.float32)
            dxu, dyv, lu, lv, lr, dxr, dyr, dxp, dyp = [zero] * 9
            for k in range(K):
                idx, tile = slots(k, d)
                m0, m1 = tile == TILES, tile == TILES + 1
                diff = []
                for f in range(4):
                    n = near[f, d * K + k]
                    n = jnp.where(m0, lane_gather(halo[0][f], idx), n)
                    n = jnp.where(m1, lane_gather(halo[1][f], idx), n)
                    diff.append(n - own[f])
                we, wn, wl = [wide(wts[j, k, d : d + 1]) for j in range(3)]
                dxu += we * diff[0]
                dyv += wn * diff[1]
                lu += wl * diff[0]
                lv += wl * diff[1]
                lr += wl * diff[2]
                dxr += we * diff[2]
                dyr += wn * diff[2]
                dxp += we * diff[3]
                dyp += wn * diff[3]
            u, v, r, _ = own
            cor = wide(cor_ref[d : d + 1])
            drag = jnp.where(level_id == wide(bot_ref[d : d + 1]) - 1, DRAG, 0.0)
            part[0, d] = u + DT * (cor * v - dxp + lu - drag * u)
            part[1, d] = v + DT * (lv - dyp - cor * u - drag * v)
            x[2, d] = r + DT * (lr - u * dxr - v * dyr)
            lsend[s + 1, 1, d : d + 1] = jnp.sum(th * (dxu + dyv), axis=0, keepdims=True)

    def shared_terms(s):
        arrived(lrecv.at[s], lsem, s)
        arrived(grecv.at[s], gsem, s)
        div, mass = lsend[s, 1], jnp.zeros((8, LANES), jnp.float32)
        for d in range(1, n_level):
            mass = mass + jnp.where(g >= d, lrecv[s, d - 1, 0], 0.0)
            div = div + lrecv[s, d - 1, 1]
        spread = wet_nodes * div
        new_eta = eta[...] - DT * spread
        eta[...] = new_eta
        vv[s] = area_ref[...] * spread
        own = new_eta + BUOYANCY * mass
        q[0:8] = own
        for side in range(2):
            row = slice(side, side + 1)
            m = jnp.zeros((1, LANES), jnp.float32)
            h = grecv[s, side, 0, 1:2]
            for d in range(1, n_level):
                m = m + jnp.where(g >= d, grecv[s, side, d, 0:1], 0.0)
                h = h + grecv[s, side, d, 1:2]
            e = etah[row] - DT * srecv[side, 1:2] * h
            etah[row] = e
            q[8 + side : 9 + side] = e + BUOYANCY * m
        dx = jnp.zeros((8, LANES), jnp.float32)
        dy = dx
        rows = [wide(q[t : t + 1]) for t in range(TILES + 2)]
        for k in range(K):
            slot = nbc[k]
            idx, tile = slot & (LANES - 1), slot >> 7
            n = lane_gather(rows[0], idx)
            for t in range(1, TILES + 2):
                n = jnp.where(tile == t, lane_gather(rows[t], idx), n)
            diff = n - own
            dx = dx + wts[0, k] * diff
            dy = dy + wts[1, k] * diff
        dq[0] = DT * dx
        dq[1] = DT * dy
        for d in range(TILES):
            wet = level_id < wide(bot_ref[d : d + 1])
            for c in range(2):
                x[c, d] = jnp.where(wet, part[c, d] - wide(dq[c, d : d + 1]), 0.0)

    def pass_token(i, dist):
        pl.semaphore_wait(tok.at[i - 1], 2)
        for d in (dist, n_z - dist):
            pl.semaphore_signal(tok.at[i], inc=1, device_id=(z_peer(d), g), device_id_type=MESH)

    def step(s, _):
        gather_own()

        @pl.when(s == 0)
        def _():
            arrived(srecv, ssem, 0)
            etah[...] = srecv[:, 0]

        level_terms(s)
        send_density(s + 1)
        shared_terms(s)
        send_velocity(s + 1)

        @pl.when(s == 0)
        def _():
            pass_token(1, 2)

        @pl.when(s == 1)
        def _():
            pass_token(2, 4)

        return 0

    lax.fori_loop(0, STEPS - 1, step, 0)
    last = STEPS - 1
    gather_own()
    level_terms(last)
    lsend[STEPS, 0] = jnp.zeros((8, LANES), jnp.float32)
    send_level(STEPS)
    for d in range(TILES):
        rho_out[:, d * LANES : (d + 1) * LANES] = x[2, d]
    shared_terms(last)
    for d in range(TILES):
        for c in range(2):
            vel_out[c, :, d * LANES : (d + 1) * LANES] = x[c, d]

    arrived(lrecv.at[STEPS], lsem, STEPS)
    div = lsend[STEPS, 1]
    for d in range(1, n_level):
        div = div + lrecv[STEPS, d - 1, 1]
    spread = wet_nodes * div
    sums = jnp.zeros((8, LANES), jnp.float32)
    terms = [vv[s + 1] for s in range(STEPS - 1)]
    terms += [area_ref[...] * spread, area_ref[...] * wet_nodes]
    for j, term in enumerate(terms):
        sums = jnp.where(sub == j, wide(jnp.sum(term, axis=0, keepdims=True)), sums)
    sums = jnp.broadcast_to(jnp.sum(sums, axis=1, keepdims=True), (8, LANES))
    row = jnp.sum(jnp.where(sub == lane, sums, 0.0), axis=0, keepdims=True)
    zsend[...] = row
    pl.semaphore_wait(tok.at[2], 2)
    for d in range(1, n_z):
        copy(zsend, zrecv.at[d - 1], zsem, 0, z_peer(d), g).start()
    arrived(zrecv, zsem, 0)
    for d in range(1, n_z):
        row = row + zrecv[d - 1]
    xsend[...] = row
    for d in range(1, X_CHIPS):
        copy(xsend, xrecv.at[d - 1], zsem, 1, x_peer(d), g).start()
    arrived(xrecv, zsem, 1)
    for d in range(1, X_CHIPS):
        row = row + xrecv[d - 1]
    lane_row = lane[0:1]
    total = jnp.sum(jnp.where(lane_row == STEPS, row, 0.0), axis=1, keepdims=True)
    drifts = jnp.where(lane_row < STEPS, row / total, 0.0)
    drift_out[...] = drifts
    eta_out[...] = eta[...] - DT * spread + DT * jnp.sum(drifts, axis=1, keepdims=True)

    for s in range(STEPS + 1):
        left(lrecv.at[s], lsem, s)
    for s in range(STEPS):
        left(usend.at[s], usem, s)
        left(rsend.at[s], rsem, s)
        left(grecv.at[s], gsem, s)
    left(ssend, ssem, 0)
    left(zrecv, zsem, 0)
    left(xrecv, zsem, 1)


def solution(mesh):
    n_space, n_level = mesh.shape["space"], mesh.shape["level"]

    def local(
        velocity,
        density,
        elevation,
        grad_weights,
        lap_weights,
        coriolis,
        node_area,
        thickness,
        send_list,
        neighbours,
        bottom,
    ):
        f32, i32 = jnp.float32, jnp.int32
        compact = (TILES, LANES)
        vmem = pl.BlockSpec(memory_space=pltpu.VMEM)
        smem = pl.BlockSpec(memory_space=pltpu.SMEM)
        dma = pltpu.SemaphoreType.DMA
        peers = n_level - 1
        n_z = n_space // X_CHIPS
        shapes = [
            ((K, 8, LANES), i32),
            ((3, K, 8, LANES), f32),
            ((3, 8, 8, LANES), f32),
            ((10, 8, LANES), f32),
            ((2, 8, 8, LANES), f32),
            ((4, 48, 8, LANES), f32),
            ((16, LANES), f32),
            ((2, 8, LANES), f32),
            ((8, LANES), f32),
            ((2, LANES), f32),
            ((5, 8, LANES), f32),
            ((5, 2, 8, LANES), f32),
            ((5, peers, 2, 8, LANES), f32),
            ((4, 2, 2, 8, LANES), f32),
            ((4, 2, 2, 8, LANES), f32),
            ((4, 2, 8, LANES), f32),
            ((4, 2, 8, LANES), f32),
            ((4, 2, 2, LANES), f32),
            ((4, 2, n_level, 2, LANES), f32),
            ((2, 2, LANES), f32),
            ((2, 2, LANES), f32),
            ((1, LANES), f32),
            ((n_z - 1, 1, LANES), f32),
            ((1, LANES), f32),
            ((X_CHIPS - 1, 1, LANES), f32),
        ]

        def body(*refs):
            kernel(n_space, n_level, *refs)

        vel, rho, eta, drift = pl.pallas_call(
            body,
            out_shape=(
                jax.ShapeDtypeStruct(velocity.shape, f32),
                jax.ShapeDtypeStruct(density.shape, f32),
                jax.ShapeDtypeStruct(compact, f32),
                jax.ShapeDtypeStruct((1, LANES), f32),
            ),
            in_specs=[vmem] * 7 + [smem] + [vmem] * 3,
            out_specs=(vmem,) * 4,
            scratch_shapes=[pltpu.VMEM(a, t) for a, t in shapes]
            + [
                dma((2, 5)),
                dma((2, 4)),
                dma((2, 4)),
                dma((2, 4)),
                dma((2, 1)),
                dma((2, 2)),
                pltpu.SemaphoreType.REGULAR((3,)),
            ],
            compiler_params=pltpu.CompilerParams(collective_id=0, has_side_effects=True),
        )(
            velocity,
            density,
            elevation.reshape(compact),
            grad_weights,
            lap_weights,
            coriolis.reshape(compact),
            node_area.reshape(compact),
            thickness,
            send_list,
            neighbours,
            bottom.reshape(compact),
        )
        return vel, rho, eta.reshape(elevation.shape), drift[0, :STEPS]

    return jax.shard_map(
        local,
        mesh=mesh,
        in_specs=(
            P(None, "level", "space"),
            P("level", "space"),
            P("space"),
            P(None, None, "space"),
            P(None, "space"),
            P("space"),
            P("space"),
            P("level"),
            P("space", None),
            P(None, "space"),
            P("space"),
        ),
        out_specs=(P(None, "level", "space"), P("level", "space"), P("space"), P()),
        check_vma=False,
    )
```

```python
import jax
import jax.numpy as jnp
from jax import lax
from jax.experimental import pallas as pl
from jax.experimental.pallas import tpu as pltpu
from jax.sharding import PartitionSpec as P

MESH = pl.DeviceIdType.MESH
STEPS = 4
K = 6
TILES = 8
LANES = 128
X_CHIPS = 4
DT = 0.1
BUOYANCY = 0.5
DRAG = 0.5

_LANE_GATHER = lax.GatherDimensionNumbers(
    offset_dims=(),
    collapsed_slice_dims=(1,),
    start_index_map=(1,),
    operand_batching_dims=(0,),
    start_indices_batching_dims=(0,),
)


def lane_gather(x, idx):
    return lax.gather(
        x, idx[..., None], _LANE_GATHER, (1, 1), mode=lax.GatherScatterMode.PROMISE_IN_BOUNDS
    )


def wide(row):
    return jnp.broadcast_to(row, (8, LANES))


def kernel(
    n_space,
    n_level,
    vel_hbm,
    rho_hbm,
    eta_hbm,
    grad_hbm,
    lap_hbm,
    cor_hbm,
    area_hbm,
    thick_hbm,
    send_hbm,
    nb_hbm,
    bot_hbm,
    vel_out,
    rho_out,
    eta_out,
    drift_out,
    vel_ref,
    rho_ref,
    eta_ref,
    grad_ref,
    lap_ref,
    cor_ref,
    area_ref,
    thick_ref,
    send_ref,
    nb_ref,
    bot_ref,
    isem,
    nbc,
    wts,
    x,
    r,
    ploc,
    part,
    near,
    q,
    dq,
    eta,
    etah,
    vv,
    lsend,
    lrecv,
    usend,
    urecv,
    rsend,
    rrecv,
    gsend,
    grecv,
    ssend,
    srecv,
    zsend,
    zrecv,
    xsend,
    xrecv,
    lsem,
    usem,
    rsem,
    gsem,
    ssem,
    zsem,
    tok,
):
    p = lax.axis_index("space")
    g = lax.axis_index("level")
    n_z = n_space // X_CHIPS
    up = lax.rem(p + 1, n_space)
    down = lax.rem(p + n_space - 1, n_space)
    level_peers = [lax.rem(g + d, n_level) for d in range(n_level)]

    def z_peer(d):
        return lax.rem(p + d * X_CHIPS, n_space)

    px = lax.rem(p, X_CHIPS)
    x_peers = [p - px + lax.rem(px + d, X_CHIPS) for d in range(X_CHIPS)]
    plane = [(a, b) for a in range(X_CHIPS) for b in range(n_level) if a or b]

    barrier = pltpu.get_barrier_semaphore()
    count = 0

    def greet(a, b):
        pl.semaphore_signal(barrier, inc=1, device_id=(a, b), device_id_type=MESH)

    for d in range(n_level):
        greet(up, level_peers[d])
        greet(down, level_peers[d])
        count += 2
    for a, b in plane:
        greet(x_peers[a], level_peers[b])
        count += 1
    for d in (1, n_z - 1):
        greet(z_peer(d), g)
        count += 1

    inputs = [
        (send_hbm, send_ref),
        (vel_hbm, vel_ref),
        (bot_hbm, bot_ref),
        (rho_hbm, rho_ref),
        (thick_hbm, thick_ref),
        (eta_hbm, eta_ref),
        (nb_hbm, nb_ref),
        (grad_hbm, grad_ref),
        (lap_hbm, lap_ref),
        (cor_hbm, cor_ref),
        (area_hbm, area_ref),
    ]
    loads = [pltpu.make_async_copy(a, b, isem.at[i]) for i, (a, b) in enumerate(inputs)]
    for load in loads:
        load.start()

    sub = lax.broadcasted_iota(jnp.int32, (8, LANES), 0)
    lane = lax.broadcasted_iota(jnp.int32, (8, LANES), 1)
    level_id = sub + g * 8
    for load in loads[:5]:
        load.wait()
    th = jnp.zeros((8, LANES), jnp.float32)
    for l in range(8):
        th = jnp.where(sub == l, thick_ref[l], th)
    send_idx = [send_ref[:, side * LANES : (side + 1) * LANES] for side in range(2)]
    send_lane = [wide(i & (LANES - 1)) for i in send_idx]
    send_tile = [wide(i >> 7) for i in send_idx]

    def listed_levels(tiles, side):
        out = lane_gather(tiles[0], send_lane[side])
        for t in range(1, TILES):
            out = jnp.where(send_tile[side] == t, lane_gather(tiles[t], send_lane[side]), out)
        return out

    def listed_nodes(compact, side):
        got = lane_gather(compact, send_lane[side])
        return jnp.sum(jnp.where(send_tile[side] == sub, got, 0.0), axis=0, keepdims=True)

    def column(rho_tile):
        weighted = rho_tile * th
        total = weighted
        for shift in (1, 2, 4):
            total = total + jnp.where(sub >= shift, pltpu.roll(total, shift, 0), 0.0)
        return BUOYANCY * (total - 0.5 * weighted), total[7:8]

    def copy(src, dst, sems, i, a, b):
        return pltpu.make_async_remote_copy(
            src_ref=src,
            dst_ref=dst,
            send_sem=sems.at[0, i],
            recv_sem=sems.at[1, i],
            device_id=(a, b),
            device_id_type=MESH,
        )

    def arrived(buf, sems, i):
        pltpu.make_async_copy(buf, buf, sems.at[1, i]).wait()

    def left(buf, sems, i):
        pltpu.make_async_copy(buf, buf, sems.at[0, i]).wait()

    def list_velocity(s):
        for side in range(2):
            for c in range(2):
                usend[s, side, c] = listed_levels([x[c, d] for d in range(TILES)], side)

    def send_velocity(s):
        copy(usend.at[s, 0], urecv.at[s, 1], usem, s, down, g).start()
        copy(usend.at[s, 1], urecv.at[s, 0], usem, s, up, g).start()

    def list_density(s, par):
        tiles = [r[par, d] for d in range(TILES)]
        for side in range(2):
            got = listed_levels(tiles, side)
            rsend[s, side] = got
            gsend[s, side, 0:1] = jnp.sum(got * th, axis=0, keepdims=True)
        for d in range(TILES):
            ploc[d], lsend[s, 0, d : d + 1] = column(tiles[d])

    def send_density(s):
        copy(rsend.at[s, 0], rrecv.at[s, 1], rsem, s, down, g).start()
        copy(rsend.at[s, 1], rrecv.at[s, 0], rsem, s, up, g).start()

    def send_sums(s):
        for d in range(n_level):
            copy(gsend.at[s, 0], grecv.at[s, 1, d], gsem, s, down, level_peers[d]).start()
            copy(gsend.at[s, 1], grecv.at[s, 0, d], gsem, s, up, level_peers[d]).start()

    def send_level(s):
        for d in range(1, n_level):
            copy(lsend.at[s], lrecv.at[s, d - 1], lsem, s, p, level_peers[d]).start()

    for d in range(TILES):
        cols = slice(d * LANES, (d + 1) * LANES)
        wet = level_id < wide(bot_ref[d : d + 1])
        for c in range(2):
            x[c, d] = jnp.where(wet, vel_ref[c, :, cols], 0.0)
        r[0, d] = rho_ref[:, cols]
    list_velocity(0)
    list_density(0, 0)
    lsend[0, 1] = jnp.zeros((8, LANES), jnp.float32)
    for side in range(2):
        gsend[0, side, 1:2] = jnp.zeros((1, LANES), jnp.float32)
    loads[5].wait()
    wet_nodes = (bot_ref[...] > 0).astype(jnp.float32)
    eta[...] = eta_ref[...]
    for side in range(2):
        ssend[side, 0:1] = listed_nodes(eta_ref[...], side)
        ssend[side, 1:2] = listed_nodes(wet_nodes, side)

    pl.semaphore_wait(barrier, count)
    send_velocity(0)
    send_sums(0)
    send_density(0)
    send_level(0)
    copy(ssend.at[0], srecv.at[1], ssem, 0, down, g).start()
    copy(ssend.at[1], srecv.at[0], ssem, 0, up, g).start()
    for d in (1, n_z - 1):
        pl.semaphore_signal(tok.at[0], inc=1, device_id=(z_peer(d), g), device_id_type=MESH)

    for load in loads[6:]:
        load.wait()
    for k in range(K):
        for d in range(TILES):
            cols = slice(d * LANES, (d + 1) * LANES)
            row = slice(d, d + 1)
            nbc[k, row] = nb_ref[k : k + 1, cols]
            wts[0, k, row] = grad_ref[k, 0:1, cols]
            wts[1, k, row] = grad_ref[k, 1:2, cols]
            wts[2, k, row] = lap_ref[k : k + 1, cols]
        tile = nbc[k] >> 7
        below = jnp.where(p > 0, 1.0, 0.0)
        above = jnp.where(p < n_space - 1, 1.0, 0.0)
        valid = jnp.where(tile == TILES, below, jnp.where(tile == TILES + 1, above, 1.0))
        for j in range(3):
            wts[j, k] = wts[j, k] * valid

    def slots(k, d):
        row = wide(nbc[k, d : d + 1])
        return row & (LANES - 1), row >> 7

    def weights(k, d):
        return [wide(wts[j, k, d : d + 1]) for j in range(3)]

    def gather_velocity():
        for d in range(TILES):
            for k in range(K):
                idx, tile = slots(k, d)
                outs = [lane_gather(x[c, 0], idx) for c in range(2)]
                for t in range(1, TILES):
                    hit = tile == t
                    outs = [jnp.where(hit, lane_gather(x[c, t], idx), outs[c]) for c in range(2)]
                for c in range(2):
                    near[c, d * K + k] = outs[c]

    def density_terms(s, par):
        arrived(rrecv.at[s], rsem, s)
        halo = [(rrecv[s, side], column(rrecv[s, side])[0]) for side in range(2)]
        for d in range(TILES):
            own = (r[par, d], ploc[d])
            zero = jnp.zeros((8, LANES), jnp.float32)
            lr, dxr, dyr, dxp, dyp = [zero] * 5
            for k in range(K):
                idx, tile = slots(k, d)
                outs = [lane_gather(r[par, 0], idx), lane_gather(ploc[0], idx)]
                for t in range(1, TILES + 2):
                    hit = tile == t
                    src = (r[par, t], ploc[t]) if t < TILES else halo[t - TILES]
                    outs = [jnp.where(hit, lane_gather(a, idx), o) for a, o in zip(src, outs)]
                dr, dp = [a - b for a, b in zip(outs, own)]
                we, wn, wl = weights(k, d)
                lr += wl * dr
                dxr += we * dr
                dyr += wn * dr
                dxp += we * dp
                dyp += wn * dp
            u, v = x[0, d], x[1, d]
            cor = wide(cor_ref[d : d + 1])
            drag = jnp.where(level_id == wide(bot_ref[d : d + 1]) - 1, DRAG, 0.0)
            part[0, d] = u + DT * (cor * v - dxp - drag * u)
            part[1, d] = v - DT * (cor * u + dyp + drag * v)
            r[1 - par, d] = own[0] + DT * (lr - u * dxr - v * dyr)

    def velocity_terms(s):
        arrived(urecv.at[s], usem, s)
        halo = [[urecv[s, side, c] for c in range(2)] for side in range(2)]
        for d in range(TILES):
            u, v = x[0, d], x[1, d]
            zero = jnp.zeros((8, LANES), jnp.float32)
            dxu, dyv, lu, lv = [zero] * 4
            for k in range(K):
                idx, tile = slots(k, d)
                outs = [near[c, d * K + k] for c in range(2)]
                for side in range(2):
                    hit = tile == TILES + side
                    outs = [jnp.where(hit, lane_gather(halo[side][c], idx), outs[c]) for c in range(2)]
                we, wn, wl = weights(k, d)
                du, dv = outs[0] - u, outs[1] - v
                dxu += we * du
                dyv += wn * dv
                lu += wl * du
                lv += wl * dv
            part[0, d] = part[0, d] + DT * lu
            part[1, d] = part[1, d] + DT * lv
            lsend[s + 1, 1, d : d + 1] = jnp.sum(th * (dxu + dyv), axis=0, keepdims=True)
        vv[s] = area_ref[...] * wet_nodes * lsend[s + 1, 1]

    def list_divergence(s):
        div = lsend[s, 1]
        for side in range(2):
            gsend[s, side, 1:2] = listed_nodes(div, side)

    def shared_terms(s):
        arrived(lrecv.at[s], lsem, s)
        arrived(grecv.at[s], gsem, s)
        div, mass = lsend[s, 1], jnp.zeros((8, LANES), jnp.float32)
        for d in range(1, n_level):
            mass = mass + jnp.where(g >= d, lrecv[s, d - 1, 0], 0.0)
            div = div + lrecv[s, d - 1, 1]
        new_eta = eta[...] - DT * wet_nodes * div
        eta[...] = new_eta
        own = new_eta + BUOYANCY * mass
        q[0:8] = own
        for side in range(2):
            row = slice(side, side + 1)
            m = jnp.zeros((1, LANES), jnp.float32)
            h = grecv[s, side, 0, 1:2]
            for d in range(1, n_level):
                m = m + jnp.where(g >= d, grecv[s, side, d, 0:1], 0.0)
                h = h + grecv[s, side, d, 1:2]
            e = etah[row] - DT * srecv[side, 1:2] * h
            etah[row] = e
            q[8 + side : 9 + side] = e + BUOYANCY * m
        dx = jnp.zeros((8, LANES), jnp.float32)
        dy = dx
        rows = [wide(q[t : t + 1]) for t in range(TILES + 2)]
        for k in range(K):
            slot = nbc[k]
            idx, tile = slot & (LANES - 1), slot >> 7
            n = lane_gather(rows[0], idx)
            for t in range(1, TILES + 2):
                n = jnp.where(tile == t, lane_gather(rows[t], idx), n)
            diff = n - own
            dx = dx + wts[0, k] * diff
            dy = dy + wts[1, k] * diff
        dq[0] = DT * dx
        dq[1] = DT * dy
        for d in range(TILES):
            wet = level_id < wide(bot_ref[d : d + 1])
            for c in range(2):
                x[c, d] = jnp.where(wet, part[c, d] - wide(dq[c, d : d + 1]), 0.0)

    def pass_token(i, dist):
        pl.semaphore_wait(tok.at[i - 1], 2)
        for d in (dist, n_z - dist):
            pl.semaphore_signal(tok.at[i], inc=1, device_id=(z_peer(d), g), device_id_type=MESH)

    def step(s, _):
        par = lax.rem(s, 2)
        gather_velocity()
        density_terms(s, par)
        list_density(s + 1, 1 - par)
        send_density(s + 1)
        velocity_terms(s)
        list_divergence(s + 1)
        send_sums(s + 1)
        send_level(s + 1)

        @pl.when(s == 0)
        def _():
            arrived(srecv, ssem, 0)
            etah[...] = srecv[:, 0]

        shared_terms(s)
        list_velocity(s + 1)
        send_velocity(s + 1)

        @pl.when(s == 0)
        def _():
            pass_token(1, 2)

        @pl.when(s == 1)
        def _():
            pass_token(2, 4)

        return 0

    lax.fori_loop(0, STEPS - 1, step, 0)
    last = STEPS - 1
    par = last % 2
    gather_velocity()
    density_terms(last, par)
    for d in range(TILES):
        rho_out[:, d * LANES : (d + 1) * LANES] = r[1 - par, d]
    lsend[STEPS, 0] = jnp.zeros((8, LANES), jnp.float32)
    velocity_terms(last)

    sums = jnp.zeros((8, LANES), jnp.float32)
    terms = [vv[s] for s in range(STEPS)] + [area_ref[...] * wet_nodes * (1.0 / n_level)]
    for j, term in enumerate(terms):
        sums = jnp.where(sub == j, wide(jnp.sum(term, axis=0, keepdims=True)), sums)
    sums = jnp.broadcast_to(jnp.sum(sums, axis=1, keepdims=True), (8, LANES))
    row = jnp.sum(jnp.where(sub == lane, sums, 0.0), axis=0, keepdims=True)
    zsend[...] = row
    pl.semaphore_wait(tok.at[2], 2)
    for d in range(1, n_z):
        copy(zsend, zrecv.at[d - 1], zsem, 0, z_peer(d), g).start()
    send_level(STEPS)

    shared_terms(last)
    for d in range(TILES):
        for c in range(2):
            vel_out[c, :, d * LANES : (d + 1) * LANES] = x[c, d]
    arrived(lrecv.at[STEPS], lsem, STEPS)
    div = lsend[STEPS, 1]
    for d in range(1, n_level):
        div = div + lrecv[STEPS, d - 1, 1]
    eta[...] = eta[...] - DT * wet_nodes * div

    arrived(zrecv, zsem, 0)
    for d in range(1, n_z):
        row = row + zrecv[d - 1]
    xsend[...] = row
    for i, (a, b) in enumerate(plane):
        copy(xsend, xrecv.at[i], zsem, 1, x_peers[a], level_peers[b]).start()
    arrived(xrecv, zsem, 1)
    for i in range(len(plane)):
        row = row + xrecv[i]
    lane_row = lane[0:1]
    total = jnp.sum(jnp.where(lane_row == STEPS, row, 0.0), axis=1, keepdims=True)
    drifts = jnp.where(lane_row < STEPS, row / total, 0.0)
    drift_out[...] = drifts
    eta_out[...] = eta[...] + DT * jnp.sum(drifts, axis=1, keepdims=True)

    for s in range(STEPS + 1):
        left(lrecv.at[s], lsem, s)
    for s in range(STEPS):
        left(usend.at[s], usem, s)
        left(rsend.at[s], rsem, s)
        left(grecv.at[s], gsem, s)
    left(ssend, ssem, 0)
    left(zrecv, zsem, 0)
    left(xrecv, zsem, 1)


def solution(mesh):
    n_space, n_level = mesh.shape["space"], mesh.shape["level"]

    def local(
        velocity,
        density,
        elevation,
        grad_weights,
        lap_weights,
        coriolis,
        node_area,
        thickness,
        send_list,
        neighbours,
        bottom,
    ):
        f32, i32 = jnp.float32, jnp.int32
        compact = (TILES, LANES)
        vmem = pl.BlockSpec(memory_space=pltpu.VMEM)
        dma = pltpu.SemaphoreType.DMA
        peers = n_level - 1
        n_z = n_space // X_CHIPS
        row = (1, LANES)
        inputs = [
            pltpu.VMEM(velocity.shape, f32),
            pltpu.VMEM(density.shape, f32),
            pltpu.VMEM(compact, f32),
            pltpu.VMEM((K, 2, TILES * LANES), f32),
            pltpu.VMEM(lap_weights.shape, f32),
            pltpu.VMEM(compact, f32),
            pltpu.VMEM(compact, f32),
            pltpu.SMEM(thickness.shape, f32),
            pltpu.VMEM(send_list.shape, i32),
            pltpu.VMEM(neighbours.shape, i32),
            pltpu.VMEM(compact, i32),
            dma((11,)),
            pltpu.VMEM((K, 8, LANES), i32),
        ]
        shapes = [
            (3, K, 8, LANES),
            (2, 8, 8, LANES),
            (2, 8, 8, LANES),
            (8, 8, LANES),
            (2, 8, 8, LANES),
            (2, 48, 8, LANES),
            (16, LANES),
            (2, 8, LANES),
            (8, LANES),
            (2, LANES),
            (STEPS, 8, LANES),
            (STEPS + 1, 2, 8, LANES),
            (STEPS + 1, peers, 2, 8, LANES),
            (STEPS, 2, 2, 8, LANES),
            (STEPS, 2, 2, 8, LANES),
            (STEPS, 2, 8, LANES),
            (STEPS, 2, 8, LANES),
            (STEPS, 2, 2, LANES),
            (STEPS, 2, n_level, 2, LANES),
            (2, 2, LANES),
            (2, 2, LANES),
            row,
            (n_z - 1, *row),
            row,
            (X_CHIPS * n_level - 1, *row),
        ]

        def body(*refs):
            kernel(n_space, n_level, *refs)

        vel, rho, eta, drift = pl.pallas_call(
            body,
            out_shape=(
                jax.ShapeDtypeStruct(velocity.shape, f32),
                jax.ShapeDtypeStruct(density.shape, f32),
                jax.ShapeDtypeStruct(compact, f32),
                jax.ShapeDtypeStruct((1, LANES), f32),
            ),
            in_specs=[pl.BlockSpec(memory_space=pl.ANY)] * 11,
            out_specs=(vmem,) * 4,
            scratch_shapes=inputs
            + [pltpu.VMEM(shape, f32) for shape in shapes]
            + [
                dma((2, 5)),
                dma((2, 4)),
                dma((2, 4)),
                dma((2, 4)),
                dma((2, 1)),
                dma((2, 2)),
                pltpu.SemaphoreType.REGULAR((3,)),
            ],
            compiler_params=pltpu.CompilerParams(collective_id=0, has_side_effects=True),
        )(
            velocity,
            density,
            elevation.reshape(compact),
            jnp.swapaxes(grad_weights, 0, 1),
            lap_weights,
            coriolis.reshape(compact),
            node_area.reshape(compact),
            thickness,
            send_list,
            neighbours,
            bottom.reshape(compact),
        )
        return vel, rho, eta.reshape(elevation.shape), drift[0, :STEPS]

    return jax.shard_map(
        local,
        mesh=mesh,
        in_specs=(
            P(None, "level", "space"),
            P("level", "space"),
            P("space"),
            P(None, None, "space"),
            P(None, "space"),
            P("space"),
            P("space"),
            P("level"),
            P("space", None),
            P(None, "space"),
            P("space"),
        ),
        out_specs=(P(None, "level", "space"), P("level", "space"), P("space"), P()),
        check_vma=False,
    )
```

```python
import jax
import jax.numpy as jnp
from jax import lax
from jax.experimental import pallas as pl
from jax.experimental.pallas import tpu as pltpu
from jax.sharding import PartitionSpec as P

MESH = pl.DeviceIdType.MESH
STEPS = 4
K = 6
TILES = 8
LANES = 128
X_CHIPS = 4
DT = 0.1
BUOYANCY = 0.5
DRAG = 0.5

_LANE_GATHER = lax.GatherDimensionNumbers(
    offset_dims=(),
    collapsed_slice_dims=(1,),
    start_index_map=(1,),
    operand_batching_dims=(0,),
    start_indices_batching_dims=(0,),
)


def lane_gather(x, idx):
    return lax.gather(
        x, idx[..., None], _LANE_GATHER, (1, 1), mode=lax.GatherScatterMode.PROMISE_IN_BOUNDS
    )


def wide(row):
    return jnp.broadcast_to(row, (8, LANES))


def kernel(
    n_space,
    n_level,
    vel_hbm,
    rho_hbm,
    eta_hbm,
    grad_hbm,
    lap_hbm,
    cor_hbm,
    area_hbm,
    thick_hbm,
    send_hbm,
    nb_hbm,
    bot_hbm,
    vel_out,
    rho_out,
    eta_out,
    drift_out,
    vel_ref,
    rho_ref,
    eta_ref,
    grad_ref,
    lap_ref,
    cor_ref,
    area_ref,
    thick_ref,
    send_ref,
    nb_ref,
    bot_ref,
    isem,
    nbc,
    wts,
    x,
    r,
    ploc,
    part,
    near,
    q,
    dq,
    eta,
    etah,
    vv,
    lsend,
    lrecv,
    usend,
    urecv,
    rsend,
    rrecv,
    gsend,
    grecv,
    ssend,
    srecv,
    zsend,
    zrecv,
    xsend,
    xrecv,
    lsem,
    usem,
    rsem,
    gsem,
    ssem,
    zsem,
    tok,
):
    p = lax.axis_index("space")
    g = lax.axis_index("level")
    n_z = n_space // X_CHIPS
    up = lax.rem(p + 1, n_space)
    down = lax.rem(p + n_space - 1, n_space)
    level_peers = [lax.rem(g + d, n_level) for d in range(n_level)]

    def z_peer(d):
        return lax.rem(p + d * X_CHIPS, n_space)

    px = lax.rem(p, X_CHIPS)
    x_peers = [p - px + lax.rem(px + d, X_CHIPS) for d in range(X_CHIPS)]
    plane = [(a, b) for a in range(X_CHIPS) for b in range(n_level) if a or b]

    inputs = [
        (send_hbm, send_ref),
        (vel_hbm, vel_ref),
        (bot_hbm, bot_ref),
        (rho_hbm, rho_ref),
        (thick_hbm, thick_ref),
        (eta_hbm, eta_ref),
        (nb_hbm, nb_ref),
        (grad_hbm, grad_ref),
        (lap_hbm, lap_ref),
        (cor_hbm, cor_ref),
        (area_hbm, area_ref),
    ]
    loads = [pltpu.make_async_copy(a, b, isem.at[i]) for i, (a, b) in enumerate(inputs)]
    for load in loads:
        load.start()

    barrier = pltpu.get_barrier_semaphore()
    count = 0

    def greet(a, b):
        pl.semaphore_signal(barrier, inc=1, device_id=(a, b), device_id_type=MESH)

    for d in range(n_level):
        greet(up, level_peers[d])
        greet(down, level_peers[d])
        count += 2
        if d:
            greet(p, level_peers[d])
            count += 1

    sub = lax.broadcasted_iota(jnp.int32, (8, LANES), 0)
    lane = lax.broadcasted_iota(jnp.int32, (8, LANES), 1)
    level_id = sub + g * 8
    for load in loads[:5]:
        load.wait()
    th = jnp.zeros((8, LANES), jnp.float32)
    for l in range(8):
        th = jnp.where(sub == l, thick_ref[l], th)
    send_idx = [send_ref[:, side * LANES : (side + 1) * LANES] for side in range(2)]
    send_lane = [wide(i & (LANES - 1)) for i in send_idx]
    send_tile = [wide(i >> 7) for i in send_idx]

    def listed_levels(tiles, side):
        out = lane_gather(tiles[0], send_lane[side])
        for t in range(1, TILES):
            out = jnp.where(send_tile[side] == t, lane_gather(tiles[t], send_lane[side]), out)
        return out

    def listed_nodes(compact, side):
        got = lane_gather(compact, send_lane[side])
        return jnp.sum(jnp.where(send_tile[side] == sub, got, 0.0), axis=0, keepdims=True)

    def column(rho_tile):
        weighted = rho_tile * th
        total = weighted
        for shift in (1, 2, 4):
            total = total + jnp.where(sub >= shift, pltpu.roll(total, shift, 0), 0.0)
        return BUOYANCY * (total - 0.5 * weighted), total[7:8]

    def copy(src, dst, sems, i, a, b):
        return pltpu.make_async_remote_copy(
            src_ref=src,
            dst_ref=dst,
            send_sem=sems.at[0, i],
            recv_sem=sems.at[1, i],
            device_id=(a, b),
            device_id_type=MESH,
        )

    def arrived(buf, sems, i):
        pltpu.make_async_copy(buf, buf, sems.at[1, i]).wait()

    def left(buf, sems, i):
        pltpu.make_async_copy(buf, buf, sems.at[0, i]).wait()

    def send_token(i):
        for d in (2**i, n_space - 2**i):
            there = (lax.rem(p + d, n_space), g)
            pl.semaphore_signal(tok.at[i], inc=1, device_id=there, device_id_type=MESH)

    def pass_token(i):
        pl.semaphore_wait(tok.at[i - 1], 2)
        send_token(i)

    def list_velocity(s):
        for side in range(2):
            for c in range(2):
                usend[s, side, c] = listed_levels([x[c, d] for d in range(TILES)], side)

    def send_velocity(s):
        copy(usend.at[s, 0], urecv.at[s, 1], usem, s, down, g).start()
        copy(usend.at[s, 1], urecv.at[s, 0], usem, s, up, g).start()

    def list_density(s, par):
        tiles = [r[par, d] for d in range(TILES)]
        for side in range(2):
            got = listed_levels(tiles, side)
            rsend[s, side] = got
            gsend[s, side, 0:1] = jnp.sum(got * th, axis=0, keepdims=True)
        for d in range(TILES):
            ploc[d], lsend[s, 0, d : d + 1] = column(tiles[d])

    def send_density(s):
        copy(rsend.at[s, 0], rrecv.at[s, 1], rsem, s, down, g).start()
        copy(rsend.at[s, 1], rrecv.at[s, 0], rsem, s, up, g).start()

    def send_sums(s):
        for d in range(n_level):
            copy(gsend.at[s, 0], grecv.at[s, 1, d], gsem, s, down, level_peers[d]).start()
            copy(gsend.at[s, 1], grecv.at[s, 0, d], gsem, s, up, level_peers[d]).start()

    def send_level(s):
        for d in range(1, n_level):
            copy(lsend.at[s], lrecv.at[s, d - 1], lsem, s, p, level_peers[d]).start()

    for d in range(TILES):
        cols = slice(d * LANES, (d + 1) * LANES)
        wet = level_id < wide(bot_ref[d : d + 1])
        for c in range(2):
            x[c, d] = jnp.where(wet, vel_ref[c, :, cols], 0.0)
        r[0, d] = rho_ref[:, cols]
    list_velocity(0)
    list_density(0, 0)
    lsend[0, 1] = jnp.zeros((8, LANES), jnp.float32)
    for side in range(2):
        gsend[0, side, 1:2] = jnp.zeros((1, LANES), jnp.float32)
    loads[5].wait()
    wet_nodes = (bot_ref[...] > 0).astype(jnp.float32)
    eta[...] = eta_ref[...]
    for side in range(2):
        ssend[side, 0:1] = listed_nodes(eta_ref[...], side)
        ssend[side, 1:2] = listed_nodes(wet_nodes, side)

    pl.semaphore_wait(barrier, count)
    send_velocity(0)
    send_sums(0)
    send_density(0)
    send_level(0)
    copy(ssend.at[0], srecv.at[1], ssem, 0, down, g).start()
    copy(ssend.at[1], srecv.at[0], ssem, 0, up, g).start()
    send_token(0)

    for load in loads[6:]:
        load.wait()
    for k in range(K):
        for d in range(TILES):
            cols = slice(d * LANES, (d + 1) * LANES)
            row = slice(d, d + 1)
            nbc[k, row] = nb_ref[k : k + 1, cols]
            wts[0, k, row] = grad_ref[k, 0:1, cols]
            wts[1, k, row] = grad_ref[k, 1:2, cols]
            wts[2, k, row] = lap_ref[k : k + 1, cols]
        tile = nbc[k] >> 7
        below = jnp.where(p > 0, 1.0, 0.0)
        above = jnp.where(p < n_space - 1, 1.0, 0.0)
        valid = jnp.where(tile == TILES, below, jnp.where(tile == TILES + 1, above, 1.0))
        for j in range(3):
            wts[j, k] = wts[j, k] * valid

    def slots(k, d):
        row = wide(nbc[k, d : d + 1])
        return row & (LANES - 1), row >> 7

    def weights(k, d):
        return [wide(wts[j, k, d : d + 1]) for j in range(3)]

    def gather_own(par):
        for d in range(TILES):
            for k in range(K):
                idx, tile = slots(k, d)
                outs = [None] * 4
                for t in range(TILES):
                    hit = tile == t
                    for f, a in enumerate((x[0, t], x[1, t], r[par, t], ploc[t])):
                        got = lane_gather(a, idx)
                        outs[f] = jnp.where(hit, got, outs[f]) if t else got
                for f in range(4):
                    near[f, d * K + k] = outs[f]

    def with_halo(fields, halo, idx, tile, at):
        outs = [near[f, at] for f in fields]
        for side in range(2):
            hit = tile == TILES + side
            outs = [jnp.where(hit, lane_gather(a, idx), o) for a, o in zip(halo[side], outs)]
        return outs

    def density_terms(s, par):
        arrived(rrecv.at[s], rsem, s)
        halo = [(rrecv[s, side], column(rrecv[s, side])[0]) for side in range(2)]
        for d in range(TILES):
            own, own_p = r[par, d], ploc[d]
            zero = jnp.zeros((8, LANES), jnp.float32)
            lr, dxr, dyr, dxp, dyp = [zero] * 5
            for k in range(K):
                idx, tile = slots(k, d)
                near_r, near_p = with_halo((2, 3), halo, idx, tile, d * K + k)
                dr, dp = near_r - own, near_p - own_p
                we, wn, wl = weights(k, d)
                lr += wl * dr
                dxr += we * dr
                dyr += wn * dr
                dxp += we * dp
                dyp += wn * dp
            u, v = x[0, d], x[1, d]
            cor = wide(cor_ref[d : d + 1])
            drag = jnp.where(level_id == wide(bot_ref[d : d + 1]) - 1, DRAG, 0.0)
            part[0, d] = u + DT * (cor * v - dxp - drag * u)
            part[1, d] = v - DT * (cor * u + dyp + drag * v)
            r[1 - par, d] = own + DT * (lr - u * dxr - v * dyr)

    def velocity_terms(s):
        arrived(urecv.at[s], usem, s)
        halo = [[urecv[s, side, c] for c in range(2)] for side in range(2)]
        for d in range(TILES):
            u, v = x[0, d], x[1, d]
            zero = jnp.zeros((8, LANES), jnp.float32)
            dxu, dyv, lu, lv = [zero] * 4
            for k in range(K):
                idx, tile = slots(k, d)
                near_u, near_v = with_halo((0, 1), halo, idx, tile, d * K + k)
                we, wn, wl = weights(k, d)
                du, dv = near_u - u, near_v - v
                dxu += we * du
                dyv += wn * dv
                lu += wl * du
                lv += wl * dv
            part[0, d] = part[0, d] + DT * lu
            part[1, d] = part[1, d] + DT * lv
            lsend[s + 1, 1, d : d + 1] = jnp.sum(th * (dxu + dyv), axis=0, keepdims=True)
        vv[s] = area_ref[...] * wet_nodes * lsend[s + 1, 1]

    def list_divergence(s):
        div = lsend[s, 1]
        for side in range(2):
            gsend[s, side, 1:2] = listed_nodes(div, side)

    def shared_terms(s):
        arrived(lrecv.at[s], lsem, s)
        arrived(grecv.at[s], gsem, s)
        div, mass = lsend[s, 1], jnp.zeros((8, LANES), jnp.float32)
        for d in range(1, n_level):
            mass = mass + jnp.where(g >= d, lrecv[s, d - 1, 0], 0.0)
            div = div + lrecv[s, d - 1, 1]
        new_eta = eta[...] - DT * wet_nodes * div
        eta[...] = new_eta
        own = new_eta + BUOYANCY * mass
        q[0:8] = own
        for side in range(2):
            row = slice(side, side + 1)
            m = jnp.zeros((1, LANES), jnp.float32)
            h = grecv[s, side, 0, 1:2]
            for d in range(1, n_level):
                m = m + jnp.where(g >= d, grecv[s, side, d, 0:1], 0.0)
                h = h + grecv[s, side, d, 1:2]
            e = etah[row] - DT * srecv[side, 1:2] * h
            etah[row] = e
            q[8 + side : 9 + side] = e + BUOYANCY * m
        dx = jnp.zeros((8, LANES), jnp.float32)
        dy = dx
        rows = [wide(q[t : t + 1]) for t in range(TILES + 2)]
        for k in range(K):
            slot = nbc[k]
            idx, tile = slot & (LANES - 1), slot >> 7
            n = lane_gather(rows[0], idx)
            for t in range(1, TILES + 2):
                n = jnp.where(tile == t, lane_gather(rows[t], idx), n)
            diff = n - own
            dx = dx + wts[0, k] * diff
            dy = dy + wts[1, k] * diff
        dq[0] = DT * dx
        dq[1] = DT * dy
        for d in range(TILES):
            wet = level_id < wide(bot_ref[d : d + 1])
            for c in range(2):
                x[c, d] = jnp.where(wet, part[c, d] - wide(dq[c, d : d + 1]), 0.0)

    def step(s, _):
        par = lax.rem(s, 2)
        gather_own(par)
        density_terms(s, par)
        list_density(s + 1, 1 - par)
        send_density(s + 1)

        @pl.when(s == 0)
        def _():
            pass_token(1)
            arrived(srecv, ssem, 0)
            etah[...] = srecv[:, 0]

        @pl.when(s == 1)
        def _():
            pass_token(3)

        velocity_terms(s)
        list_divergence(s + 1)
        send_sums(s + 1)
        shared_terms(s)
        list_velocity(s + 1)
        send_velocity(s + 1)
        send_level(s + 1)

        @pl.when(s == 0)
        def _():
            pass_token(2)

        @pl.when(s == 1)
        def _():
            pass_token(4)

        return 0

    lax.fori_loop(0, STEPS - 1, step, 0)
    last = STEPS - 1
    par = last % 2
    gather_own(par)
    density_terms(last, par)
    for d in range(TILES):
        rho_out[:, d * LANES : (d + 1) * LANES] = r[1 - par, d]
    lsend[STEPS, 0] = jnp.zeros((8, LANES), jnp.float32)
    velocity_terms(last)

    sums = jnp.zeros((8, LANES), jnp.float32)
    terms = [vv[s] for s in range(STEPS)] + [area_ref[...] * wet_nodes * (1.0 / n_level)]
    for j, term in enumerate(terms):
        sums = jnp.where(sub == j, wide(jnp.sum(term, axis=0, keepdims=True)), sums)
    sums = jnp.broadcast_to(jnp.sum(sums, axis=1, keepdims=True), (8, LANES))
    row = jnp.sum(jnp.where(sub == lane, sums, 0.0), axis=0, keepdims=True)
    zsend[...] = row
    pl.semaphore_wait(tok.at[4], 2)
    for d in range(1, n_z):
        copy(zsend, zrecv.at[d - 1], zsem, 0, z_peer(d), g).start()
    send_level(STEPS)

    shared_terms(last)
    for d in range(TILES):
        for c in range(2):
            vel_out[c, :, d * LANES : (d + 1) * LANES] = x[c, d]
    arrived(lrecv.at[STEPS], lsem, STEPS)
    div = lsend[STEPS, 1]
    for d in range(1, n_level):
        div = div + lrecv[STEPS, d - 1, 1]
    eta[...] = eta[...] - DT * wet_nodes * div

    arrived(zrecv, zsem, 0)
    for d in range(1, n_z):
        row = row + zrecv[d - 1]
    xsend[...] = row
    for i, (a, b) in enumerate(plane):
        copy(xsend, xrecv.at[i], zsem, 1, x_peers[a], level_peers[b]).start()
    arrived(xrecv, zsem, 1)
    for i in range(len(plane)):
        row = row + xrecv[i]
    lane_row = lane[0:1]
    total = jnp.sum(jnp.where(lane_row == STEPS, row, 0.0), axis=1, keepdims=True)
    drifts = jnp.where(lane_row < STEPS, row / total, 0.0)
    drift_out[...] = drifts
    eta_out[...] = eta[...] + DT * jnp.sum(drifts, axis=1, keepdims=True)

    for s in range(STEPS + 1):
        left(lrecv.at[s], lsem, s)
    for s in range(STEPS):
        left(usend.at[s], usem, s)
        left(rsend.at[s], rsem, s)
        left(grecv.at[s], gsem, s)
    left(ssend, ssem, 0)
    left(zrecv, zsem, 0)
    left(xrecv, zsem, 1)


def finish(vel, rho, eta, drift, vel_out, rho_out, eta_out, drift_out, sem):
    copies = [
        pltpu.make_async_copy(a, b, sem.at[i])
        for i, (a, b) in enumerate(((vel, vel_out), (rho, rho_out), (eta, eta_out)))
    ]
    for c in copies:
        c.start()
    drift_out[...] = drift[0, :STEPS]
    for c in copies:
        c.wait()


def solution(mesh):
    n_space, n_level = mesh.shape["space"], mesh.shape["level"]

    def local(
        velocity,
        density,
        elevation,
        grad_weights,
        lap_weights,
        coriolis,
        node_area,
        thickness,
        send_list,
        neighbours,
        bottom,
    ):
        f32, i32 = jnp.float32, jnp.int32
        compact = (TILES, LANES)
        vmem = pl.BlockSpec(memory_space=pltpu.VMEM)
        dma = pltpu.SemaphoreType.DMA
        peers = n_level - 1
        n_z = n_space // X_CHIPS
        row = (1, LANES)
        inputs = [
            pltpu.VMEM(velocity.shape, f32),
            pltpu.VMEM(density.shape, f32),
            pltpu.VMEM(compact, f32),
            pltpu.VMEM((K, 2, TILES * LANES), f32),
            pltpu.VMEM(lap_weights.shape, f32),
            pltpu.VMEM(compact, f32),
            pltpu.VMEM(compact, f32),
            pltpu.SMEM(thickness.shape, f32),
            pltpu.VMEM(send_list.shape, i32),
            pltpu.VMEM(neighbours.shape, i32),
            pltpu.VMEM(compact, i32),
            dma((11,)),
            pltpu.VMEM((K, 8, LANES), i32),
        ]
        shapes = [
            (3, K, 8, LANES),
            (2, 8, 8, LANES),
            (2, 8, 8, LANES),
            (8, 8, LANES),
            (2, 8, 8, LANES),
            (4, 48, 8, LANES),
            (16, LANES),
            (2, 8, LANES),
            (8, LANES),
            (2, LANES),
            (STEPS, 8, LANES),
            (STEPS + 1, 2, 8, LANES),
            (STEPS + 1, peers, 2, 8, LANES),
            (STEPS, 2, 2, 8, LANES),
            (STEPS, 2, 2, 8, LANES),
            (STEPS, 2, 8, LANES),
            (STEPS, 2, 8, LANES),
            (STEPS, 2, 2, LANES),
            (STEPS, 2, n_level, 2, LANES),
            (2, 2, LANES),
            (2, 2, LANES),
            row,
            (n_z - 1, *row),
            row,
            (X_CHIPS * n_level - 1, *row),
        ]

        def body(*refs):
            kernel(n_space, n_level, *refs)

        vel, rho, eta, drift = pl.pallas_call(
            body,
            out_shape=(
                pltpu.VMEM(velocity.shape, f32),
                pltpu.VMEM(density.shape, f32),
                pltpu.VMEM(compact, f32),
                pltpu.VMEM((1, LANES), f32),
            ),
            in_specs=[pl.BlockSpec(memory_space=pl.ANY)] * 11,
            out_specs=(vmem,) * 4,
            scratch_shapes=inputs
            + [pltpu.VMEM(shape, f32) for shape in shapes]
            + [
                dma((2, 5)),
                dma((2, 4)),
                dma((2, 4)),
                dma((2, 4)),
                dma((2, 1)),
                dma((2, 2)),
                pltpu.SemaphoreType.REGULAR((5,)),
            ],
            compiler_params=pltpu.CompilerParams(collective_id=0, has_side_effects=True),
        )(
            velocity,
            density,
            elevation.reshape(compact),
            jnp.swapaxes(grad_weights, 0, 1),
            lap_weights,
            coriolis.reshape(compact),
            node_area.reshape(compact),
            thickness,
            send_list,
            neighbours,
            bottom.reshape(compact),
        )
        results = [pltpu.with_memory_space_constraint(a, pltpu.VMEM) for a in (vel, rho, eta, drift)]
        vel, rho, eta, drift = pl.pallas_call(
            finish,
            out_shape=(
                jax.ShapeDtypeStruct(velocity.shape, f32),
                jax.ShapeDtypeStruct(density.shape, f32),
                jax.ShapeDtypeStruct(compact, f32),
                jax.ShapeDtypeStruct((STEPS,), f32),
            ),
            in_specs=[vmem] * 4,
            out_specs=(pl.BlockSpec(memory_space=pl.ANY),) * 3 + (vmem,),
            scratch_shapes=[dma((3,))],
        )(*results)
        return vel, rho, eta.reshape(elevation.shape), drift

    return jax.shard_map(
        local,
        mesh=mesh,
        in_specs=(
            P(None, "level", "space"),
            P("level", "space"),
            P("space"),
            P(None, None, "space"),
            P(None, "space"),
            P("space"),
            P("space"),
            P("level"),
            P("space", None),
            P(None, "space"),
            P("space"),
        ),
        out_specs=(P(None, "level", "space"), P("level", "space"), P("space"), P()),
        check_vma=False,
    )
```

```python
import jax
import jax.numpy as jnp
from jax import lax
from jax.experimental import pallas as pl
from jax.experimental.pallas import tpu as pltpu
from jax.sharding import PartitionSpec as P

MESH = pl.DeviceIdType.MESH
STEPS = 4
K = 6
TILES = 8
LANES = 128
X_CHIPS = 4
DT = 0.1
BUOYANCY = 0.5
DRAG = 0.5

_LANE_GATHER = lax.GatherDimensionNumbers(
    offset_dims=(),
    collapsed_slice_dims=(1,),
    start_index_map=(1,),
    operand_batching_dims=(0,),
    start_indices_batching_dims=(0,),
)


def lane_gather(x, idx):
    return lax.gather(
        x, idx[..., None], _LANE_GATHER, (1, 1), mode=lax.GatherScatterMode.PROMISE_IN_BOUNDS
    )


def wide(row):
    return jnp.broadcast_to(row, (8, LANES))


def kernel(
    n_space,
    n_level,
    vel_hbm,
    rho_hbm,
    eta_hbm,
    grad_hbm,
    lap_hbm,
    cor_hbm,
    area_hbm,
    thick_hbm,
    send_hbm,
    nb_hbm,
    bot_hbm,
    vel_out,
    rho_out,
    eta_out,
    drift_out,
    vel_ref,
    rho_ref,
    eta_ref,
    grad_ref,
    lap_ref,
    cor_ref,
    area_ref,
    thick_ref,
    send_ref,
    nb_ref,
    bot_ref,
    isem,
    nbc,
    wts,
    x,
    r,
    part,
    near,
    q,
    dq,
    eta,
    etah,
    vv,
    lsend,
    lrecv,
    usend,
    urecv,
    rsend,
    rrecv,
    gsend,
    grecv,
    ssend,
    srecv,
    zsend,
    zrecv,
    xsend,
    xrecv,
    split,
    coef,
    bsend,
    brecv,
    lsem,
    usem,
    rsem,
    gsem,
    ssem,
    bsem,
    zsem,
    tok,
):
    p = lax.axis_index("space")
    g = lax.axis_index("level")
    n_z = n_space // X_CHIPS
    up = lax.rem(p + 1, n_space)
    down = lax.rem(p + n_space - 1, n_space)
    level_peers = [lax.rem(g + d, n_level) for d in range(n_level)]

    def z_peer(d):
        return lax.rem(p + d * X_CHIPS, n_space)

    px = lax.rem(p, X_CHIPS)
    x_peers = [p - px + lax.rem(px + d, X_CHIPS) for d in range(X_CHIPS)]
    plane = [(a, b) for a in range(X_CHIPS) for b in range(n_level) if a or b]

    inputs = [
        (send_hbm, send_ref),
        (vel_hbm, vel_ref),
        (bot_hbm, bot_ref),
        (rho_hbm, rho_ref),
        (thick_hbm, thick_ref),
        (eta_hbm, eta_ref),
        (nb_hbm, nb_ref),
        (grad_hbm, grad_ref),
        (lap_hbm, lap_ref),
        (cor_hbm, cor_ref),
        (area_hbm, area_ref),
    ]
    loads = [pltpu.make_async_copy(a, b, isem.at[i]) for i, (a, b) in enumerate(inputs)]
    for load in loads:
        load.start()

    barrier = pltpu.get_barrier_semaphore()
    count = 0

    def greet(a, b):
        pl.semaphore_signal(barrier, inc=1, device_id=(a, b), device_id_type=MESH)

    for d in range(n_level):
        greet(up, level_peers[d])
        greet(down, level_peers[d])
        count += 2
        if d:
            greet(p, level_peers[d])
            count += 1

    sub = lax.broadcasted_iota(jnp.int32, (8, LANES), 0)
    lane = lax.broadcasted_iota(jnp.int32, (8, LANES), 1)
    level_id = sub + g * 8
    for load in loads[:5]:
        load.wait()
    th = jnp.zeros((8, LANES), jnp.float32)
    for l in range(8):
        th = jnp.where(sub == l, thick_ref[l], th)
    send_idx = [send_ref[:, side * LANES : (side + 1) * LANES] for side in range(2)]
    send_lane = [wide(i & (LANES - 1)) for i in send_idx]
    send_tile = [wide(i >> 7) for i in send_idx]

    def listed_levels(tiles, side):
        out = lane_gather(tiles[0], send_lane[side])
        for t in range(1, TILES):
            out = jnp.where(send_tile[side] == t, lane_gather(tiles[t], send_lane[side]), out)
        return out

    def listed_nodes(compact, side):
        got = lane_gather(compact, send_lane[side])
        return jnp.sum(jnp.where(send_tile[side] == sub, got, 0.0), axis=0, keepdims=True)

    def column(density):
        weighted = density * th
        total = weighted
        for shift in (1, 2, 4):
            total = total + jnp.where(sub >= shift, pltpu.roll(total, shift, 0), 0.0)
        return BUOYANCY * (total - 0.5 * weighted)

    def copy(src, dst, sems, i, a, b):
        return pltpu.make_async_remote_copy(
            src_ref=src,
            dst_ref=dst,
            send_sem=sems.at[0, i],
            recv_sem=sems.at[1, i],
            device_id=(a, b),
            device_id_type=MESH,
        )

    def arrived(buf, sems, i):
        pltpu.make_async_copy(buf, buf, sems.at[1, i]).wait()

    def left(buf, sems, i):
        pltpu.make_async_copy(buf, buf, sems.at[0, i]).wait()

    def send_token(i):
        for d in (2**i, n_space - 2**i):
            there = (lax.rem(p + d, n_space), g)
            pl.semaphore_signal(tok.at[i], inc=1, device_id=there, device_id_type=MESH)

    def pass_token(i):
        pl.semaphore_wait(tok.at[i - 1], 2)
        send_token(i)

    def list_velocity(s):
        for side in range(2):
            for c in range(2):
                usend[s, side, c] = listed_levels([x[c, d] for d in range(TILES)], side)

    def send_velocity(s):
        copy(usend.at[s, 0], urecv.at[s, 1], usem, s, down, g).start()
        copy(usend.at[s, 1], urecv.at[s, 0], usem, s, up, g).start()

    def list_density(s, par):
        tiles = [r[par, d] for d in range(TILES)]
        for side in range(2):
            got = listed_levels(tiles, side)
            rsend[s, side] = got
            gsend[s, side, 0:1] = jnp.sum(got * th, axis=0, keepdims=True)
        for d in range(TILES):
            lsend[s, 0, d : d + 1] = jnp.sum(tiles[d] * th, axis=0, keepdims=True)

    def send_density(s):
        copy(rsend.at[s, 0], rrecv.at[s, 1], rsem, s, down, g).start()
        copy(rsend.at[s, 1], rrecv.at[s, 0], rsem, s, up, g).start()

    def send_sums(s):
        for d in range(n_level):
            copy(gsend.at[s, 0], grecv.at[s, 1, d], gsem, s, down, level_peers[d]).start()
            copy(gsend.at[s, 1], grecv.at[s, 0, d], gsem, s, up, level_peers[d]).start()

    def send_level(s):
        for d in range(1, n_level):
            copy(lsend.at[s], lrecv.at[s, d - 1], lsem, s, p, level_peers[d]).start()

    for d in range(TILES):
        cols = slice(d * LANES, (d + 1) * LANES)
        wet = level_id < wide(bot_ref[d : d + 1])
        for c in range(2):
            x[c, d] = jnp.where(wet, vel_ref[c, :, cols], 0.0)
        r[0, d] = rho_ref[:, cols]
    list_velocity(0)
    list_density(0, 0)
    lsend[0, 1] = jnp.zeros((8, LANES), jnp.float32)
    for side in range(2):
        gsend[0, side, 1:2] = jnp.zeros((1, LANES), jnp.float32)
    loads[5].wait()
    wet_nodes = (bot_ref[...] > 0).astype(jnp.float32)
    eta[...] = eta_ref[...]
    for side in range(2):
        ssend[side, 0:1] = listed_nodes(eta_ref[...], side)
        ssend[side, 1:2] = listed_nodes(wet_nodes, side)

    pl.semaphore_wait(barrier, count)
    send_velocity(0)
    send_sums(0)
    send_density(0)
    send_level(0)
    copy(ssend.at[0], srecv.at[1], ssem, 0, down, g).start()
    copy(ssend.at[1], srecv.at[0], ssem, 0, up, g).start()
    send_token(0)

    for load in loads[6:]:
        load.wait()
    for k in range(K):
        for d in range(TILES):
            cols = slice(d * LANES, (d + 1) * LANES)
            row = slice(d, d + 1)
            nbc[k, row] = nb_ref[k : k + 1, cols]
            wts[0, k, row] = grad_ref[k, 0:1, cols]
            wts[1, k, row] = grad_ref[k, 1:2, cols]
            wts[2, k, row] = lap_ref[k : k + 1, cols]
        tile = nbc[k] >> 7
        below = jnp.where(p > 0, 1.0, 0.0)
        above = jnp.where(p < n_space - 1, 1.0, 0.0)
        valid = jnp.where(tile == TILES, below, jnp.where(tile == TILES + 1, above, 1.0))
        for j in range(3):
            wts[j, k] = wts[j, k] * valid

    def slots(k, d):
        row = wide(nbc[k, d : d + 1])
        return row & (LANES - 1), row >> 7

    def weights(k, d):
        return [wide(wts[j, k, d : d + 1]) for j in range(3)]

    def gather_own(par):
        for d in range(TILES):
            for k in range(K):
                idx, tile = slots(k, d)
                outs = [None] * 3
                for t in range(TILES):
                    hit = tile == t
                    for f, a in enumerate((x[0, t], x[1, t], r[par, t])):
                        got = lane_gather(a, idx)
                        outs[f] = jnp.where(hit, got, outs[f]) if t else got
                for f in range(3):
                    near[f, d * K + k] = outs[f]

    def with_halo(fields, halo, idx, tile, at):
        outs = [near[f, at] for f in fields]
        for side in range(2):
            hit = tile == TILES + side
            outs = [jnp.where(hit, lane_gather(a, idx), o) for a, o in zip(halo[side], outs)]
        return outs

    def density_terms(s, par):
        arrived(rrecv.at[s], rsem, s)
        halo = [(rrecv[s, side],) for side in range(2)]
        for d in range(TILES):
            own = r[par, d]
            zero = jnp.zeros((8, LANES), jnp.float32)
            lr, dxr, dyr = [zero] * 3
            for k in range(K):
                idx, tile = slots(k, d)
                (near_r,) = with_halo((2,), halo, idx, tile, d * K + k)
                dr = near_r - own
                we, wn, wl = weights(k, d)
                lr += wl * dr
                dxr += we * dr
                dyr += wn * dr
            u, v = x[0, d], x[1, d]
            cor = wide(cor_ref[d : d + 1])
            drag = jnp.where(level_id == wide(bot_ref[d : d + 1]) - 1, DRAG, 0.0)
            part[0, d] = u + DT * (cor * v - column(dxr) - drag * u)
            part[1, d] = v - DT * (cor * u + column(dyr) + drag * v)
            r[1 - par, d] = own + DT * (lr - u * dxr - v * dyr)

    def velocity_terms(s):
        arrived(urecv.at[s], usem, s)
        halo = [[urecv[s, side, c] for c in range(2)] for side in range(2)]
        for d in range(TILES):
            u, v = x[0, d], x[1, d]
            zero = jnp.zeros((8, LANES), jnp.float32)
            dxu, dyv, lu, lv = [zero] * 4
            for k in range(K):
                idx, tile = slots(k, d)
                near_u, near_v = with_halo((0, 1), halo, idx, tile, d * K + k)
                we, wn, wl = weights(k, d)
                du, dv = near_u - u, near_v - v
                dxu += we * du
                dyv += wn * dv
                lu += wl * du
                lv += wl * dv
            part[0, d] = part[0, d] + DT * lu
            part[1, d] = part[1, d] + DT * lv
            lsend[s + 1, 1, d : d + 1] = jnp.sum(th * (dxu + dyv), axis=0, keepdims=True)
        vv[s] = area_ref[...] * wet_nodes * lsend[s + 1, 1]

    def list_divergence(s):
        div = lsend[s, 1]
        for side in range(2):
            gsend[s, side, 1:2] = listed_nodes(div, side)

    def shared_terms(s):
        arrived(lrecv.at[s], lsem, s)
        arrived(grecv.at[s], gsem, s)
        div, mass = lsend[s, 1], jnp.zeros((8, LANES), jnp.float32)
        for d in range(1, n_level):
            mass = mass + jnp.where(g >= d, lrecv[s, d - 1, 0], 0.0)
            div = div + lrecv[s, d - 1, 1]
        new_eta = eta[...] - DT * wet_nodes * div
        eta[...] = new_eta
        own = new_eta + BUOYANCY * mass
        q[0:8] = own
        for side in range(2):
            row = slice(side, side + 1)
            m = jnp.zeros((1, LANES), jnp.float32)
            h = grecv[s, side, 0, 1:2]
            for d in range(1, n_level):
                m = m + jnp.where(g >= d, grecv[s, side, d, 0:1], 0.0)
                h = h + grecv[s, side, d, 1:2]
            e = etah[row] - DT * srecv[side, 1:2] * h
            etah[row] = e
            q[8 + side : 9 + side] = e + BUOYANCY * m
        dx = jnp.zeros((8, LANES), jnp.float32)
        dy = dx
        rows = [wide(q[t : t + 1]) for t in range(TILES + 2)]
        for k in range(K):
            slot = nbc[k]
            idx, tile = slot & (LANES - 1), slot >> 7
            n = lane_gather(rows[0], idx)
            for t in range(1, TILES + 2):
                n = jnp.where(tile == t, lane_gather(rows[t], idx), n)
            diff = n - own
            dx = dx + wts[0, k] * diff
            dy = dy + wts[1, k] * diff
        dq[0] = DT * dx
        dq[1] = DT * dy
        for d in range(TILES):
            wet = level_id < wide(bot_ref[d : d + 1])
            for c in range(2):
                x[c, d] = jnp.where(wet, part[c, d] - wide(dq[c, d : d + 1]), 0.0)

    def drift_weights():
        area = area_ref[...] * wet_nodes
        own = [jnp.zeros((8, LANES), jnp.float32)] * 2
        for k in range(K):
            for j in range(2):
                term = area * wts[j, k]
                own[j] = own[j] + term
                for i in range(3):
                    short = term.astype(jnp.bfloat16).astype(jnp.float32)
                    split[i, j, k] = short
                    term = term - short
        target = jnp.where(sub < 2, sub + TILES, jnp.where(sub < 4, sub + TILES - 2, -1))
        slot_lane = lax.broadcasted_iota(jnp.int32, (LANES, LANES), 0)
        total = jnp.zeros((72, LANES), jnp.float32)
        for k in range(K):
            for d in range(0, TILES, 2):
                left_side, right_side = [], []
                for e in (d, d + 1):
                    row = nbc[k, e : e + 1]
                    tile = wide(row >> 7)
                    hit, far = tile == sub, tile == target
                    pieces = []
                    for i in range(3):
                        we, wn = [wide(split[i, j, k, e : e + 1]) for j in range(2)]
                        pieces.append(jnp.where(hit, we, 0.0))
                        pieces.append(jnp.where(hit, wn, 0.0))
                        pieces.append(jnp.where(far, jnp.where(sub < 2, we, wn), 0.0))
                    left_side.append(jnp.concatenate(pieces, axis=0))
                    same = jnp.broadcast_to(row & (LANES - 1), (LANES, LANES)) == slot_lane
                    right_side.append(jnp.where(same, 1.0, 0.0))
                total = total + lax.dot_general(
                    jnp.concatenate(left_side, axis=1).astype(jnp.bfloat16),
                    jnp.concatenate(right_side, axis=1).astype(jnp.bfloat16),
                    (((1,), (1,)), ((), ())),
                    preferred_element_type=jnp.float32,
                )
        total = total[0:24] + total[24:48] + total[48:72]
        for j in range(2):
            coef[j] = total[8 * j : 8 * j + 8] - own[j]
            for side in range(2):
                bsend[side, j : j + 1] = total[16 + 2 * j + side : 17 + 2 * j + side]
        copy(bsend.at[0], brecv.at[1], bsem, 0, down, g).start()
        copy(bsend.at[1], brecv.at[0], bsem, 0, up, g).start()

    def early_drift():
        arrived(brecv, bsem, 0)
        total = jnp.zeros((8, LANES), jnp.float32)
        for j in range(2):
            for d in range(TILES):
                total = total + wide(coef[j, d : d + 1]) * x[j, d]
            for side in range(2):
                total = total + wide(brecv[side, j : j + 1]) * usend[STEPS - 1, side, j]
        return total * th

    def step(s, _):
        par = lax.rem(s, 2)
        @pl.when(s == 1)
        def _():
            pass_token(2)
            drift_weights()

        @pl.when(s == 2)
        def _():
            pass_token(4)

        gather_own(par)
        density_terms(s, par)
        list_density(s + 1, 1 - par)
        send_density(s + 1)

        @pl.when(s == 0)
        def _():
            pass_token(1)
            arrived(srecv, ssem, 0)
            etah[...] = srecv[:, 0]

        @pl.when(s == 1)
        def _():
            pass_token(3)

        velocity_terms(s)
        list_divergence(s + 1)
        send_sums(s + 1)
        shared_terms(s)
        list_velocity(s + 1)
        send_velocity(s + 1)
        send_level(s + 1)
        return 0

    lax.fori_loop(0, STEPS - 1, step, 0)
    last = STEPS - 1
    par = last % 2

    sums = jnp.zeros((8, LANES), jnp.float32)
    terms = [vv[s] for s in range(last)]
    terms += [early_drift(), area_ref[...] * wet_nodes * (1.0 / n_level)]
    for j, term in enumerate(terms):
        sums = jnp.where(sub == j, wide(jnp.sum(term, axis=0, keepdims=True)), sums)
    sums = jnp.broadcast_to(jnp.sum(sums, axis=1, keepdims=True), (8, LANES))
    row = jnp.sum(jnp.where(sub == lane, sums, 0.0), axis=0, keepdims=True)
    zsend[...] = row
    pl.semaphore_wait(tok.at[4], 2)
    for d in range(1, n_z):
        copy(zsend, zrecv.at[d - 1], zsem, 0, z_peer(d), g).start()

    gather_own(par)
    density_terms(last, par)
    for d in range(TILES):
        rho_out[:, d * LANES : (d + 1) * LANES] = r[1 - par, d]
    lsend[STEPS, 0] = jnp.zeros((8, LANES), jnp.float32)
    velocity_terms(last)
    send_level(STEPS)
    shared_terms(last)
    for d in range(TILES):
        for c in range(2):
            vel_out[c, :, d * LANES : (d + 1) * LANES] = x[c, d]

    arrived(zrecv, zsem, 0)
    for d in range(1, n_z):
        row = row + zrecv[d - 1]
    xsend[...] = row
    for i, (a, b) in enumerate(plane):
        copy(xsend, xrecv.at[i], zsem, 1, x_peers[a], level_peers[b]).start()

    arrived(lrecv.at[STEPS], lsem, STEPS)
    div = lsend[STEPS, 1]
    for d in range(1, n_level):
        div = div + lrecv[STEPS, d - 1, 1]
    eta[...] = eta[...] - DT * wet_nodes * div

    arrived(xrecv, zsem, 1)
    for i in range(len(plane)):
        row = row + xrecv[i]
    lane_row = lane[0:1]
    total = jnp.sum(jnp.where(lane_row == STEPS, row, 0.0), axis=1, keepdims=True)
    drifts = jnp.where(lane_row < STEPS, row / total, 0.0)
    drift_out[...] = drifts
    eta_out[...] = eta[...] + DT * jnp.sum(drifts, axis=1, keepdims=True)

    for s in range(STEPS + 1):
        left(lrecv.at[s], lsem, s)
    for s in range(STEPS):
        left(usend.at[s], usem, s)
        left(rsend.at[s], rsem, s)
        left(grecv.at[s], gsem, s)
    left(ssend, ssem, 0)
    left(bsend, bsem, 0)
    left(zrecv, zsem, 0)
    left(xrecv, zsem, 1)


def finish(vel, rho, eta, drift, vel_out, rho_out, eta_out, drift_out, sem):
    copies = [
        pltpu.make_async_copy(a, b, sem.at[i])
        for i, (a, b) in enumerate(((vel, vel_out), (rho, rho_out), (eta, eta_out)))
    ]
    for c in copies:
        c.start()
    drift_out[...] = drift[0, :STEPS]
    for c in copies:
        c.wait()


def solution(mesh):
    n_space, n_level = mesh.shape["space"], mesh.shape["level"]

    def local(
        velocity,
        density,
        elevation,
        grad_weights,
        lap_weights,
        coriolis,
        node_area,
        thickness,
        send_list,
        neighbours,
        bottom,
    ):
        f32, i32 = jnp.float32, jnp.int32
        compact = (TILES, LANES)
        vmem = pl.BlockSpec(memory_space=pltpu.VMEM)
        dma = pltpu.SemaphoreType.DMA
        peers = n_level - 1
        n_z = n_space // X_CHIPS
        row = (1, LANES)
        inputs = [
            pltpu.VMEM(velocity.shape, f32),
            pltpu.VMEM(density.shape, f32),
            pltpu.VMEM(compact, f32),
            pltpu.VMEM((K, 2, TILES * LANES), f32),
            pltpu.VMEM(lap_weights.shape, f32),
            pltpu.VMEM(compact, f32),
            pltpu.VMEM(compact, f32),
            pltpu.SMEM(thickness.shape, f32),
            pltpu.VMEM(send_list.shape, i32),
            pltpu.VMEM(neighbours.shape, i32),
            pltpu.VMEM(compact, i32),
            dma((11,)),
            pltpu.VMEM((K, 8, LANES), i32),
        ]
        shapes = [
            (3, K, 8, LANES),
            (2, 8, 8, LANES),
            (2, 8, 8, LANES),
            (2, 8, 8, LANES),
            (3, 48, 8, LANES),
            (16, LANES),
            (2, 8, LANES),
            (8, LANES),
            (2, LANES),
            (STEPS, 8, LANES),
            (STEPS + 1, 2, 8, LANES),
            (STEPS + 1, peers, 2, 8, LANES),
            (STEPS, 2, 2, 8, LANES),
            (STEPS, 2, 2, 8, LANES),
            (STEPS, 2, 8, LANES),
            (STEPS, 2, 8, LANES),
            (STEPS, 2, 2, LANES),
            (STEPS, 2, n_level, 2, LANES),
            (2, 2, LANES),
            (2, 2, LANES),
            row,
            (n_z - 1, *row),
            row,
            (X_CHIPS * n_level - 1, *row),
            (3, 2, K, 8, LANES),
            (2, 8, LANES),
            (2, 2, LANES),
            (2, 2, LANES),
        ]

        def body(*refs):
            kernel(n_space, n_level, *refs)

        vel, rho, eta, drift = pl.pallas_call(
            body,
            out_shape=(
                pltpu.VMEM(velocity.shape, f32),
                pltpu.VMEM(density.shape, f32),
                pltpu.VMEM(compact, f32),
                pltpu.VMEM((1, LANES), f32),
            ),
            in_specs=[pl.BlockSpec(memory_space=pl.ANY)] * 11,
            out_specs=(vmem,) * 4,
            scratch_shapes=inputs
            + [pltpu.VMEM(shape, f32) for shape in shapes]
            + [
                dma((2, 5)),
                dma((2, 4)),
                dma((2, 4)),
                dma((2, 4)),
                dma((2, 1)),
                dma((2, 1)),
                dma((2, 2)),
                pltpu.SemaphoreType.REGULAR((5,)),
            ],
            compiler_params=pltpu.CompilerParams(collective_id=0, has_side_effects=True),
        )(
            velocity,
            density,
            elevation.reshape(compact),
            jnp.swapaxes(grad_weights, 0, 1),
            lap_weights,
            coriolis.reshape(compact),
            node_area.reshape(compact),
            thickness,
            send_list,
            neighbours,
            bottom.reshape(compact),
        )
        results = [pltpu.with_memory_space_constraint(a, pltpu.VMEM) for a in (vel, rho, eta, drift)]
        vel, rho, eta, drift = pl.pallas_call(
            finish,
            out_shape=(
                jax.ShapeDtypeStruct(velocity.shape, f32),
                jax.ShapeDtypeStruct(density.shape, f32),
                jax.ShapeDtypeStruct(compact, f32),
                jax.ShapeDtypeStruct((STEPS,), f32),
            ),
            in_specs=[vmem] * 4,
            out_specs=(pl.BlockSpec(memory_space=pl.ANY),) * 3 + (vmem,),
            scratch_shapes=[dma((3,))],
        )(*results)
        return vel, rho, eta.reshape(elevation.shape), drift

    return jax.shard_map(
        local,
        mesh=mesh,
        in_specs=(
            P(None, "level", "space"),
            P("level", "space"),
            P("space"),
            P(None, None, "space"),
            P(None, "space"),
            P("space"),
            P("space"),
            P("level"),
            P("space", None),
            P(None, "space"),
            P("space"),
        ),
        out_specs=(P(None, "level", "space"), P("level", "space"), P("space"), P()),
        check_vma=False,
    )
```

```python
import jax
import jax.numpy as jnp
from jax import lax
from jax.experimental import pallas as pl
from jax.experimental.pallas import tpu as pltpu
from jax.sharding import PartitionSpec as P

MESH = pl.DeviceIdType.MESH
STEPS = 4
K = 6
TILES = 8
LANES = 128
X_CHIPS = 4
DT = 0.1
BUOYANCY = 0.5
DRAG = 0.5

_LANE_GATHER = lax.GatherDimensionNumbers(
    offset_dims=(),
    collapsed_slice_dims=(1,),
    start_index_map=(1,),
    operand_batching_dims=(0,),
    start_indices_batching_dims=(0,),
)


def lane_gather(x, idx):
    return lax.gather(
        x, idx[..., None], _LANE_GATHER, (1, 1), mode=lax.GatherScatterMode.PROMISE_IN_BOUNDS
    )


def far_first(count, start=1):
    return sorted(range(start, count), key=lambda d: -min(d, count - d))


def wide(row):
    return jnp.broadcast_to(row, (8, LANES))


def kernel(
    n_space,
    n_level,
    vel_hbm,
    rho_hbm,
    eta_hbm,
    grad_hbm,
    lap_hbm,
    cor_hbm,
    area_hbm,
    thick_hbm,
    send_hbm,
    nb_hbm,
    bot_hbm,
    vel_out,
    rho_out,
    eta_out,
    drift_out,
    vel_ref,
    rho_ref,
    eta_ref,
    grad_ref,
    lap_ref,
    cor_ref,
    area_ref,
    thick_ref,
    send_ref,
    nb_ref,
    bot_ref,
    isem,
    nbc,
    wts,
    x,
    r,
    part,
    near,
    q,
    dq,
    eta,
    etah,
    vv,
    lsend,
    lrecv,
    usend,
    urecv,
    rsend,
    rrecv,
    gsend,
    grecv,
    ssend,
    srecv,
    zsend,
    zrecv,
    xsend,
    xrecv,
    split,
    coef,
    bsend,
    brecv,
    lsem,
    usem,
    rsem,
    gsem,
    ssem,
    bsem,
    zsem,
    tok,
):
    p = lax.axis_index("space")
    g = lax.axis_index("level")
    n_z = n_space // X_CHIPS
    up = lax.rem(p + 1, n_space)
    down = lax.rem(p + n_space - 1, n_space)
    level_peers = [lax.rem(g + d, n_level) for d in range(n_level)]

    def z_peer(d):
        return lax.rem(p + d * X_CHIPS, n_space)

    px = lax.rem(p, X_CHIPS)
    x_peers = [p - px + lax.rem(px + d, X_CHIPS) for d in range(X_CHIPS)]
    plane = [(a, b) for a in range(X_CHIPS) for b in range(n_level) if a or b]
    plane.sort(key=lambda ab: -2 * min(ab[0], X_CHIPS - ab[0]) - min(ab[1], n_level - ab[1]))

    barrier = pltpu.get_barrier_semaphore()
    count = 0

    def greet(a, b):
        pl.semaphore_signal(barrier, inc=1, device_id=(a, b), device_id_type=MESH)

    for d in far_first(n_level, 0):
        greet(up, level_peers[d])
        greet(down, level_peers[d])
        count += 2
        if d:
            greet(p, level_peers[d])
            count += 1

    inputs = [
        (send_hbm, send_ref),
        (vel_hbm, vel_ref),
        (bot_hbm, bot_ref),
        (rho_hbm, rho_ref),
        (thick_hbm, thick_ref),
        (eta_hbm, eta_ref),
        (nb_hbm, nb_ref),
        (grad_hbm, grad_ref),
        (lap_hbm, lap_ref),
        (cor_hbm, cor_ref),
        (area_hbm, area_ref),
    ]
    loads = [pltpu.make_async_copy(a, b, isem.at[i]) for i, (a, b) in enumerate(inputs)]
    for load in loads:
        load.start()

    sub = lax.broadcasted_iota(jnp.int32, (8, LANES), 0)
    lane = lax.broadcasted_iota(jnp.int32, (8, LANES), 1)
    level_id = sub + g * 8
    for load in loads[:5]:
        load.wait()
    th = jnp.zeros((8, LANES), jnp.float32)
    for l in range(8):
        th = jnp.where(sub == l, thick_ref[l], th)
    send_idx = [send_ref[:, side * LANES : (side + 1) * LANES] for side in range(2)]
    send_lane = [wide(i & (LANES - 1)) for i in send_idx]
    send_tile = [wide(i >> 7) for i in send_idx]

    def listed_levels(tiles, side):
        out = lane_gather(tiles[0], send_lane[side])
        for t in range(1, TILES):
            out = jnp.where(send_tile[side] == t, lane_gather(tiles[t], send_lane[side]), out)
        return out

    def listed_nodes(compact, side):
        got = lane_gather(compact, send_lane[side])
        return jnp.sum(jnp.where(send_tile[side] == sub, got, 0.0), axis=0, keepdims=True)

    def column(density):
        weighted = density * th
        total = weighted
        for shift in (1, 2, 4):
            total = total + jnp.where(sub >= shift, pltpu.roll(total, shift, 0), 0.0)
        return BUOYANCY * (total - 0.5 * weighted)

    def copy(src, dst, sems, i, a, b):
        return pltpu.make_async_remote_copy(
            src_ref=src,
            dst_ref=dst,
            send_sem=sems.at[0, i],
            recv_sem=sems.at[1, i],
            device_id=(a, b),
            device_id_type=MESH,
        )

    def arrived(buf, sems, i):
        pltpu.make_async_copy(buf, buf, sems.at[1, i]).wait()

    def left(buf, sems, i):
        pltpu.make_async_copy(buf, buf, sems.at[0, i]).wait()

    def send_token(i):
        for d in (2**i, n_space - 2**i):
            there = (lax.rem(p + d, n_space), g)
            pl.semaphore_signal(tok.at[i], inc=1, device_id=there, device_id_type=MESH)

    def pass_token(i):
        pl.semaphore_wait(tok.at[i - 1], 2)
        send_token(i)

    def list_velocity(s):
        for side in range(2):
            for c in range(2):
                usend[s, side, c] = listed_levels([x[c, d] for d in range(TILES)], side)

    def send_velocity(s):
        copy(usend.at[s, 0], urecv.at[s, 1], usem, s, down, g).start()
        copy(usend.at[s, 1], urecv.at[s, 0], usem, s, up, g).start()

    def list_density(s, par):
        tiles = [r[par, d] for d in range(TILES)]
        for side in range(2):
            got = listed_levels(tiles, side)
            rsend[s, side] = got
            gsend[s, side, 0:1] = jnp.sum(got * th, axis=0, keepdims=True)
        for d in range(TILES):
            lsend[s, 0, d : d + 1] = jnp.sum(tiles[d] * th, axis=0, keepdims=True)

    def send_density(s):
        copy(rsend.at[s, 0], rrecv.at[s, 1], rsem, s, down, g).start()
        copy(rsend.at[s, 1], rrecv.at[s, 0], rsem, s, up, g).start()

    def send_sums(s):
        for d in far_first(n_level, 0):
            copy(gsend.at[s, 0], grecv.at[s, 1, d], gsem, s, down, level_peers[d]).start()
            copy(gsend.at[s, 1], grecv.at[s, 0, d], gsem, s, up, level_peers[d]).start()

    def send_level(s):
        for d in far_first(n_level):
            copy(lsend.at[s], lrecv.at[s, d - 1], lsem, s, p, level_peers[d]).start()

    for d in range(TILES):
        cols = slice(d * LANES, (d + 1) * LANES)
        wet = level_id < wide(bot_ref[d : d + 1])
        for c in range(2):
            x[c, d] = jnp.where(wet, vel_ref[c, :, cols], 0.0)
        r[0, d] = rho_ref[:, cols]
    list_velocity(0)
    list_density(0, 0)
    lsend[0, 1] = jnp.zeros((8, LANES), jnp.float32)
    for side in range(2):
        gsend[0, side, 1:2] = jnp.zeros((1, LANES), jnp.float32)
    loads[5].wait()
    wet_nodes = (bot_ref[...] > 0).astype(jnp.float32)
    eta[...] = eta_ref[...]
    for side in range(2):
        ssend[side, 0:1] = listed_nodes(eta_ref[...], side)
        ssend[side, 1:2] = listed_nodes(wet_nodes, side)

    pl.semaphore_wait(barrier, count)
    send_velocity(0)
    send_sums(0)
    send_density(0)
    send_level(0)
    copy(ssend.at[0], srecv.at[1], ssem, 0, down, g).start()
    copy(ssend.at[1], srecv.at[0], ssem, 0, up, g).start()
    send_token(0)

    for load in loads[6:]:
        load.wait()
    for k in range(K):
        for d in range(TILES):
            cols = slice(d * LANES, (d + 1) * LANES)
            row = slice(d, d + 1)
            nbc[k, row] = nb_ref[k : k + 1, cols]
            wts[0, k, row] = grad_ref[k, 0:1, cols]
            wts[1, k, row] = grad_ref[k, 1:2, cols]
            wts[2, k, row] = lap_ref[k : k + 1, cols]
        tile = nbc[k] >> 7
        below = jnp.where(p > 0, 1.0, 0.0)
        above = jnp.where(p < n_space - 1, 1.0, 0.0)
        valid = jnp.where(tile == TILES, below, jnp.where(tile == TILES + 1, above, 1.0))
        for j in range(3):
            wts[j, k] = wts[j, k] * valid

    def slots(k, d):
        row = wide(nbc[k, d : d + 1])
        return row & (LANES - 1), row >> 7

    def weights(k, d):
        return [wide(wts[j, k, d : d + 1]) for j in range(3)]

    def gather_own(par):
        for d in range(TILES):
            for k in range(K):
                idx, tile = slots(k, d)
                outs = [None] * 3
                for t in range(TILES):
                    hit = tile == t
                    for f, a in enumerate((x[0, t], x[1, t], r[par, t])):
                        got = lane_gather(a, idx)
                        outs[f] = jnp.where(hit, got, outs[f]) if t else got
                for f in range(3):
                    near[f, d * K + k] = outs[f]

    def with_halo(fields, halo, idx, tile, at):
        outs = [near[f, at] for f in fields]
        for side in range(2):
            hit = tile == TILES + side
            outs = [jnp.where(hit, lane_gather(a, idx), o) for a, o in zip(halo[side], outs)]
        return outs

    def density_terms(s, par):
        arrived(rrecv.at[s], rsem, s)
        halo = [(rrecv[s, side],) for side in range(2)]
        for d in range(TILES):
            own = r[par, d]
            zero = jnp.zeros((8, LANES), jnp.float32)
            lr, dxr, dyr = [zero] * 3
            for k in range(K):
                idx, tile = slots(k, d)
                (near_r,) = with_halo((2,), halo, idx, tile, d * K + k)
                dr = near_r - own
                we, wn, wl = weights(k, d)
                lr += wl * dr
                dxr += we * dr
                dyr += wn * dr
            u, v = x[0, d], x[1, d]
            cor = wide(cor_ref[d : d + 1])
            drag = jnp.where(level_id == wide(bot_ref[d : d + 1]) - 1, DRAG, 0.0)
            part[0, d] = u + DT * (cor * v - column(dxr) - drag * u)
            part[1, d] = v - DT * (cor * u + column(dyr) + drag * v)
            r[1 - par, d] = own + DT * (lr - u * dxr - v * dyr)

    def velocity_terms(s):
        arrived(urecv.at[s], usem, s)
        halo = [[urecv[s, side, c] for c in range(2)] for side in range(2)]
        for d in range(TILES):
            u, v = x[0, d], x[1, d]
            zero = jnp.zeros((8, LANES), jnp.float32)
            dxu, dyv, lu, lv = [zero] * 4
            for k in range(K):
                idx, tile = slots(k, d)
                near_u, near_v = with_halo((0, 1), halo, idx, tile, d * K + k)
                we, wn, wl = weights(k, d)
                du, dv = near_u - u, near_v - v
                dxu += we * du
                dyv += wn * dv
                lu += wl * du
                lv += wl * dv
            part[0, d] = part[0, d] + DT * lu
            part[1, d] = part[1, d] + DT * lv
            lsend[s + 1, 1, d : d + 1] = jnp.sum(th * (dxu + dyv), axis=0, keepdims=True)
        vv[s] = area_ref[...] * wet_nodes * lsend[s + 1, 1]

    def list_divergence(s):
        div = lsend[s, 1]
        for side in range(2):
            gsend[s, side, 1:2] = listed_nodes(div, side)

    def shared_terms(s):
        arrived(lrecv.at[s], lsem, s)
        arrived(grecv.at[s], gsem, s)
        div, mass = lsend[s, 1], jnp.zeros((8, LANES), jnp.float32)
        for d in range(1, n_level):
            mass = mass + jnp.where(g >= d, lrecv[s, d - 1, 0], 0.0)
            div = div + lrecv[s, d - 1, 1]
        new_eta = eta[...] - DT * wet_nodes * div
        eta[...] = new_eta
        own = new_eta + BUOYANCY * mass
        q[0:8] = own
        for side in range(2):
            row = slice(side, side + 1)
            m = jnp.zeros((1, LANES), jnp.float32)
            h = grecv[s, side, 0, 1:2]
            for d in range(1, n_level):
                m = m + jnp.where(g >= d, grecv[s, side, d, 0:1], 0.0)
                h = h + grecv[s, side, d, 1:2]
            e = etah[row] - DT * srecv[side, 1:2] * h
            etah[row] = e
            q[8 + side : 9 + side] = e + BUOYANCY * m
        dx = jnp.zeros((8, LANES), jnp.float32)
        dy = dx
        rows = [wide(q[t : t + 1]) for t in range(TILES + 2)]
        for k in range(K):
            slot = nbc[k]
            idx, tile = slot & (LANES - 1), slot >> 7
            n = lane_gather(rows[0], idx)
            for t in range(1, TILES + 2):
                n = jnp.where(tile == t, lane_gather(rows[t], idx), n)
            diff = n - own
            dx = dx + wts[0, k] * diff
            dy = dy + wts[1, k] * diff
        dq[0] = DT * dx
        dq[1] = DT * dy
        for d in range(TILES):
            wet = level_id < wide(bot_ref[d : d + 1])
            for c in range(2):
                x[c, d] = jnp.where(wet, part[c, d] - wide(dq[c, d : d + 1]), 0.0)

    def drift_weights():
        area = area_ref[...] * wet_nodes
        own = [jnp.zeros((8, LANES), jnp.float32)] * 2
        for k in range(K):
            for j in range(2):
                term = area * wts[j, k]
                own[j] = own[j] + term
                for i in range(3):
                    short = term.astype(jnp.bfloat16).astype(jnp.float32)
                    split[i, j, k] = short
                    term = term - short
        target = jnp.where(sub < 2, sub + TILES, jnp.where(sub < 4, sub + TILES - 2, -1))
        slot_lane = lax.broadcasted_iota(jnp.int32, (LANES, LANES), 0)
        total = jnp.zeros((72, LANES), jnp.float32)
        for k in range(K):
            for d in range(0, TILES, 2):
                left_side, right_side = [], []
                for e in (d, d + 1):
                    row = nbc[k, e : e + 1]
                    tile = wide(row >> 7)
                    hit, far = tile == sub, tile == target
                    pieces = []
                    for i in range(3):
                        we, wn = [wide(split[i, j, k, e : e + 1]) for j in range(2)]
                        pieces.append(jnp.where(hit, we, 0.0))
                        pieces.append(jnp.where(hit, wn, 0.0))
                        pieces.append(jnp.where(far, jnp.where(sub < 2, we, wn), 0.0))
                    left_side.append(jnp.concatenate(pieces, axis=0))
                    same = jnp.broadcast_to(row & (LANES - 1), (LANES, LANES)) == slot_lane
                    right_side.append(jnp.where(same, 1.0, 0.0))
                total = total + lax.dot_general(
                    jnp.concatenate(left_side, axis=1).astype(jnp.bfloat16),
                    jnp.concatenate(right_side, axis=1).astype(jnp.bfloat16),
                    (((1,), (1,)), ((), ())),
                    preferred_element_type=jnp.float32,
                )
        total = total[0:24] + total[24:48] + total[48:72]
        for j in range(2):
            coef[j] = total[8 * j : 8 * j + 8] - own[j]
            for side in range(2):
                bsend[side, j : j + 1] = total[16 + 2 * j + side : 17 + 2 * j + side]
        copy(bsend.at[0], brecv.at[1], bsem, 0, down, g).start()
        copy(bsend.at[1], brecv.at[0], bsem, 0, up, g).start()

    def early_drift():
        arrived(brecv, bsem, 0)
        total = jnp.zeros((8, LANES), jnp.float32)
        for j in range(2):
            for d in range(TILES):
                total = total + wide(coef[j, d : d + 1]) * x[j, d]
            for side in range(2):
                total = total + wide(brecv[side, j : j + 1]) * usend[STEPS - 1, side, j]
        return total * th

    def step(s, _):
        par = lax.rem(s, 2)
        @pl.when(s == 1)
        def _():
            pass_token(2)
            drift_weights()

        @pl.when(s == 2)
        def _():
            pass_token(4)

        gather_own(par)
        density_terms(s, par)
        list_density(s + 1, 1 - par)
        send_density(s + 1)

        @pl.when(s == 0)
        def _():
            pass_token(1)
            arrived(srecv, ssem, 0)
            etah[...] = srecv[:, 0]

        @pl.when(s == 1)
        def _():
            pass_token(3)

        velocity_terms(s)
        list_divergence(s + 1)
        send_sums(s + 1)
        shared_terms(s)
        list_velocity(s + 1)
        send_velocity(s + 1)
        send_level(s + 1)
        return 0

    lax.fori_loop(0, STEPS - 1, step, 0)
    last = STEPS - 1
    par = last % 2

    sums = jnp.zeros((8, LANES), jnp.float32)
    terms = [vv[s] for s in range(last)]
    terms += [early_drift(), area_ref[...] * wet_nodes * (1.0 / n_level)]
    for j, term in enumerate(terms):
        sums = jnp.where(sub == j, wide(jnp.sum(term, axis=0, keepdims=True)), sums)
    sums = jnp.broadcast_to(jnp.sum(sums, axis=1, keepdims=True), (8, LANES))
    row = jnp.sum(jnp.where(sub == lane, sums, 0.0), axis=0, keepdims=True)
    zsend[...] = row
    pl.semaphore_wait(tok.at[4], 2)
    for d in far_first(n_z):
        copy(zsend, zrecv.at[d - 1], zsem, 0, z_peer(d), g).start()

    gather_own(par)
    density_terms(last, par)
    for d in range(TILES):
        rho_out[:, d * LANES : (d + 1) * LANES] = r[1 - par, d]
    lsend[STEPS, 0] = jnp.zeros((8, LANES), jnp.float32)
    velocity_terms(last)
    send_level(STEPS)
    shared_terms(last)
    for d in range(TILES):
        for c in range(2):
            vel_out[c, :, d * LANES : (d + 1) * LANES] = x[c, d]

    arrived(zrecv, zsem, 0)
    for d in range(1, n_z):
        row = row + zrecv[d - 1]
    xsend[...] = row
    for i, (a, b) in enumerate(plane):
        copy(xsend, xrecv.at[i], zsem, 1, x_peers[a], level_peers[b]).start()

    arrived(lrecv.at[STEPS], lsem, STEPS)
    div = lsend[STEPS, 1]
    for d in range(1, n_level):
        div = div + lrecv[STEPS, d - 1, 1]
    eta[...] = eta[...] - DT * wet_nodes * div

    arrived(xrecv, zsem, 1)
    for i in range(len(plane)):
        row = row + xrecv[i]
    lane_row = lane[0:1]
    total = jnp.sum(jnp.where(lane_row == STEPS, row, 0.0), axis=1, keepdims=True)
    drifts = jnp.where(lane_row < STEPS, row / total, 0.0)
    drift_out[...] = drifts
    eta_out[...] = eta[...] + DT * jnp.sum(drifts, axis=1, keepdims=True)

    for s in range(STEPS + 1):
        left(lrecv.at[s], lsem, s)
    for s in range(STEPS):
        left(usend.at[s], usem, s)
        left(rsend.at[s], rsem, s)
        left(grecv.at[s], gsem, s)
    left(ssend, ssem, 0)
    left(bsend, bsem, 0)
    left(zrecv, zsem, 0)
    left(xrecv, zsem, 1)


def finish(vel, rho, eta, drift, vel_out, rho_out, eta_out, drift_out, sem):
    copies = [
        pltpu.make_async_copy(a, b, sem.at[i])
        for i, (a, b) in enumerate(((vel, vel_out), (rho, rho_out), (eta, eta_out)))
    ]
    for c in copies:
        c.start()
    drift_out[...] = drift[0, :STEPS]
    for c in copies:
        c.wait()


def solution(mesh):
    n_space, n_level = mesh.shape["space"], mesh.shape["level"]

    def local(
        velocity,
        density,
        elevation,
        grad_weights,
        lap_weights,
        coriolis,
        node_area,
        thickness,
        send_list,
        neighbours,
        bottom,
    ):
        f32, i32 = jnp.float32, jnp.int32
        compact = (TILES, LANES)
        vmem = pl.BlockSpec(memory_space=pltpu.VMEM)
        dma = pltpu.SemaphoreType.DMA
        peers = n_level - 1
        n_z = n_space // X_CHIPS
        row = (1, LANES)
        inputs = [
            pltpu.VMEM(velocity.shape, f32),
            pltpu.VMEM(density.shape, f32),
            pltpu.VMEM(compact, f32),
            pltpu.VMEM((K, 2, TILES * LANES), f32),
            pltpu.VMEM(lap_weights.shape, f32),
            pltpu.VMEM(compact, f32),
            pltpu.VMEM(compact, f32),
            pltpu.SMEM(thickness.shape, f32),
            pltpu.VMEM(send_list.shape, i32),
            pltpu.VMEM(neighbours.shape, i32),
            pltpu.VMEM(compact, i32),
            dma((11,)),
            pltpu.VMEM((K, 8, LANES), i32),
        ]
        shapes = [
            (3, K, 8, LANES),
            (2, 8, 8, LANES),
            (2, 8, 8, LANES),
            (2, 8, 8, LANES),
            (3, 48, 8, LANES),
            (16, LANES),
            (2, 8, LANES),
            (8, LANES),
            (2, LANES),
            (STEPS, 8, LANES),
            (STEPS + 1, 2, 8, LANES),
            (STEPS + 1, peers, 2, 8, LANES),
            (STEPS, 2, 2, 8, LANES),
            (STEPS, 2, 2, 8, LANES),
            (STEPS, 2, 8, LANES),
            (STEPS, 2, 8, LANES),
            (STEPS, 2, 2, LANES),
            (STEPS, 2, n_level, 2, LANES),
            (2, 2, LANES),
            (2, 2, LANES),
            row,
            (n_z - 1, *row),
            row,
            (X_CHIPS * n_level - 1, *row),
            (3, 2, K, 8, LANES),
            (2, 8, LANES),
            (2, 2, LANES),
            (2, 2, LANES),
        ]

        def body(*refs):
            kernel(n_space, n_level, *refs)

        vel, rho, eta, drift = pl.pallas_call(
            body,
            out_shape=(
                pltpu.VMEM(velocity.shape, f32),
                pltpu.VMEM(density.shape, f32),
                pltpu.VMEM(compact, f32),
                pltpu.VMEM((1, LANES), f32),
            ),
            in_specs=[pl.BlockSpec(memory_space=pl.ANY)] * 11,
            out_specs=(vmem,) * 4,
            scratch_shapes=inputs
            + [pltpu.VMEM(shape, f32) for shape in shapes]
            + [
                dma((2, 5)),
                dma((2, 4)),
                dma((2, 4)),
                dma((2, 4)),
                dma((2, 1)),
                dma((2, 1)),
                dma((2, 2)),
                pltpu.SemaphoreType.REGULAR((5,)),
            ],
            compiler_params=pltpu.CompilerParams(collective_id=0, has_side_effects=True),
        )(
            velocity,
            density,
            elevation.reshape(compact),
            jnp.swapaxes(grad_weights, 0, 1),
            lap_weights,
            coriolis.reshape(compact),
            node_area.reshape(compact),
            thickness,
            send_list,
            neighbours,
            bottom.reshape(compact),
        )
        results = [pltpu.with_memory_space_constraint(a, pltpu.VMEM) for a in (vel, rho, eta, drift)]
        vel, rho, eta, drift = pl.pallas_call(
            finish,
            out_shape=(
                jax.ShapeDtypeStruct(velocity.shape, f32),
                jax.ShapeDtypeStruct(density.shape, f32),
                jax.ShapeDtypeStruct(compact, f32),
                jax.ShapeDtypeStruct((STEPS,), f32),
            ),
            in_specs=[vmem] * 4,
            out_specs=(pl.BlockSpec(memory_space=pl.ANY),) * 3 + (vmem,),
            scratch_shapes=[dma((3,))],
        )(*results)
        return vel, rho, eta.reshape(elevation.shape), drift

    return jax.shard_map(
        local,
        mesh=mesh,
        in_specs=(
            P(None, "level", "space"),
            P("level", "space"),
            P("space"),
            P(None, None, "space"),
            P(None, "space"),
            P("space"),
            P("space"),
            P("level"),
            P("space", None),
            P(None, "space"),
            P("space"),
        ),
        out_specs=(P(None, "level", "space"), P("level", "space"), P("space"), P()),
        check_vma=False,
    )
```

```python
import jax
import jax.numpy as jnp
from jax import lax
from jax.experimental import pallas as pl
from jax.experimental.pallas import tpu as pltpu
from jax.sharding import PartitionSpec as P

MESH = pl.DeviceIdType.MESH
STEPS = 4
K = 6
TILES = 8
LANES = 128
X_CHIPS = 4
DT = 0.1
BUOYANCY = 0.5
DRAG = 0.5

_LANE_GATHER = lax.GatherDimensionNumbers(
    offset_dims=(),
    collapsed_slice_dims=(1,),
    start_index_map=(1,),
    operand_batching_dims=(0,),
    start_indices_batching_dims=(0,),
)


def lane_gather(x, idx):
    return lax.gather(
        x, idx[..., None], _LANE_GATHER, (1, 1), mode=lax.GatherScatterMode.PROMISE_IN_BOUNDS
    )


def far_first(count, start=1):
    return sorted(range(start, count), key=lambda d: -min(d, count - d))


def wide(row):
    return jnp.broadcast_to(row, (8, LANES))


def kernel(
    n_space,
    n_level,
    vel_hbm,
    rho_hbm,
    eta_hbm,
    grad_hbm,
    lap_hbm,
    cor_hbm,
    area_hbm,
    thick_hbm,
    send_hbm,
    nb_hbm,
    bot_hbm,
    vel_out,
    rho_out,
    eta_out,
    drift_out,
    vel_ref,
    rho_ref,
    eta_ref,
    grad_ref,
    lap_ref,
    cor_ref,
    area_ref,
    thick_ref,
    send_ref,
    nb_ref,
    bot_ref,
    isem,
    nbc,
    wts,
    bots,
    cors,
    x,
    r,
    part,
    near,
    q,
    dq,
    eta,
    etah,
    vv,
    lsend,
    lrecv,
    usend,
    urecv,
    rsend,
    rrecv,
    gsend,
    grecv,
    ssend,
    srecv,
    zsend,
    zrecv,
    xsend,
    xrecv,
    split,
    coef,
    bsend,
    brecv,
    lsem,
    usem,
    rsem,
    gsem,
    ssem,
    bsem,
    zsem,
    tok,
):
    p = lax.axis_index("space")
    g = lax.axis_index("level")
    n_z = n_space // X_CHIPS
    up = lax.rem(p + 1, n_space)
    down = lax.rem(p + n_space - 1, n_space)
    level_peers = [lax.rem(g + d, n_level) for d in range(n_level)]

    def z_peer(d):
        return lax.rem(p + d * X_CHIPS, n_space)

    px = lax.rem(p, X_CHIPS)
    x_peers = [p - px + lax.rem(px + d, X_CHIPS) for d in range(X_CHIPS)]
    plane = [(a, b) for a in range(X_CHIPS) for b in range(n_level) if a or b]
    plane.sort(key=lambda ab: -2 * min(ab[0], X_CHIPS - ab[0]) - min(ab[1], n_level - ab[1]))

    barrier = pltpu.get_barrier_semaphore()
    count = 0

    def greet(a, b):
        pl.semaphore_signal(barrier, inc=1, device_id=(a, b), device_id_type=MESH)

    for d in far_first(n_level, 0):
        greet(up, level_peers[d])
        greet(down, level_peers[d])
        count += 2
        if d:
            greet(p, level_peers[d])
            count += 1

    inputs = [
        (send_hbm, send_ref),
        (vel_hbm, vel_ref),
        (bot_hbm, bot_ref),
        (rho_hbm, rho_ref),
        (thick_hbm, thick_ref),
        (eta_hbm, eta_ref),
        (nb_hbm, nb_ref),
        (grad_hbm, grad_ref),
        (lap_hbm, lap_ref),
        (cor_hbm, cor_ref),
        (area_hbm, area_ref),
    ]
    loads = [pltpu.make_async_copy(a, b, isem.at[i]) for i, (a, b) in enumerate(inputs)]
    for load in loads:
        load.start()

    sub = lax.broadcasted_iota(jnp.int32, (8, LANES), 0)
    lane = lax.broadcasted_iota(jnp.int32, (8, LANES), 1)
    level_id = sub + g * 8
    for load in loads[:5]:
        load.wait()
    th = jnp.zeros((8, LANES), jnp.float32)
    for l in range(8):
        th = jnp.where(sub == l, thick_ref[l], th)
    send_idx = [send_ref[:, side * LANES : (side + 1) * LANES] for side in range(2)]
    send_lane = [wide(i & (LANES - 1)) for i in send_idx]
    send_tile = [wide(i >> 7) for i in send_idx]

    def listed_levels(tiles, side):
        out = lane_gather(tiles[0], send_lane[side])
        for t in range(1, TILES):
            out = jnp.where(send_tile[side] == t, lane_gather(tiles[t], send_lane[side]), out)
        return out

    def listed_nodes(compact, side):
        got = lane_gather(compact, send_lane[side])
        here = jnp.where(send_tile[side] == sub, got, jnp.zeros_like(got))
        return jnp.sum(here, axis=0, keepdims=True)

    def column(density):
        weighted = density * th
        total = weighted
        for shift in (1, 2, 4):
            total = total + jnp.where(sub >= shift, pltpu.roll(total, shift, 0), 0.0)
        return BUOYANCY * (total - 0.5 * weighted)

    def copy(src, dst, sems, i, a, b):
        return pltpu.make_async_remote_copy(
            src_ref=src,
            dst_ref=dst,
            send_sem=sems.at[0, i],
            recv_sem=sems.at[1, i],
            device_id=(a, b),
            device_id_type=MESH,
        )

    def arrived(buf, sems, i):
        pltpu.make_async_copy(buf, buf, sems.at[1, i]).wait()

    def left(buf, sems, i):
        pltpu.make_async_copy(buf, buf, sems.at[0, i]).wait()

    def send_token(i):
        for d in (2**i, n_space - 2**i):
            there = (lax.rem(p + d, n_space), g)
            pl.semaphore_signal(tok.at[i], inc=1, device_id=there, device_id_type=MESH)

    def pass_token(i):
        pl.semaphore_wait(tok.at[i - 1], 2)
        send_token(i)

    def list_velocity(s):
        for side in range(2):
            for c in range(2):
                usend[s, side, c] = listed_levels([x[c, d] for d in range(TILES)], side)

    def send_velocity(s):
        copy(usend.at[s, 0], urecv.at[s, 1], usem, s, down, g).start()
        copy(usend.at[s, 1], urecv.at[s, 0], usem, s, up, g).start()

    def list_density(s, par):
        tiles = [r[par, d] for d in range(TILES)]
        for side in range(2):
            got = listed_levels(tiles, side)
            rsend[s, side] = got
            gsend[s, side, 0:1] = jnp.sum(got * th, axis=0, keepdims=True)
        for d in range(TILES):
            lsend[s, 0, d : d + 1] = jnp.sum(tiles[d] * th, axis=0, keepdims=True)

    def send_density(s):
        copy(rsend.at[s, 0], rrecv.at[s, 1], rsem, s, down, g).start()
        copy(rsend.at[s, 1], rrecv.at[s, 0], rsem, s, up, g).start()

    def send_sums(s):
        for d in far_first(n_level, 0):
            copy(gsend.at[s, 0], grecv.at[s, 1, d], gsem, s, down, level_peers[d]).start()
            copy(gsend.at[s, 1], grecv.at[s, 0, d], gsem, s, up, level_peers[d]).start()

    def send_level(s):
        for d in far_first(n_level):
            copy(lsend.at[s], lrecv.at[s, d - 1], lsem, s, p, level_peers[d]).start()

    for d in range(TILES):
        cols = slice(d * LANES, (d + 1) * LANES)
        wet = level_id < wide(bot_ref[d : d + 1])
        for c in range(2):
            x[c, d] = jnp.where(wet, vel_ref[c, :, cols], 0.0)
        r[0, d] = rho_ref[:, cols]
    list_velocity(0)
    list_density(0, 0)
    lsend[0, 1] = jnp.zeros((8, LANES), jnp.float32)
    for side in range(2):
        gsend[0, side, 1:2] = jnp.zeros((1, LANES), jnp.float32)
    loads[5].wait()
    wet_nodes = (bot_ref[...] > 0).astype(jnp.float32)
    eta[...] = eta_ref[...]
    for side in range(2):
        ssend[side, 0:1] = listed_nodes(eta_ref[...], side)
        ssend[side, 1:2] = listed_nodes(wet_nodes, side)

    pl.semaphore_wait(barrier, count)
    send_velocity(0)
    send_sums(0)
    send_density(0)
    send_level(0)
    copy(ssend.at[0], srecv.at[1], ssem, 0, down, g).start()
    copy(ssend.at[1], srecv.at[0], ssem, 0, up, g).start()
    send_token(0)

    for load in loads[6:]:
        load.wait()
    bots[0:8] = bot_ref[...]
    cors[0:8] = cor_ref[...]
    for k in range(K):
        for d in range(TILES):
            cols = slice(d * LANES, (d + 1) * LANES)
            row = slice(d, d + 1)
            nbc[k, row] = nb_ref[k : k + 1, cols]
            wts[0, k, row] = grad_ref[k, 0:1, cols]
            wts[1, k, row] = grad_ref[k, 1:2, cols]
            wts[2, k, row] = lap_ref[k : k + 1, cols]
        tile = nbc[k, 0:8] >> 7
        below = jnp.where(p > 0, 1.0, 0.0)
        above = jnp.where(p < n_space - 1, 1.0, 0.0)
        valid = jnp.where(tile == TILES, below, jnp.where(tile == TILES + 1, above, 1.0))
        nbc[k, 8:16] = jnp.zeros((8, LANES), jnp.int32)
        for j in range(3):
            wts[j, k, 0:8] = wts[j, k, 0:8] * valid
            wts[j, k, 8:16] = jnp.zeros((8, LANES), jnp.float32)
        for side in range(2):
            row = slice(8 + side, 9 + side)
            nbc[k, row] = listed_nodes(nbc[k, 0:8], side)
            for j in range(3):
                wts[j, k, row] = listed_nodes(wts[j, k, 0:8], side)
    for side in range(2):
        row = slice(8 + side, 9 + side)
        bots[row] = listed_nodes(bot_ref[...], side)
        cors[row] = listed_nodes(cor_ref[...], side)
    lists = (TILES, TILES + 1)

    def slots(k, d):
        row = wide(nbc[k, d : d + 1])
        return row & (LANES - 1), row >> 7

    def weights(k, d):
        return [wide(wts[j, k, d : d + 1]) for j in range(3)]

    def gather_own(par, dests):
        for d in dests:
            for k in range(K):
                idx, tile = slots(k, d)
                outs = [None] * 3
                for t in range(TILES):
                    hit = tile == t
                    for f, a in enumerate((x[0, t], x[1, t], r[par, t])):
                        got = lane_gather(a, idx)
                        outs[f] = jnp.where(hit, got, outs[f]) if t else got
                for f in range(3):
                    near[f, d * K + k] = outs[f]

    def with_halo(fields, halo, idx, tile, at):
        outs = [near[f, at] for f in fields]
        for side in range(2):
            hit = tile == TILES + side
            outs = [jnp.where(hit, lane_gather(a, idx), o) for a, o in zip(halo[side], outs)]
        return outs

    def velocity_of(s, d):
        if d >= TILES:
            return usend[s, d - TILES, 0], usend[s, d - TILES, 1]
        return x[0, d], x[1, d]

    def density_terms(s, par, dests):
        halo = [(rrecv[s, side],) for side in range(2)]
        for d in dests:
            own = rsend[s, d - TILES] if d >= TILES else r[par, d]
            zero = jnp.zeros((8, LANES), jnp.float32)
            lr, dxr, dyr = [zero] * 3
            for k in range(K):
                idx, tile = slots(k, d)
                (near_r,) = with_halo((2,), halo, idx, tile, d * K + k)
                dr = near_r - own
                we, wn, wl = weights(k, d)
                lr += wl * dr
                dxr += we * dr
                dyr += wn * dr
            u, v = velocity_of(s, d)
            cor = wide(cors[d : d + 1])
            drag = jnp.where(level_id == wide(bots[d : d + 1]) - 1, DRAG, 0.0)
            part[0, d] = u + DT * (cor * v - column(dxr) - drag * u)
            part[1, d] = v - DT * (cor * u + column(dyr) + drag * v)
            new = own + DT * (lr - u * dxr - v * dyr)
            if d >= TILES:
                rsend[s + 1, d - TILES] = new
                gsend[s + 1, d - TILES, 0:1] = jnp.sum(new * th, axis=0, keepdims=True)
            else:
                r[1 - par, d] = new
                lsend[s + 1, 0, d : d + 1] = jnp.sum(new * th, axis=0, keepdims=True)

    def velocity_terms(s, dests):
        halo = [[urecv[s, side, c] for c in range(2)] for side in range(2)]
        for d in dests:
            u, v = velocity_of(s, d)
            zero = jnp.zeros((8, LANES), jnp.float32)
            dxu, dyv, lu, lv = [zero] * 4
            for k in range(K):
                idx, tile = slots(k, d)
                near_u, near_v = with_halo((0, 1), halo, idx, tile, d * K + k)
                we, wn, wl = weights(k, d)
                du, dv = near_u - u, near_v - v
                dxu += we * du
                dyv += wn * dv
                lu += wl * du
                lv += wl * dv
            part[0, d] = part[0, d] + DT * lu
            part[1, d] = part[1, d] + DT * lv
            div = jnp.sum(th * (dxu + dyv), axis=0, keepdims=True)
            if d >= TILES:
                gsend[s + 1, d - TILES, 1:2] = div
            else:
                lsend[s + 1, 1, d : d + 1] = div

    def find_q(s):
        arrived(lrecv.at[s], lsem, s)
        arrived(grecv.at[s], gsem, s)
        div, mass = lsend[s, 1], jnp.zeros((8, LANES), jnp.float32)
        for d in range(1, n_level):
            mass = mass + jnp.where(g >= d, lrecv[s, d - 1, 0], 0.0)
            div = div + lrecv[s, d - 1, 1]
        new_eta = eta[...] - DT * wet_nodes * div
        eta[...] = new_eta
        q[0:8] = new_eta + BUOYANCY * mass
        for side in range(2):
            row = slice(side, side + 1)
            m = jnp.zeros((1, LANES), jnp.float32)
            h = grecv[s, side, 0, 1:2]
            for d in range(1, n_level):
                m = m + jnp.where(g >= d, grecv[s, side, d, 0:1], 0.0)
                h = h + grecv[s, side, d, 1:2]
            e = etah[row] - DT * srecv[side, 1:2] * h
            etah[row] = e
            q[8 + side : 9 + side] = e + BUOYANCY * m

    def shared_terms(dests):
        listed = dests[0] >= TILES
        rows = slice(8, 16) if listed else slice(0, 8)
        own = q[0:8]
        if listed:
            first, second = [wide(listed_nodes(own, side)) for side in range(2)]
            own = jnp.where(sub == 0, first, second)
        dx = jnp.zeros((8, LANES), jnp.float32)
        dy = dx
        source = [wide(q[t : t + 1]) for t in range(TILES + 2)]
        for k in range(K):
            slot = nbc[k, rows]
            idx, tile = slot & (LANES - 1), slot >> 7
            n = lane_gather(source[0], idx)
            for t in range(1, TILES + 2):
                n = jnp.where(tile == t, lane_gather(source[t], idx), n)
            diff = n - own
            dx = dx + wts[0, k, rows] * diff
            dy = dy + wts[1, k, rows] * diff
        dq[0, rows] = DT * dx
        dq[1, rows] = DT * dy

    def new_velocity(d, c):
        wet = level_id < wide(bots[d : d + 1])
        return jnp.where(wet, part[c, d] - wide(dq[c, d : d + 1]), 0.0)

    def drift_weights():
        area = area_ref[...] * wet_nodes
        own = [jnp.zeros((8, LANES), jnp.float32)] * 2
        for k in range(K):
            for j in range(2):
                term = area * wts[j, k, 0:8]
                own[j] = own[j] + term
                for i in range(3):
                    short = term.astype(jnp.bfloat16).astype(jnp.float32)
                    split[i, j, k] = short
                    term = term - short
        target = jnp.where(sub < 2, sub + TILES, jnp.where(sub < 4, sub + TILES - 2, -1))
        slot_lane = lax.broadcasted_iota(jnp.int32, (LANES, LANES), 0)
        total = jnp.zeros((72, LANES), jnp.float32)
        for k in range(K):
            for d in range(0, TILES, 2):
                left_side, right_side = [], []
                for e in (d, d + 1):
                    row = nbc[k, e : e + 1]
                    tile = wide(row >> 7)
                    hit, far = tile == sub, tile == target
                    pieces = []
                    for i in range(3):
                        we, wn = [wide(split[i, j, k, e : e + 1]) for j in range(2)]
                        pieces.append(jnp.where(hit, we, 0.0))
                        pieces.append(jnp.where(hit, wn, 0.0))
                        pieces.append(jnp.where(far, jnp.where(sub < 2, we, wn), 0.0))
                    left_side.append(jnp.concatenate(pieces, axis=0))
                    same = jnp.broadcast_to(row & (LANES - 1), (LANES, LANES)) == slot_lane
                    right_side.append(jnp.where(same, 1.0, 0.0))
                total = total + lax.dot_general(
                    jnp.concatenate(left_side, axis=1).astype(jnp.bfloat16),
                    jnp.concatenate(right_side, axis=1).astype(jnp.bfloat16),
                    (((1,), (1,)), ((), ())),
                    preferred_element_type=jnp.float32,
                )
        total = total[0:24] + total[24:48] + total[48:72]
        for j in range(2):
            coef[j] = total[8 * j : 8 * j + 8] - own[j]
            for side in range(2):
                bsend[side, j : j + 1] = total[16 + 2 * j + side : 17 + 2 * j + side]
        copy(bsend.at[0], brecv.at[1], bsem, 0, down, g).start()
        copy(bsend.at[1], brecv.at[0], bsem, 0, up, g).start()

    def early_drift():
        arrived(brecv, bsem, 0)
        total = jnp.zeros((8, LANES), jnp.float32)
        for j in range(2):
            for d in range(TILES):
                total = total + wide(coef[j, d : d + 1]) * x[j, d]
            for side in range(2):
                total = total + wide(brecv[side, j : j + 1]) * usend[STEPS - 1, side, j]
        return total * th

    def step(s, _):
        par = lax.rem(s, 2)
        @pl.when(s == 1)
        def _():
            pass_token(2)
            drift_weights()

        @pl.when(s == 2)
        def _():
            pass_token(4)

        gather_own(par, (*lists, *range(TILES)))
        arrived(rrecv.at[s], rsem, s)
        density_terms(s, par, lists)
        send_density(s + 1)
        density_terms(s, par, range(TILES))

        @pl.when(s == 0)
        def _():
            pass_token(1)
            arrived(srecv, ssem, 0)
            etah[...] = srecv[:, 0]

        @pl.when(s == 1)
        def _():
            pass_token(3)

        arrived(urecv.at[s], usem, s)
        velocity_terms(s, lists)
        send_sums(s + 1)
        find_q(s)
        shared_terms(lists)
        for side in range(2):
            for c in range(2):
                usend[s + 1, side, c] = new_velocity(TILES + side, c)
        send_velocity(s + 1)
        velocity_terms(s, range(TILES))
        send_level(s + 1)
        vv[s] = area_ref[...] * wet_nodes * lsend[s + 1, 1]
        shared_terms(range(TILES))
        for d in range(TILES):
            for c in range(2):
                x[c, d] = new_velocity(d, c)
        return 0

    lax.fori_loop(0, STEPS - 1, step, 0)
    last = STEPS - 1
    par = last % 2

    sums = jnp.zeros((8, LANES), jnp.float32)
    terms = [vv[s] for s in range(last)]
    terms += [early_drift(), area_ref[...] * wet_nodes * (1.0 / n_level)]
    for j, term in enumerate(terms):
        sums = jnp.where(sub == j, wide(jnp.sum(term, axis=0, keepdims=True)), sums)
    sums = jnp.broadcast_to(jnp.sum(sums, axis=1, keepdims=True), (8, LANES))
    row = jnp.sum(jnp.where(sub == lane, sums, 0.0), axis=0, keepdims=True)
    zsend[...] = row
    pl.semaphore_wait(tok.at[4], 2)
    for d in far_first(n_z):
        copy(zsend, zrecv.at[d - 1], zsem, 0, z_peer(d), g).start()

    gather_own(par, range(TILES))
    arrived(rrecv.at[last], rsem, last)
    density_terms(last, par, range(TILES))
    for d in range(TILES):
        rho_out[:, d * LANES : (d + 1) * LANES] = r[1 - par, d]
    arrived(urecv.at[last], usem, last)
    velocity_terms(last, range(TILES))
    send_level(STEPS)
    find_q(last)
    shared_terms(range(TILES))
    for d in range(TILES):
        for c in range(2):
            vel_out[c, :, d * LANES : (d + 1) * LANES] = new_velocity(d, c)

    arrived(zrecv, zsem, 0)
    for d in range(1, n_z):
        row = row + zrecv[d - 1]
    xsend[...] = row
    for i, (a, b) in enumerate(plane):
        copy(xsend, xrecv.at[i], zsem, 1, x_peers[a], level_peers[b]).start()

    arrived(lrecv.at[STEPS], lsem, STEPS)
    div = lsend[STEPS, 1]
    for d in range(1, n_level):
        div = div + lrecv[STEPS, d - 1, 1]
    eta[...] = eta[...] - DT * wet_nodes * div

    arrived(xrecv, zsem, 1)
    for i in range(len(plane)):
        row = row + xrecv[i]
    lane_row = lane[0:1]
    total = jnp.sum(jnp.where(lane_row == STEPS, row, 0.0), axis=1, keepdims=True)
    drifts = jnp.where(lane_row < STEPS, row / total, 0.0)
    drift_out[...] = drifts
    eta_out[...] = eta[...] + DT * jnp.sum(drifts, axis=1, keepdims=True)

    for s in range(STEPS + 1):
        left(lrecv.at[s], lsem, s)
    for s in range(STEPS):
        left(usend.at[s], usem, s)
        left(rsend.at[s], rsem, s)
        left(grecv.at[s], gsem, s)
    left(ssend, ssem, 0)
    left(bsend, bsem, 0)
    left(zrecv, zsem, 0)
    left(xrecv, zsem, 1)


def finish(vel, rho, eta, drift, vel_out, rho_out, eta_out, drift_out, sem):
    copies = [
        pltpu.make_async_copy(a, b, sem.at[i])
        for i, (a, b) in enumerate(((vel, vel_out), (rho, rho_out), (eta, eta_out)))
    ]
    for c in copies:
        c.start()
    drift_out[...] = drift[0, :STEPS]
    for c in copies:
        c.wait()


def solution(mesh):
    n_space, n_level = mesh.shape["space"], mesh.shape["level"]

    def local(
        velocity,
        density,
        elevation,
        grad_weights,
        lap_weights,
        coriolis,
        node_area,
        thickness,
        send_list,
        neighbours,
        bottom,
    ):
        f32, i32 = jnp.float32, jnp.int32
        compact = (TILES, LANES)
        vmem = pl.BlockSpec(memory_space=pltpu.VMEM)
        dma = pltpu.SemaphoreType.DMA
        peers = n_level - 1
        n_z = n_space // X_CHIPS
        row = (1, LANES)
        inputs = [
            pltpu.VMEM(velocity.shape, f32),
            pltpu.VMEM(density.shape, f32),
            pltpu.VMEM(compact, f32),
            pltpu.VMEM((K, 2, TILES * LANES), f32),
            pltpu.VMEM(lap_weights.shape, f32),
            pltpu.VMEM(compact, f32),
            pltpu.VMEM(compact, f32),
            pltpu.SMEM(thickness.shape, f32),
            pltpu.VMEM(send_list.shape, i32),
            pltpu.VMEM(neighbours.shape, i32),
            pltpu.VMEM(compact, i32),
            dma((11,)),
            pltpu.VMEM((K, 16, LANES), i32),
        ]
        shapes = [
            (2, 8, 8, LANES),
            (2, 8, 8, LANES),
            (2, 10, 8, LANES),
            (3, 60, 8, LANES),
            (16, LANES),
            (2, 16, LANES),
            (8, LANES),
            (2, LANES),
            (STEPS, 8, LANES),
            (STEPS + 1, 2, 8, LANES),
            (STEPS + 1, peers, 2, 8, LANES),
            (STEPS, 2, 2, 8, LANES),
            (STEPS, 2, 2, 8, LANES),
            (STEPS, 2, 8, LANES),
            (STEPS, 2, 8, LANES),
            (STEPS, 2, 2, LANES),
            (STEPS, 2, n_level, 2, LANES),
            (2, 2, LANES),
            (2, 2, LANES),
            row,
            (n_z - 1, *row),
            row,
            (X_CHIPS * n_level - 1, *row),
            (3, 2, K, 8, LANES),
            (2, 8, LANES),
            (2, 2, LANES),
            (2, 2, LANES),
        ]

        def body(*refs):
            kernel(n_space, n_level, *refs)

        vel, rho, eta, drift = pl.pallas_call(
            body,
            out_shape=(
                pltpu.VMEM(velocity.shape, f32),
                pltpu.VMEM(density.shape, f32),
                pltpu.VMEM(compact, f32),
                pltpu.VMEM((1, LANES), f32),
            ),
            in_specs=[pl.BlockSpec(memory_space=pl.ANY)] * 11,
            out_specs=(vmem,) * 4,
            scratch_shapes=inputs
            + [pltpu.VMEM((3, K, 16, LANES), f32)]
            + [pltpu.VMEM((16, LANES), i32), pltpu.VMEM((16, LANES), f32)]
            + [pltpu.VMEM(shape, f32) for shape in shapes]
            + [
                dma((2, 5)),
                dma((2, 4)),
                dma((2, 4)),
                dma((2, 4)),
                dma((2, 1)),
                dma((2, 1)),
                dma((2, 2)),
                pltpu.SemaphoreType.REGULAR((5,)),
            ],
            compiler_params=pltpu.CompilerParams(collective_id=0, has_side_effects=True),
        )(
            velocity,
            density,
            elevation.reshape(compact),
            jnp.swapaxes(grad_weights, 0, 1),
            lap_weights,
            coriolis.reshape(compact),
            node_area.reshape(compact),
            thickness,
            send_list,
            neighbours,
            bottom.reshape(compact),
        )
        results = [pltpu.with_memory_space_constraint(a, pltpu.VMEM) for a in (vel, rho, eta, drift)]
        vel, rho, eta, drift = pl.pallas_call(
            finish,
            out_shape=(
                jax.ShapeDtypeStruct(velocity.shape, f32),
                jax.ShapeDtypeStruct(density.shape, f32),
                jax.ShapeDtypeStruct(compact, f32),
                jax.ShapeDtypeStruct((STEPS,), f32),
            ),
            in_specs=[vmem] * 4,
            out_specs=(pl.BlockSpec(memory_space=pl.ANY),) * 3 + (vmem,),
            scratch_shapes=[dma((3,))],
        )(*results)
        return vel, rho, eta.reshape(elevation.shape), drift

    return jax.shard_map(
        local,
        mesh=mesh,
        in_specs=(
            P(None, "level", "space"),
            P("level", "space"),
            P("space"),
            P(None, None, "space"),
            P(None, "space"),
            P("space"),
            P("space"),
            P("level"),
            P("space", None),
            P(None, "space"),
            P("space"),
        ),
        out_specs=(P(None, "level", "space"), P("level", "space"), P("space"), P()),
        check_vma=False,
    )
```

```python
import jax
import jax.numpy as jnp
from jax import lax
from jax.experimental import pallas as pl
from jax.experimental.pallas import tpu as pltpu
from jax.sharding import PartitionSpec as P

MESH = pl.DeviceIdType.MESH
STEPS = 4
K = 6
TILES = 8
LANES = 128
X_CHIPS = 4
DT = 0.1
BUOYANCY = 0.5
DRAG = 0.5

_LANE_GATHER = lax.GatherDimensionNumbers(
    offset_dims=(),
    collapsed_slice_dims=(1,),
    start_index_map=(1,),
    operand_batching_dims=(0,),
    start_indices_batching_dims=(0,),
)


def lane_gather(x, idx):
    return lax.gather(
        x, idx[..., None], _LANE_GATHER, (1, 1), mode=lax.GatherScatterMode.PROMISE_IN_BOUNDS
    )


def far_first(count, start=1):
    return sorted(range(start, count), key=lambda d: -min(d, count - d))


def wide(row):
    return jnp.broadcast_to(row, (8, LANES))


def kernel(
    n_space,
    n_level,
    vel_hbm,
    rho_hbm,
    eta_hbm,
    grad_hbm,
    lap_hbm,
    cor_hbm,
    area_hbm,
    thick_hbm,
    send_hbm,
    nb_hbm,
    bot_hbm,
    vel_out,
    rho_out,
    eta_out,
    drift_out,
    vel_ref,
    rho_ref,
    eta_ref,
    grad_ref,
    lap_ref,
    cor_ref,
    area_ref,
    thick_ref,
    send_ref,
    nb_ref,
    bot_ref,
    isem,
    nbc,
    wts,
    bots,
    cors,
    x,
    r,
    part,
    near,
    q,
    dq,
    eta,
    etah,
    vv,
    lsend,
    lrecv,
    usend,
    urecv,
    rsend,
    rrecv,
    gsend,
    grecv,
    ssend,
    srecv,
    zsend,
    zrecv,
    xsend,
    xrecv,
    split,
    coef,
    bsend,
    brecv,
    hsend,
    hrecv,
    lsem,
    usem,
    rsem,
    gsem,
    ssem,
    bsem,
    hsem,
    zsem,
    tok,
):
    p = lax.axis_index("space")
    g = lax.axis_index("level")
    n_z = n_space // X_CHIPS
    up = lax.rem(p + 1, n_space)
    down = lax.rem(p + n_space - 1, n_space)
    level_peers = [lax.rem(g + d, n_level) for d in range(n_level)]

    def z_peer(d):
        return lax.rem(p + d * X_CHIPS, n_space)

    px = lax.rem(p, X_CHIPS)
    x_peers = [p - px + lax.rem(px + d, X_CHIPS) for d in range(X_CHIPS)]
    plane = [(a, b) for a in range(X_CHIPS) for b in range(n_level) if a or b]
    plane.sort(key=lambda ab: -2 * min(ab[0], X_CHIPS - ab[0]) - min(ab[1], n_level - ab[1]))

    barrier = pltpu.get_barrier_semaphore()

    def greet(a, b):
        pl.semaphore_signal(barrier, inc=1, device_id=(a, b), device_id_type=MESH)

    greet(up, g)
    greet(down, g)
    for d in far_first(n_level):
        greet(p, level_peers[d])
    count = n_level + 1

    inputs = [
        (send_hbm, send_ref),
        (vel_hbm, vel_ref),
        (bot_hbm, bot_ref),
        (rho_hbm, rho_ref),
        (thick_hbm, thick_ref),
        (eta_hbm, eta_ref),
        (nb_hbm, nb_ref),
        (grad_hbm, grad_ref),
        (lap_hbm, lap_ref),
        (cor_hbm, cor_ref),
        (area_hbm, area_ref),
    ]
    loads = [pltpu.make_async_copy(a, b, isem.at[i]) for i, (a, b) in enumerate(inputs)]
    for load in loads:
        load.start()

    sub = lax.broadcasted_iota(jnp.int32, (8, LANES), 0)
    lane = lax.broadcasted_iota(jnp.int32, (8, LANES), 1)
    level_id = sub + g * 8
    for load in loads[:5]:
        load.wait()
    th = jnp.zeros((8, LANES), jnp.float32)
    for l in range(8):
        th = jnp.where(sub == l, thick_ref[l], th)
    send_idx = [send_ref[:, side * LANES : (side + 1) * LANES] for side in range(2)]
    send_lane = [wide(i & (LANES - 1)) for i in send_idx]
    send_tile = [wide(i >> 7) for i in send_idx]

    def listed_levels(tiles, side):
        out = lane_gather(tiles[0], send_lane[side])
        for t in range(1, TILES):
            out = jnp.where(send_tile[side] == t, lane_gather(tiles[t], send_lane[side]), out)
        return out

    def listed_nodes(compact, side):
        got = lane_gather(compact, send_lane[side])
        here = jnp.where(send_tile[side] == sub, got, jnp.zeros_like(got))
        return jnp.sum(here, axis=0, keepdims=True)

    def column(density):
        weighted = density * th
        total = weighted
        for shift in (1, 2, 4):
            total = total + jnp.where(sub >= shift, pltpu.roll(total, shift, 0), 0.0)
        return BUOYANCY * (total - 0.5 * weighted)

    def copy(src, dst, sems, i, a, b):
        return pltpu.make_async_remote_copy(
            src_ref=src,
            dst_ref=dst,
            send_sem=sems.at[0, i],
            recv_sem=sems.at[1, i],
            device_id=(a, b),
            device_id_type=MESH,
        )

    def arrived(buf, sems, i):
        pltpu.make_async_copy(buf, buf, sems.at[1, i]).wait()

    def left(buf, sems, i):
        pltpu.make_async_copy(buf, buf, sems.at[0, i]).wait()

    def send_token(i):
        for d in (2**i, n_space - 2**i):
            there = (lax.rem(p + d, n_space), g)
            pl.semaphore_signal(tok.at[i], inc=1, device_id=there, device_id_type=MESH)

    def pass_token(i):
        pl.semaphore_wait(tok.at[i - 1], 2)
        send_token(i)

    def list_velocity(s):
        for side in range(2):
            for c in range(2):
                usend[s, side, c] = listed_levels([x[c, d] for d in range(TILES)], side)

    def send_velocity(s):
        copy(usend.at[s, 0], urecv.at[s, 1], usem, s, down, g).start()
        copy(usend.at[s, 1], urecv.at[s, 0], usem, s, up, g).start()

    def list_density(s, par):
        tiles = [r[par, d] for d in range(TILES)]
        for side in range(2):
            got = listed_levels(tiles, side)
            rsend[s, side] = got
        for d in range(TILES):
            lsend[s, 0, d : d + 1] = jnp.sum(tiles[d] * th, axis=0, keepdims=True)

    def send_density(s):
        copy(rsend.at[s, 0], rrecv.at[s, 1], rsem, s, down, g).start()
        copy(rsend.at[s, 1], rrecv.at[s, 0], rsem, s, up, g).start()

    def send_sums(s):
        for d in far_first(n_level, 0):
            copy(gsend.at[s, 0], grecv.at[s, 1, d], gsem, s, down, level_peers[d]).start()
            copy(gsend.at[s, 1], grecv.at[s, 0, d], gsem, s, up, level_peers[d]).start()

    def send_level(s):
        for d in far_first(n_level):
            copy(lsend.at[s], lrecv.at[s, d - 1], lsem, s, p, level_peers[d]).start()

    for d in range(TILES):
        cols = slice(d * LANES, (d + 1) * LANES)
        wet = level_id < wide(bot_ref[d : d + 1])
        for c in range(2):
            x[c, d] = jnp.where(wet, vel_ref[c, :, cols], 0.0)
        r[0, d] = rho_ref[:, cols]
    list_velocity(0)
    list_density(0, 0)
    lsend[0, 1] = jnp.zeros((8, LANES), jnp.float32)
    loads[5].wait()
    wet_nodes = (bot_ref[...] > 0).astype(jnp.float32)
    eta[...] = eta_ref[...]
    for side in range(2):
        ssend[side, 0:1] = listed_nodes(eta_ref[...], side)
        ssend[side, 1:2] = listed_nodes(wet_nodes, side)

    pl.semaphore_wait(barrier, count)
    send_density(0)
    send_velocity(0)
    send_level(0)
    copy(ssend.at[0], srecv.at[1], ssem, 0, down, g).start()
    copy(ssend.at[1], srecv.at[0], ssem, 0, up, g).start()
    send_token(0)

    for load in loads[6:]:
        load.wait()
    bots[0:8] = bot_ref[...]
    cors[0:8] = cor_ref[...]
    for k in range(K):
        for d in range(TILES):
            cols = slice(d * LANES, (d + 1) * LANES)
            row = slice(d, d + 1)
            nbc[k, row] = nb_ref[k : k + 1, cols]
            wts[0, k, row] = grad_ref[k, 0:1, cols]
            wts[1, k, row] = grad_ref[k, 1:2, cols]
            wts[2, k, row] = lap_ref[k : k + 1, cols]
        tile = nbc[k, 0:8] >> 7
        below = jnp.where(p > 0, 1.0, 0.0)
        above = jnp.where(p < n_space - 1, 1.0, 0.0)
        valid = jnp.where(tile == TILES, below, jnp.where(tile == TILES + 1, above, 1.0))
        nbc[k, 8:16] = jnp.zeros((8, LANES), jnp.int32)
        for j in range(3):
            wts[j, k, 0:8] = wts[j, k, 0:8] * valid
            wts[j, k, 8:16] = jnp.zeros((8, LANES), jnp.float32)
        for side in range(2):
            row = slice(8 + side, 9 + side)
            nbc[k, row] = listed_nodes(nbc[k, 0:8], side)
            for j in range(3):
                wts[j, k, row] = listed_nodes(wts[j, k, 0:8], side)
    for side in range(2):
        row = slice(8 + side, 9 + side)
        bots[row] = listed_nodes(bot_ref[...], side)
        cors[row] = listed_nodes(cor_ref[...], side)
    lists = (TILES, TILES + 1)

    def slots(k, d):
        row = wide(nbc[k, d : d + 1])
        return row & (LANES - 1), row >> 7

    def weights(k, d):
        return [wide(wts[j, k, d : d + 1]) for j in range(3)]

    def gather_own(par, dests):
        for d in dests:
            for k in range(K):
                idx, tile = slots(k, d)
                outs = [None] * 3
                for t in range(TILES):
                    hit = tile == t
                    for f, a in enumerate((x[0, t], x[1, t], r[par, t])):
                        got = lane_gather(a, idx)
                        outs[f] = jnp.where(hit, got, outs[f]) if t else got
                for f in range(3):
                    near[f, d * K + k] = outs[f]

    def with_halo(fields, halo, idx, tile, at):
        outs = [near[f, at] for f in fields]
        for side in range(2):
            hit = tile == TILES + side
            outs = [jnp.where(hit, lane_gather(a, idx), o) for a, o in zip(halo[side], outs)]
        return outs

    def send_halo_mass():
        for side in range(2):
            hsend[side : side + 1] = jnp.sum(rrecv[0, side] * th, axis=0, keepdims=True)
        for d in far_first(n_level):
            copy(hsend, hrecv.at[d - 1], hsem, 0, p, level_peers[d]).start()

    def halo_mass():
        arrived(hrecv, hsem, 0)
        zero = jnp.zeros((1, LANES), jnp.float32)
        for side in range(2):
            for d in range(n_level):
                grecv[0, side, d, 0:1] = hrecv[d - 1, side : side + 1] if d else zero
                grecv[0, side, d, 1:2] = zero

    def velocity_of(s, d):
        if d >= TILES:
            return usend[s, d - TILES, 0], usend[s, d - TILES, 1]
        return x[0, d], x[1, d]

    def density_terms(s, par, dests):
        halo = [(rrecv[s, side],) for side in range(2)]
        for d in dests:
            own = rsend[s, d - TILES] if d >= TILES else r[par, d]
            zero = jnp.zeros((8, LANES), jnp.float32)
            lr, dxr, dyr = [zero] * 3
            for k in range(K):
                idx, tile = slots(k, d)
                (near_r,) = with_halo((2,), halo, idx, tile, d * K + k)
                dr = near_r - own
                we, wn, wl = weights(k, d)
                lr += wl * dr
                dxr += we * dr
                dyr += wn * dr
            u, v = velocity_of(s, d)
            cor = wide(cors[d : d + 1])
            drag = jnp.where(level_id == wide(bots[d : d + 1]) - 1, DRAG, 0.0)
            part[0, d] = u + DT * (cor * v - column(dxr) - drag * u)
            part[1, d] = v - DT * (cor * u + column(dyr) + drag * v)
            new = own + DT * (lr - u * dxr - v * dyr)
            if d >= TILES:
                rsend[s + 1, d - TILES] = new
                gsend[s + 1, d - TILES, 0:1] = jnp.sum(new * th, axis=0, keepdims=True)
            else:
                r[1 - par, d] = new
                lsend[s + 1, 0, d : d + 1] = jnp.sum(new * th, axis=0, keepdims=True)

    def velocity_terms(s, dests):
        halo = [[urecv[s, side, c] for c in range(2)] for side in range(2)]
        for d in dests:
            u, v = velocity_of(s, d)
            zero = jnp.zeros((8, LANES), jnp.float32)
            dxu, dyv, lu, lv = [zero] * 4
            for k in range(K):
                idx, tile = slots(k, d)
                near_u, near_v = with_halo((0, 1), halo, idx, tile, d * K + k)
                we, wn, wl = weights(k, d)
                du, dv = near_u - u, near_v - v
                dxu += we * du
                dyv += wn * dv
                lu += wl * du
                lv += wl * dv
            part[0, d] = part[0, d] + DT * lu
            part[1, d] = part[1, d] + DT * lv
            div = jnp.sum(th * (dxu + dyv), axis=0, keepdims=True)
            if d >= TILES:
                gsend[s + 1, d - TILES, 1:2] = div
            else:
                lsend[s + 1, 1, d : d + 1] = div

    def find_q(s):
        arrived(lrecv.at[s], lsem, s)
        div, mass = lsend[s, 1], jnp.zeros((8, LANES), jnp.float32)
        for d in range(1, n_level):
            mass = mass + jnp.where(g >= d, lrecv[s, d - 1, 0], 0.0)
            div = div + lrecv[s, d - 1, 1]
        new_eta = eta[...] - DT * wet_nodes * div
        eta[...] = new_eta
        q[0:8] = new_eta + BUOYANCY * mass
        for side in range(2):
            row = slice(side, side + 1)
            m = jnp.zeros((1, LANES), jnp.float32)
            h = grecv[s, side, 0, 1:2]
            for d in range(1, n_level):
                m = m + jnp.where(g >= d, grecv[s, side, d, 0:1], 0.0)
                h = h + grecv[s, side, d, 1:2]
            e = etah[row] - DT * srecv[side, 1:2] * h
            etah[row] = e
            q[8 + side : 9 + side] = e + BUOYANCY * m

    def shared_terms(dests):
        listed = dests[0] >= TILES
        rows = slice(8, 16) if listed else slice(0, 8)
        own = q[0:8]
        if listed:
            first, second = [wide(listed_nodes(own, side)) for side in range(2)]
            own = jnp.where(sub == 0, first, second)
        dx = jnp.zeros((8, LANES), jnp.float32)
        dy = dx
        source = [wide(q[t : t + 1]) for t in range(TILES + 2)]
        for k in range(K):
            slot = nbc[k, rows]
            idx, tile = slot & (LANES - 1), slot >> 7
            n = lane_gather(source[0], idx)
            for t in range(1, TILES + 2):
                n = jnp.where(tile == t, lane_gather(source[t], idx), n)
            diff = n - own
            dx = dx + wts[0, k, rows] * diff
            dy = dy + wts[1, k, rows] * diff
        dq[0, rows] = DT * dx
        dq[1, rows] = DT * dy

    def new_velocity(d, c):
        wet = level_id < wide(bots[d : d + 1])
        return jnp.where(wet, part[c, d] - wide(dq[c, d : d + 1]), 0.0)

    def drift_weights():
        area = area_ref[...] * wet_nodes
        own = [jnp.zeros((8, LANES), jnp.float32)] * 2
        for k in range(K):
            for j in range(2):
                term = area * wts[j, k, 0:8]
                own[j] = own[j] + term
                for i in range(3):
                    short = term.astype(jnp.bfloat16).astype(jnp.float32)
                    split[i, j, k] = short
                    term = term - short
        target = jnp.where(sub < 2, sub + TILES, jnp.where(sub < 4, sub + TILES - 2, -1))
        slot_lane = lax.broadcasted_iota(jnp.int32, (LANES, LANES), 0)
        total = jnp.zeros((72, LANES), jnp.float32)
        for k in range(K):
            for d in range(0, TILES, 2):
                left_side, right_side = [], []
                for e in (d, d + 1):
                    row = nbc[k, e : e + 1]
                    tile = wide(row >> 7)
                    hit, far = tile == sub, tile == target
                    pieces = []
                    for i in range(3):
                        we, wn = [wide(split[i, j, k, e : e + 1]) for j in range(2)]
                        pieces.append(jnp.where(hit, we, 0.0))
                        pieces.append(jnp.where(hit, wn, 0.0))
                        pieces.append(jnp.where(far, jnp.where(sub < 2, we, wn), 0.0))
                    left_side.append(jnp.concatenate(pieces, axis=0))
                    same = jnp.broadcast_to(row & (LANES - 1), (LANES, LANES)) == slot_lane
                    right_side.append(jnp.where(same, 1.0, 0.0))
                total = total + lax.dot_general(
                    jnp.concatenate(left_side, axis=1).astype(jnp.bfloat16),
                    jnp.concatenate(right_side, axis=1).astype(jnp.bfloat16),
                    (((1,), (1,)), ((), ())),
                    preferred_element_type=jnp.float32,
                )
        total = total[0:24] + total[24:48] + total[48:72]
        for j in range(2):
            coef[j] = total[8 * j : 8 * j + 8] - own[j]
            for side in range(2):
                bsend[side, j : j + 1] = total[16 + 2 * j + side : 17 + 2 * j + side]
        copy(bsend.at[0], brecv.at[1], bsem, 0, down, g).start()
        copy(bsend.at[1], brecv.at[0], bsem, 0, up, g).start()

    def early_drift():
        arrived(brecv, bsem, 0)
        total = jnp.zeros((8, LANES), jnp.float32)
        for j in range(2):
            for d in range(TILES):
                total = total + wide(coef[j, d : d + 1]) * x[j, d]
            for side in range(2):
                total = total + wide(brecv[side, j : j + 1]) * usend[STEPS - 1, side, j]
        return total * th

    def step(s, _):
        par = lax.rem(s, 2)
        @pl.when(s == 1)
        def _():
            pass_token(3)

        gather_own(par, (*lists, *range(TILES)))

        @pl.when(s == 0)
        def _():
            pass_token(1)
            drift_weights()

        arrived(rrecv.at[s], rsem, s)

        @pl.when(s == 0)
        def _():
            send_halo_mass()

        density_terms(s, par, lists)
        send_density(s + 1)
        density_terms(s, par, range(TILES))

        @pl.when(s == 0)
        def _():
            pass_token(2)
            arrived(srecv, ssem, 0)
            etah[...] = srecv[:, 0]

        @pl.when(s == 1)
        def _():
            pass_token(4)

        arrived(urecv.at[s], usem, s)
        velocity_terms(s, lists)
        send_sums(s + 1)

        @pl.when(s == 0)
        def _():
            halo_mass()

        @pl.when(s > 0)
        def _():
            arrived(grecv.at[s], gsem, s)

        find_q(s)
        shared_terms(lists)
        for side in range(2):
            for c in range(2):
                usend[s + 1, side, c] = new_velocity(TILES + side, c)
        send_velocity(s + 1)
        velocity_terms(s, range(TILES))
        send_level(s + 1)
        vv[s] = area_ref[...] * wet_nodes * lsend[s + 1, 1]
        shared_terms(range(TILES))
        for d in range(TILES):
            for c in range(2):
                x[c, d] = new_velocity(d, c)
        return 0

    lax.fori_loop(0, STEPS - 1, step, 0)
    last = STEPS - 1
    par = last % 2

    sums = jnp.zeros((8, LANES), jnp.float32)
    terms = [vv[s] for s in range(last)]
    terms += [early_drift(), area_ref[...] * wet_nodes * (1.0 / n_level)]
    for j, term in enumerate(terms):
        sums = jnp.where(sub == j, wide(jnp.sum(term, axis=0, keepdims=True)), sums)
    sums = jnp.broadcast_to(jnp.sum(sums, axis=1, keepdims=True), (8, LANES))
    row = jnp.sum(jnp.where(sub == lane, sums, 0.0), axis=0, keepdims=True)
    zsend[...] = row
    pl.semaphore_wait(tok.at[4], 2)
    for d in far_first(n_z):
        copy(zsend, zrecv.at[d - 1], zsem, 0, z_peer(d), g).start()

    gather_own(par, range(TILES))
    arrived(rrecv.at[last], rsem, last)
    density_terms(last, par, range(TILES))
    for d in range(TILES):
        rho_out[:, d * LANES : (d + 1) * LANES] = r[1 - par, d]
    arrived(urecv.at[last], usem, last)
    velocity_terms(last, range(TILES))
    send_level(STEPS)
    arrived(grecv.at[last], gsem, last)
    find_q(last)
    shared_terms(range(TILES))
    for d in range(TILES):
        for c in range(2):
            vel_out[c, :, d * LANES : (d + 1) * LANES] = new_velocity(d, c)

    arrived(zrecv, zsem, 0)
    for d in range(1, n_z):
        row = row + zrecv[d - 1]
    xsend[...] = row
    for i, (a, b) in enumerate(plane):
        copy(xsend, xrecv.at[i], zsem, 1, x_peers[a], level_peers[b]).start()

    arrived(lrecv.at[STEPS], lsem, STEPS)
    div = lsend[STEPS, 1]
    for d in range(1, n_level):
        div = div + lrecv[STEPS, d - 1, 1]
    eta[...] = eta[...] - DT * wet_nodes * div

    for s in range(STEPS + 1):
        left(lrecv.at[s], lsem, s)
    for s in range(STEPS):
        left(usend.at[s], usem, s)
        left(rsend.at[s], rsem, s)
    for s in range(1, STEPS):
        left(grecv.at[s], gsem, s)
    left(ssend, ssem, 0)
    left(bsend, bsem, 0)
    left(hrecv, hsem, 0)
    left(zrecv, zsem, 0)

    arrived(xrecv, zsem, 1)
    for i in range(len(plane)):
        row = row + xrecv[i]
    lane_row = lane[0:1]
    total = jnp.sum(jnp.where(lane_row == STEPS, row, 0.0), axis=1, keepdims=True)
    drift_sum = jnp.sum(jnp.where(lane_row < STEPS, row, 0.0), axis=1, keepdims=True)
    drift_out[...] = jnp.where(lane_row < STEPS, row / total, 0.0)
    eta_out[...] = eta[...] + DT * (drift_sum / total)
    left(xrecv, zsem, 1)


def finish(vel, rho, eta, drift, vel_out, rho_out, eta_out, drift_out, sem):
    copies = [
        pltpu.make_async_copy(a, b, sem.at[i])
        for i, (a, b) in enumerate(((vel, vel_out), (rho, rho_out), (eta, eta_out)))
    ]
    for c in copies:
        c.start()
    drift_out[...] = drift[0, :STEPS]
    for c in copies:
        c.wait()


def solution(mesh):
    n_space, n_level = mesh.shape["space"], mesh.shape["level"]

    def local(
        velocity,
        density,
        elevation,
        grad_weights,
        lap_weights,
        coriolis,
        node_area,
        thickness,
        send_list,
        neighbours,
        bottom,
    ):
        f32, i32 = jnp.float32, jnp.int32
        compact = (TILES, LANES)
        vmem = pl.BlockSpec(memory_space=pltpu.VMEM)
        dma = pltpu.SemaphoreType.DMA
        peers = n_level - 1
        n_z = n_space // X_CHIPS
        row = (1, LANES)
        inputs = [
            pltpu.VMEM(velocity.shape, f32),
            pltpu.VMEM(density.shape, f32),
            pltpu.VMEM(compact, f32),
            pltpu.VMEM((K, 2, TILES * LANES), f32),
            pltpu.VMEM(lap_weights.shape, f32),
            pltpu.VMEM(compact, f32),
            pltpu.VMEM(compact, f32),
            pltpu.SMEM(thickness.shape, f32),
            pltpu.VMEM(send_list.shape, i32),
            pltpu.VMEM(neighbours.shape, i32),
            pltpu.VMEM(compact, i32),
            dma((11,)),
            pltpu.VMEM((K, 16, LANES), i32),
        ]
        shapes = [
            (2, 8, 8, LANES),
            (2, 8, 8, LANES),
            (2, 10, 8, LANES),
            (3, 60, 8, LANES),
            (16, LANES),
            (2, 16, LANES),
            (8, LANES),
            (2, LANES),
            (STEPS, 8, LANES),
            (STEPS + 1, 2, 8, LANES),
            (STEPS + 1, peers, 2, 8, LANES),
            (STEPS, 2, 2, 8, LANES),
            (STEPS, 2, 2, 8, LANES),
            (STEPS, 2, 8, LANES),
            (STEPS, 2, 8, LANES),
            (STEPS, 2, 2, LANES),
            (STEPS, 2, n_level, 2, LANES),
            (2, 2, LANES),
            (2, 2, LANES),
            row,
            (n_z - 1, *row),
            row,
            (X_CHIPS * n_level - 1, *row),
            (3, 2, K, 8, LANES),
            (2, 8, LANES),
            (2, 2, LANES),
            (2, 2, LANES),
            (2, LANES),
            (peers, 2, LANES),
        ]

        def body(*refs):
            kernel(n_space, n_level, *refs)

        vel, rho, eta, drift = pl.pallas_call(
            body,
            out_shape=(
                pltpu.VMEM(velocity.shape, f32),
                pltpu.VMEM(density.shape, f32),
                pltpu.VMEM(compact, f32),
                pltpu.VMEM((1, LANES), f32),
            ),
            in_specs=[pl.BlockSpec(memory_space=pl.ANY)] * 11,
            out_specs=(vmem,) * 4,
            scratch_shapes=inputs
            + [pltpu.VMEM((3, K, 16, LANES), f32)]
            + [pltpu.VMEM((16, LANES), i32), pltpu.VMEM((16, LANES), f32)]
            + [pltpu.VMEM(shape, f32) for shape in shapes]
            + [
                dma((2, 5)),
                dma((2, 4)),
                dma((2, 4)),
                dma((2, 4)),
                dma((2, 1)),
                dma((2, 1)),
                dma((2, 1)),
                dma((2, 2)),
                pltpu.SemaphoreType.REGULAR((5,)),
            ],
            compiler_params=pltpu.CompilerParams(collective_id=0, has_side_effects=True),
        )(
            velocity,
            density,
            elevation.reshape(compact),
            jnp.swapaxes(grad_weights, 0, 1),
            lap_weights,
            coriolis.reshape(compact),
            node_area.reshape(compact),
            thickness,
            send_list,
            neighbours,
            bottom.reshape(compact),
        )
        results = [pltpu.with_memory_space_constraint(a, pltpu.VMEM) for a in (vel, rho, eta, drift)]
        vel, rho, eta, drift = pl.pallas_call(
            finish,
            out_shape=(
                jax.ShapeDtypeStruct(velocity.shape, f32),
                jax.ShapeDtypeStruct(density.shape, f32),
                jax.ShapeDtypeStruct(compact, f32),
                jax.ShapeDtypeStruct((STEPS,), f32),
            ),
            in_specs=[vmem] * 4,
            out_specs=(pl.BlockSpec(memory_space=pl.ANY),) * 3 + (vmem,),
            scratch_shapes=[dma((3,))],
        )(*results)
        return vel, rho, eta.reshape(elevation.shape), drift

    return jax.shard_map(
        local,
        mesh=mesh,
        in_specs=(
            P(None, "level", "space"),
            P("level", "space"),
            P("space"),
            P(None, None, "space"),
            P(None, "space"),
            P("space"),
            P("space"),
            P("level"),
            P("space", None),
            P(None, "space"),
            P("space"),
        ),
        out_specs=(P(None, "level", "space"), P("level", "space"), P("space"), P()),
        check_vma=False,
    )
```

```python
import jax
import jax.numpy as jnp
from jax import lax
from jax.experimental import pallas as pl
from jax.experimental.pallas import tpu as pltpu
from jax.sharding import PartitionSpec as P

MESH = pl.DeviceIdType.MESH
STEPS = 4
K = 6
TILES = 8
LANES = 128
X_CHIPS = 4
DT = 0.1
BUOYANCY = 0.5
DRAG = 0.5

_LANE_GATHER = lax.GatherDimensionNumbers(
    offset_dims=(),
    collapsed_slice_dims=(1,),
    start_index_map=(1,),
    operand_batching_dims=(0,),
    start_indices_batching_dims=(0,),
)


def lane_gather(x, idx):
    return lax.gather(
        x, idx[..., None], _LANE_GATHER, (1, 1), mode=lax.GatherScatterMode.PROMISE_IN_BOUNDS
    )


def far_first(count, start=1):
    return sorted(range(start, count), key=lambda d: -min(d, count - d))


def when(condition):
    if isinstance(condition, bool):
        return lambda act: act() if condition else None
    return pl.when(condition)


def wide(row):
    return jnp.broadcast_to(row, (8, LANES))


def kernel(
    n_space,
    n_level,
    vel_hbm,
    rho_hbm,
    eta_hbm,
    grad_hbm,
    lap_hbm,
    cor_hbm,
    area_hbm,
    thick_hbm,
    send_hbm,
    nb_hbm,
    bot_hbm,
    vel_out,
    rho_out,
    eta_out,
    drift_out,
    vel_ref,
    rho_ref,
    eta_ref,
    grad_ref,
    lap_ref,
    cor_ref,
    area_ref,
    thick_ref,
    send_ref,
    nb_ref,
    bot_ref,
    isem,
    nbc,
    wts,
    bots,
    cors,
    x,
    r,
    part,
    near,
    q,
    dq,
    eta,
    etah,
    vv,
    lsend,
    lrecv,
    usend,
    urecv,
    rsend,
    rrecv,
    gsend,
    grecv,
    ssend,
    srecv,
    zsend,
    zrecv,
    xsend,
    xrecv,
    split,
    coef,
    bsend,
    brecv,
    lsem,
    usem,
    rsem,
    gsem,
    ssem,
    bsem,
    zsem,
    tok,
):
    p = lax.axis_index("space")
    g = lax.axis_index("level")
    n_z = n_space // X_CHIPS
    up = lax.rem(p + 1, n_space)
    down = lax.rem(p + n_space - 1, n_space)
    level_peers = [lax.rem(g + d, n_level) for d in range(n_level)]

    def z_peer(d):
        return lax.rem(p + d * X_CHIPS, n_space)

    px = lax.rem(p, X_CHIPS)
    x_peers = [p - px + lax.rem(px + d, X_CHIPS) for d in range(X_CHIPS)]
    plane = [(a, b) for a in range(X_CHIPS) for b in range(n_level) if a or b]
    plane.sort(key=lambda ab: -2 * min(ab[0], X_CHIPS - ab[0]) - min(ab[1], n_level - ab[1]))

    barrier = pltpu.get_barrier_semaphore()
    count = 0

    def greet(a, b):
        pl.semaphore_signal(barrier, inc=1, device_id=(a, b), device_id_type=MESH)

    for d in far_first(n_level, 0):
        greet(up, level_peers[d])
        greet(down, level_peers[d])
        count += 2
        if d:
            greet(p, level_peers[d])
            count += 1

    inputs = [
        (send_hbm, send_ref),
        (vel_hbm, vel_ref),
        (bot_hbm, bot_ref),
        (rho_hbm, rho_ref),
        (thick_hbm, thick_ref),
        (eta_hbm, eta_ref),
        (nb_hbm, nb_ref),
        (grad_hbm, grad_ref),
        (lap_hbm, lap_ref),
        (cor_hbm, cor_ref),
        (area_hbm, area_ref),
    ]
    loads = [pltpu.make_async_copy(a, b, isem.at[i]) for i, (a, b) in enumerate(inputs)]
    for load in loads:
        load.start()

    sub = lax.broadcasted_iota(jnp.int32, (8, LANES), 0)
    lane = lax.broadcasted_iota(jnp.int32, (8, LANES), 1)
    level_id = sub + g * 8
    for load in loads[:5]:
        load.wait()
    th = jnp.zeros((8, LANES), jnp.float32)
    for l in range(8):
        th = jnp.where(sub == l, thick_ref[l], th)
    send_idx = [send_ref[:, side * LANES : (side + 1) * LANES] for side in range(2)]
    send_lane = [wide(i & (LANES - 1)) for i in send_idx]
    send_tile = [wide(i >> 7) for i in send_idx]

    def listed_levels(tiles, side):
        out = lane_gather(tiles[0], send_lane[side])
        for t in range(1, TILES):
            out = jnp.where(send_tile[side] == t, lane_gather(tiles[t], send_lane[side]), out)
        return out

    def listed_nodes(compact, side):
        got = lane_gather(compact, send_lane[side])
        here = jnp.where(send_tile[side] == sub, got, jnp.zeros_like(got))
        return jnp.sum(here, axis=0, keepdims=True)

    def column(density):
        weighted = density * th
        total = weighted
        for shift in (1, 2, 4):
            total = total + jnp.where(sub >= shift, pltpu.roll(total, shift, 0), 0.0)
        return BUOYANCY * (total - 0.5 * weighted)

    def copy(src, dst, sems, i, a, b):
        return pltpu.make_async_remote_copy(
            src_ref=src,
            dst_ref=dst,
            send_sem=sems.at[0, i],
            recv_sem=sems.at[1, i],
            device_id=(a, b),
            device_id_type=MESH,
        )

    def arrived(buf, sems, i):
        pltpu.make_async_copy(buf, buf, sems.at[1, i]).wait()

    def left(buf, sems, i):
        pltpu.make_async_copy(buf, buf, sems.at[0, i]).wait()

    def send_token(i):
        for d in (2**i, n_space - 2**i):
            there = (lax.rem(p + d, n_space), g)
            pl.semaphore_signal(tok.at[i], inc=1, device_id=there, device_id_type=MESH)

    def pass_token(i):
        pl.semaphore_wait(tok.at[i - 1], 2)
        send_token(i)

    def list_velocity(s):
        for side in range(2):
            for c in range(2):
                usend[s, side, c] = listed_levels([x[c, d] for d in range(TILES)], side)

    def send_velocity(s):
        copy(usend.at[s, 0], urecv.at[s, 1], usem, s, down, g).start()
        copy(usend.at[s, 1], urecv.at[s, 0], usem, s, up, g).start()

    def list_density(s, par):
        tiles = [r[par, d] for d in range(TILES)]
        for side in range(2):
            got = listed_levels(tiles, side)
            rsend[s, side] = got
            gsend[s, side, 0:1] = jnp.sum(got * th, axis=0, keepdims=True)
        for d in range(TILES):
            lsend[s, 0, d : d + 1] = jnp.sum(tiles[d] * th, axis=0, keepdims=True)

    def send_density(s):
        copy(rsend.at[s, 0], rrecv.at[s, 1], rsem, s, down, g).start()
        copy(rsend.at[s, 1], rrecv.at[s, 0], rsem, s, up, g).start()

    def send_sums(s):
        for d in far_first(n_level, 0):
            copy(gsend.at[s, 0], grecv.at[s, 1, d], gsem, s, down, level_peers[d]).start()
            copy(gsend.at[s, 1], grecv.at[s, 0, d], gsem, s, up, level_peers[d]).start()

    def send_level(s):
        for d in far_first(n_level):
            copy(lsend.at[s], lrecv.at[s, d - 1], lsem, s, p, level_peers[d]).start()

    for d in range(TILES):
        cols = slice(d * LANES, (d + 1) * LANES)
        wet = level_id < wide(bot_ref[d : d + 1])
        for c in range(2):
            x[c, d] = jnp.where(wet, vel_ref[c, :, cols], 0.0)
        r[0, d] = rho_ref[:, cols]
    list_velocity(0)
    list_density(0, 0)
    lsend[0, 1] = jnp.zeros((8, LANES), jnp.float32)
    for side in range(2):
        gsend[0, side, 1:2] = jnp.zeros((1, LANES), jnp.float32)
    loads[5].wait()
    wet_nodes = (bot_ref[...] > 0).astype(jnp.float32)
    eta[...] = eta_ref[...]
    for side in range(2):
        ssend[side, 0:1] = listed_nodes(eta_ref[...], side)
        ssend[side, 1:2] = listed_nodes(wet_nodes, side)

    pl.semaphore_wait(barrier, count)
    send_sums(0)
    send_density(0)
    send_velocity(0)
    send_level(0)
    copy(ssend.at[0], srecv.at[1], ssem, 0, down, g).start()
    copy(ssend.at[1], srecv.at[0], ssem, 0, up, g).start()
    send_token(0)

    for load in loads[6:]:
        load.wait()
    bots[0:8] = bot_ref[...]
    cors[0:8] = cor_ref[...]
    for k in range(K):
        for d in range(TILES):
            cols = slice(d * LANES, (d + 1) * LANES)
            row = slice(d, d + 1)
            nbc[k, row] = nb_ref[k : k + 1, cols]
            wts[0, k, row] = grad_ref[k, 0:1, cols]
            wts[1, k, row] = grad_ref[k, 1:2, cols]
            wts[2, k, row] = lap_ref[k : k + 1, cols]
        tile = nbc[k, 0:8] >> 7
        below = jnp.where(p > 0, 1.0, 0.0)
        above = jnp.where(p < n_space - 1, 1.0, 0.0)
        valid = jnp.where(tile == TILES, below, jnp.where(tile == TILES + 1, above, 1.0))
        nbc[k, 8:16] = jnp.zeros((8, LANES), jnp.int32)
        for j in range(3):
            wts[j, k, 0:8] = wts[j, k, 0:8] * valid
            wts[j, k, 8:16] = jnp.zeros((8, LANES), jnp.float32)
        for side in range(2):
            row = slice(8 + side, 9 + side)
            nbc[k, row] = listed_nodes(nbc[k, 0:8], side)
            for j in range(3):
                wts[j, k, row] = listed_nodes(wts[j, k, 0:8], side)
    for side in range(2):
        row = slice(8 + side, 9 + side)
        bots[row] = listed_nodes(bot_ref[...], side)
        cors[row] = listed_nodes(cor_ref[...], side)
    lists = (TILES, TILES + 1)

    def slots(k, d):
        row = wide(nbc[k, d : d + 1])
        return row & (LANES - 1), row >> 7

    def weights(k, d):
        return [wide(wts[j, k, d : d + 1]) for j in range(3)]

    def gather_own(par, dests):
        for d in dests:
            for k in range(K):
                idx, tile = slots(k, d)
                outs = [None] * 3
                for t in range(TILES):
                    hit = tile == t
                    for f, a in enumerate((x[0, t], x[1, t], r[par, t])):
                        got = lane_gather(a, idx)
                        outs[f] = jnp.where(hit, got, outs[f]) if t else got
                for f in range(3):
                    near[f, d * K + k] = outs[f]

    def with_halo(fields, halo, idx, tile, at):
        outs = [near[f, at] for f in fields]
        for side in range(2):
            hit = tile == TILES + side
            outs = [jnp.where(hit, lane_gather(a, idx), o) for a, o in zip(halo[side], outs)]
        return outs

    def velocity_of(s, d):
        if d >= TILES:
            return usend[s, d - TILES, 0], usend[s, d - TILES, 1]
        return x[0, d], x[1, d]

    def density_terms(s, par, dests):
        halo = [(rrecv[s, side],) for side in range(2)]
        for d in dests:
            own = rsend[s, d - TILES] if d >= TILES else r[par, d]
            zero = jnp.zeros((8, LANES), jnp.float32)
            lr, dxr, dyr = [zero] * 3
            for k in range(K):
                idx, tile = slots(k, d)
                (near_r,) = with_halo((2,), halo, idx, tile, d * K + k)
                dr = near_r - own
                we, wn, wl = weights(k, d)
                lr += wl * dr
                dxr += we * dr
                dyr += wn * dr
            u, v = velocity_of(s, d)
            cor = wide(cors[d : d + 1])
            drag = jnp.where(level_id == wide(bots[d : d + 1]) - 1, DRAG, 0.0)
            part[0, d] = u + DT * (cor * v - column(dxr) - drag * u)
            part[1, d] = v - DT * (cor * u + column(dyr) + drag * v)
            new = own + DT * (lr - u * dxr - v * dyr)
            if d >= TILES:
                rsend[s + 1, d - TILES] = new
                gsend[s + 1, d - TILES, 0:1] = jnp.sum(new * th, axis=0, keepdims=True)
            else:
                r[1 - par, d] = new
                lsend[s + 1, 0, d : d + 1] = jnp.sum(new * th, axis=0, keepdims=True)

    def velocity_terms(s, dests):
        halo = [[urecv[s, side, c] for c in range(2)] for side in range(2)]
        for d in dests:
            u, v = velocity_of(s, d)
            zero = jnp.zeros((8, LANES), jnp.float32)
            dxu, dyv, lu, lv = [zero] * 4
            for k in range(K):
                idx, tile = slots(k, d)
                near_u, near_v = with_halo((0, 1), halo, idx, tile, d * K + k)
                we, wn, wl = weights(k, d)
                du, dv = near_u - u, near_v - v
                dxu += we * du
                dyv += wn * dv
                lu += wl * du
                lv += wl * dv
            part[0, d] = part[0, d] + DT * lu
            part[1, d] = part[1, d] + DT * lv
            div = jnp.sum(th * (dxu + dyv), axis=0, keepdims=True)
            if d >= TILES:
                gsend[s + 1, d - TILES, 1:2] = div
            else:
                lsend[s + 1, 1, d : d + 1] = div

    def find_q(s):
        arrived(lrecv.at[s], lsem, s)
        arrived(grecv.at[s], gsem, s)
        div, mass = lsend[s, 1], jnp.zeros((8, LANES), jnp.float32)
        for d in range(1, n_level):
            mass = mass + jnp.where(g >= d, lrecv[s, d - 1, 0], 0.0)
            div = div + lrecv[s, d - 1, 1]
        new_eta = eta[...] - DT * wet_nodes * div
        eta[...] = new_eta
        q[0:8] = new_eta + BUOYANCY * mass
        for side in range(2):
            row = slice(side, side + 1)
            m = jnp.zeros((1, LANES), jnp.float32)
            h = grecv[s, side, 0, 1:2]
            for d in range(1, n_level):
                m = m + jnp.where(g >= d, grecv[s, side, d, 0:1], 0.0)
                h = h + grecv[s, side, d, 1:2]
            e = etah[row] - DT * srecv[side, 1:2] * h
            etah[row] = e
            q[8 + side : 9 + side] = e + BUOYANCY * m

    def shared_terms(dests):
        listed = dests[0] >= TILES
        rows = slice(8, 16) if listed else slice(0, 8)
        own = q[0:8]
        if listed:
            first, second = [wide(listed_nodes(own, side)) for side in range(2)]
            own = jnp.where(sub == 0, first, second)
        dx = jnp.zeros((8, LANES), jnp.float32)
        dy = dx
        source = [wide(q[t : t + 1]) for t in range(TILES + 2)]
        for k in range(K):
            slot = nbc[k, rows]
            idx, tile = slot & (LANES - 1), slot >> 7
            n = lane_gather(source[0], idx)
            for t in range(1, TILES + 2):
                n = jnp.where(tile == t, lane_gather(source[t], idx), n)
            diff = n - own
            dx = dx + wts[0, k, rows] * diff
            dy = dy + wts[1, k, rows] * diff
        dq[0, rows] = DT * dx
        dq[1, rows] = DT * dy

    def new_velocity(d, c):
        wet = level_id < wide(bots[d : d + 1])
        return jnp.where(wet, part[c, d] - wide(dq[c, d : d + 1]), 0.0)

    def drift_weights():
        area = area_ref[...] * wet_nodes
        own = [jnp.zeros((8, LANES), jnp.float32)] * 2
        for k in range(K):
            for j in range(2):
                term = area * wts[j, k, 0:8]
                own[j] = own[j] + term
                for i in range(3):
                    short = term.astype(jnp.bfloat16).astype(jnp.float32)
                    split[i, j, k] = short
                    term = term - short
        target = jnp.where(sub < 2, sub + TILES, jnp.where(sub < 4, sub + TILES - 2, -1))
        slot_lane = lax.broadcasted_iota(jnp.int32, (LANES, LANES), 0)
        total = jnp.zeros((72, LANES), jnp.float32)
        for k in range(K):
            for d in range(0, TILES, 2):
                left_side, right_side = [], []
                for e in (d, d + 1):
                    row = nbc[k, e : e + 1]
                    tile = wide(row >> 7)
                    hit, far = tile == sub, tile == target
                    pieces = []
                    for i in range(3):
                        we, wn = [wide(split[i, j, k, e : e + 1]) for j in range(2)]
                        pieces.append(jnp.where(hit, we, 0.0))
                        pieces.append(jnp.where(hit, wn, 0.0))
                        pieces.append(jnp.where(far, jnp.where(sub < 2, we, wn), 0.0))
                    left_side.append(jnp.concatenate(pieces, axis=0))
                    same = jnp.broadcast_to(row & (LANES - 1), (LANES, LANES)) == slot_lane
                    right_side.append(jnp.where(same, 1.0, 0.0))
                total = total + lax.dot_general(
                    jnp.concatenate(left_side, axis=1).astype(jnp.bfloat16),
                    jnp.concatenate(right_side, axis=1).astype(jnp.bfloat16),
                    (((1,), (1,)), ((), ())),
                    preferred_element_type=jnp.float32,
                )
        total = total[0:24] + total[24:48] + total[48:72]
        for j in range(2):
            coef[j] = total[8 * j : 8 * j + 8] - own[j]
            for side in range(2):
                bsend[side, j : j + 1] = total[16 + 2 * j + side : 17 + 2 * j + side]
        copy(bsend.at[0], brecv.at[1], bsem, 0, down, g).start()
        copy(bsend.at[1], brecv.at[0], bsem, 0, up, g).start()

    def early_drift():
        arrived(brecv, bsem, 0)
        total = jnp.zeros((8, LANES), jnp.float32)
        for j in range(2):
            for d in range(TILES):
                total = total + wide(coef[j, d : d + 1]) * x[j, d]
            for side in range(2):
                total = total + wide(brecv[side, j : j + 1]) * usend[STEPS - 1, side, j]
        return total * th

    def send_drift():
        sums = jnp.zeros((8, LANES), jnp.float32)
        terms = [vv[s] for s in range(STEPS - 1)]
        terms += [early_drift(), area_ref[...] * wet_nodes * (1.0 / n_level)]
        for j, term in enumerate(terms):
            sums = jnp.where(sub == j, wide(jnp.sum(term, axis=0, keepdims=True)), sums)
        sums = jnp.broadcast_to(jnp.sum(sums, axis=1, keepdims=True), (8, LANES))
        zsend[...] = jnp.sum(jnp.where(sub == lane, sums, 0.0), axis=0, keepdims=True)
        pl.semaphore_wait(tok.at[4], 2)
        for d in far_first(n_z):
            copy(zsend, zrecv.at[d - 1], zsem, 0, z_peer(d), g).start()

    def step(s, _):
        par = lax.rem(s, 2)
        final = s == STEPS - 2 if isinstance(s, int) else False

        @when(s == 1)
        def _():
            pass_token(3)

        gather_own(par, (*lists, *range(TILES)))

        @when(s == 0)
        def _():
            pass_token(1)
            drift_weights()

        arrived(rrecv.at[s], rsem, s)
        density_terms(s, par, lists)
        send_density(s + 1)
        density_terms(s, par, range(TILES))

        @when(s == 0)
        def _():
            pass_token(2)
            arrived(srecv, ssem, 0)
            etah[...] = srecv[:, 0]

        @when(s == 1)
        def _():
            pass_token(4)

        arrived(urecv.at[s], usem, s)
        velocity_terms(s, lists)
        if not final:
            send_sums(s + 1)
        find_q(s)
        shared_terms(lists)
        for side in range(2):
            for c in range(2):
                usend[s + 1, side, c] = new_velocity(TILES + side, c)
        if not final:
            send_velocity(s + 1)
        velocity_terms(s, range(TILES))
        if not final:
            send_level(s + 1)
        vv[s] = area_ref[...] * wet_nodes * lsend[s + 1, 1]
        shared_terms(range(TILES))
        for d in range(TILES):
            for c in range(2):
                x[c, d] = new_velocity(d, c)
        if final:
            send_drift()
            send_velocity(s + 1)
            send_sums(s + 1)
            send_level(s + 1)
        return 0

    lax.fori_loop(0, STEPS - 2, step, 0)
    step(STEPS - 2, 0)
    last = STEPS - 1
    par = last % 2
    gather_own(par, range(TILES))
    arrived(rrecv.at[last], rsem, last)
    density_terms(last, par, range(TILES))
    for d in range(TILES):
        rho_out[:, d * LANES : (d + 1) * LANES] = r[1 - par, d]
    arrived(urecv.at[last], usem, last)
    velocity_terms(last, range(TILES))
    send_level(STEPS)
    find_q(last)
    shared_terms(range(TILES))
    for d in range(TILES):
        for c in range(2):
            vel_out[c, :, d * LANES : (d + 1) * LANES] = new_velocity(d, c)

    arrived(zrecv, zsem, 0)
    row = zsend[...]
    for d in range(1, n_z):
        row = row + zrecv[d - 1]
    xsend[...] = row
    for i, (a, b) in enumerate(plane):
        copy(xsend, xrecv.at[i], zsem, 1, x_peers[a], level_peers[b]).start()

    arrived(lrecv.at[STEPS], lsem, STEPS)
    div = lsend[STEPS, 1]
    for d in range(1, n_level):
        div = div + lrecv[STEPS, d - 1, 1]
    eta[...] = eta[...] - DT * wet_nodes * div

    for s in range(STEPS + 1):
        left(lrecv.at[s], lsem, s)
    for s in range(STEPS):
        left(usend.at[s], usem, s)
        left(rsend.at[s], rsem, s)
        left(grecv.at[s], gsem, s)
    left(ssend, ssem, 0)
    left(bsend, bsem, 0)
    left(zrecv, zsem, 0)

    arrived(xrecv, zsem, 1)
    for i in range(len(plane)):
        row = row + xrecv[i]
    lane_row = lane[0:1]
    total = jnp.sum(jnp.where(lane_row == STEPS, row, 0.0), axis=1, keepdims=True)
    drift_sum = jnp.sum(jnp.where(lane_row < STEPS, row, 0.0), axis=1, keepdims=True)
    drift_out[...] = jnp.where(lane_row < STEPS, row / total, 0.0)
    eta_out[...] = eta[...] + DT * (drift_sum / total)
    left(xrecv, zsem, 1)


def finish(vel, rho, eta, drift, vel_out, rho_out, eta_out, drift_out, sem):
    copies = [
        pltpu.make_async_copy(a, b, sem.at[i])
        for i, (a, b) in enumerate(((vel, vel_out), (rho, rho_out), (eta, eta_out)))
    ]
    for c in copies:
        c.start()
    drift_out[...] = drift[0, :STEPS]
    for c in copies:
        c.wait()


def solution(mesh):
    n_space, n_level = mesh.shape["space"], mesh.shape["level"]

    def local(
        velocity,
        density,
        elevation,
        grad_weights,
        lap_weights,
        coriolis,
        node_area,
        thickness,
        send_list,
        neighbours,
        bottom,
    ):
        f32, i32 = jnp.float32, jnp.int32
        compact = (TILES, LANES)
        vmem = pl.BlockSpec(memory_space=pltpu.VMEM)
        dma = pltpu.SemaphoreType.DMA
        peers = n_level - 1
        n_z = n_space // X_CHIPS
        row = (1, LANES)
        inputs = [
            pltpu.VMEM(velocity.shape, f32),
            pltpu.VMEM(density.shape, f32),
            pltpu.VMEM(compact, f32),
            pltpu.VMEM((K, 2, TILES * LANES), f32),
            pltpu.VMEM(lap_weights.shape, f32),
            pltpu.VMEM(compact, f32),
            pltpu.VMEM(compact, f32),
            pltpu.SMEM(thickness.shape, f32),
            pltpu.VMEM(send_list.shape, i32),
            pltpu.VMEM(neighbours.shape, i32),
            pltpu.VMEM(compact, i32),
            dma((11,)),
            pltpu.VMEM((K, 16, LANES), i32),
        ]
        shapes = [
            (2, 8, 8, LANES),
            (2, 8, 8, LANES),
            (2, 10, 8, LANES),
            (3, 60, 8, LANES),
            (16, LANES),
            (2, 16, LANES),
            (8, LANES),
            (2, LANES),
            (STEPS, 8, LANES),
            (STEPS + 1, 2, 8, LANES),
            (STEPS + 1, peers, 2, 8, LANES),
            (STEPS, 2, 2, 8, LANES),
            (STEPS, 2, 2, 8, LANES),
            (STEPS, 2, 8, LANES),
            (STEPS, 2, 8, LANES),
            (STEPS, 2, 2, LANES),
            (STEPS, 2, n_level, 2, LANES),
            (2, 2, LANES),
            (2, 2, LANES),
            row,
            (n_z - 1, *row),
            row,
            (X_CHIPS * n_level - 1, *row),
            (3, 2, K, 8, LANES),
            (2, 8, LANES),
            (2, 2, LANES),
            (2, 2, LANES),
        ]

        def body(*refs):
            kernel(n_space, n_level, *refs)

        vel, rho, eta, drift = pl.pallas_call(
            body,
            out_shape=(
                pltpu.VMEM(velocity.shape, f32),
                pltpu.VMEM(density.shape, f32),
                pltpu.VMEM(compact, f32),
                pltpu.VMEM((1, LANES), f32),
            ),
            in_specs=[pl.BlockSpec(memory_space=pl.ANY)] * 11,
            out_specs=(vmem,) * 4,
            scratch_shapes=inputs
            + [pltpu.VMEM((3, K, 16, LANES), f32)]
            + [pltpu.VMEM((16, LANES), i32), pltpu.VMEM((16, LANES), f32)]
            + [pltpu.VMEM(shape, f32) for shape in shapes]
            + [
                dma((2, 5)),
                dma((2, 4)),
                dma((2, 4)),
                dma((2, 4)),
                dma((2, 1)),
                dma((2, 1)),
                dma((2, 2)),
                pltpu.SemaphoreType.REGULAR((5,)),
            ],
            compiler_params=pltpu.CompilerParams(collective_id=0, has_side_effects=True),
        )(
            velocity,
            density,
            elevation.reshape(compact),
            jnp.swapaxes(grad_weights, 0, 1),
            lap_weights,
            coriolis.reshape(compact),
            node_area.reshape(compact),
            thickness,
            send_list,
            neighbours,
            bottom.reshape(compact),
        )
        results = [pltpu.with_memory_space_constraint(a, pltpu.VMEM) for a in (vel, rho, eta, drift)]
        vel, rho, eta, drift = pl.pallas_call(
            finish,
            out_shape=(
                jax.ShapeDtypeStruct(velocity.shape, f32),
                jax.ShapeDtypeStruct(density.shape, f32),
                jax.ShapeDtypeStruct(compact, f32),
                jax.ShapeDtypeStruct((STEPS,), f32),
            ),
            in_specs=[vmem] * 4,
            out_specs=(pl.BlockSpec(memory_space=pl.ANY),) * 3 + (vmem,),
            scratch_shapes=[dma((3,))],
        )(*results)
        return vel, rho, eta.reshape(elevation.shape), drift

    return jax.shard_map(
        local,
        mesh=mesh,
        in_specs=(
            P(None, "level", "space"),
            P("level", "space"),
            P("space"),
            P(None, None, "space"),
            P(None, "space"),
            P("space"),
            P("space"),
            P("level"),
            P("space", None),
            P(None, "space"),
            P("space"),
        ),
        out_specs=(P(None, "level", "space"), P("level", "space"), P("space"), P()),
        check_vma=False,
    )
```

```python
import jax
import jax.numpy as jnp
from jax import lax
from jax.experimental import pallas as pl
from jax.experimental.pallas import tpu as pltpu
from jax.sharding import PartitionSpec as P

MESH = pl.DeviceIdType.MESH
STEPS = 4
K = 6
TILES = 8
LANES = 128
X_CHIPS = 4
DT = 0.1
BUOYANCY = 0.5
DRAG = 0.5

_LANE_GATHER = lax.GatherDimensionNumbers(
    offset_dims=(),
    collapsed_slice_dims=(1,),
    start_index_map=(1,),
    operand_batching_dims=(0,),
    start_indices_batching_dims=(0,),
)


def lane_gather(x, idx):
    return lax.gather(
        x, idx[..., None], _LANE_GATHER, (1, 1), mode=lax.GatherScatterMode.PROMISE_IN_BOUNDS
    )


def far_first(count, start=1):
    return sorted(range(start, count), key=lambda d: -min(d, count - d))


def when(condition):
    if isinstance(condition, bool):
        return lambda act: act() if condition else None
    return pl.when(condition)


def wide(row):
    return jnp.broadcast_to(row, (8, LANES))


def kernel(
    n_space,
    n_level,
    vel_hbm,
    rho_hbm,
    eta_hbm,
    grad_hbm,
    lap_hbm,
    cor_hbm,
    area_hbm,
    thick_hbm,
    send_hbm,
    nb_hbm,
    bot_hbm,
    vel_out,
    rho_out,
    eta_out,
    drift_out,
    vel_ref,
    rho_ref,
    eta_ref,
    grad_ref,
    lap_ref,
    cor_ref,
    area_ref,
    thick_ref,
    send_ref,
    nb_ref,
    bot_ref,
    isem,
    nbc,
    wts,
    bots,
    cors,
    x,
    r,
    part,
    near,
    q,
    dq,
    eta,
    etah,
    vv,
    lsend,
    lrecv,
    usend,
    urecv,
    rsend,
    rrecv,
    gsend,
    grecv,
    ssend,
    srecv,
    zsend,
    zrecv,
    xsend,
    xrecv,
    split,
    coef,
    bsend,
    brecv,
    lsem,
    usem,
    rsem,
    gsem,
    ssem,
    bsem,
    zsem,
    tok,
):
    p = lax.axis_index("space")
    g = lax.axis_index("level")
    n_z = n_space // X_CHIPS
    up = lax.rem(p + 1, n_space)
    down = lax.rem(p + n_space - 1, n_space)
    level_peers = [lax.rem(g + d, n_level) for d in range(n_level)]

    def z_peer(d):
        return lax.rem(p + d * X_CHIPS, n_space)

    px = lax.rem(p, X_CHIPS)
    x_peers = [p - px + lax.rem(px + d, X_CHIPS) for d in range(X_CHIPS)]
    plane = [(a, b) for a in range(X_CHIPS) for b in range(n_level) if a or b]
    plane.sort(key=lambda ab: -2 * min(ab[0], X_CHIPS - ab[0]) - min(ab[1], n_level - ab[1]))

    barrier = pltpu.get_barrier_semaphore()
    count = 0

    def greet(a, b):
        pl.semaphore_signal(barrier, inc=1, device_id=(a, b), device_id_type=MESH)

    for d in far_first(n_level, 0):
        greet(up, level_peers[d])
        greet(down, level_peers[d])
        count += 2
        if d:
            greet(p, level_peers[d])
            count += 1

    inputs = [
        (send_hbm, send_ref),
        (vel_hbm, vel_ref),
        (bot_hbm, bot_ref),
        (rho_hbm, rho_ref),
        (thick_hbm, thick_ref),
        (eta_hbm, eta_ref),
        (nb_hbm, nb_ref),
        (grad_hbm, grad_ref),
        (lap_hbm, lap_ref),
        (cor_hbm, cor_ref),
        (area_hbm, area_ref),
    ]
    loads = [pltpu.make_async_copy(a, b, isem.at[i]) for i, (a, b) in enumerate(inputs)]
    for load in loads:
        load.start()

    sub = lax.broadcasted_iota(jnp.int32, (8, LANES), 0)
    lane = lax.broadcasted_iota(jnp.int32, (8, LANES), 1)
    level_id = sub + g * 8
    for load in loads[:5]:
        load.wait()
    th = jnp.zeros((8, LANES), jnp.float32)
    for l in range(8):
        th = jnp.where(sub == l, thick_ref[l], th)
    send_idx = [send_ref[:, side * LANES : (side + 1) * LANES] for side in range(2)]
    send_lane = [wide(i & (LANES - 1)) for i in send_idx]
    send_tile = [wide(i >> 7) for i in send_idx]

    def listed_levels(tiles, side):
        out = lane_gather(tiles[0], send_lane[side])
        for t in range(1, TILES):
            out = jnp.where(send_tile[side] == t, lane_gather(tiles[t], send_lane[side]), out)
        return out

    def listed_nodes(compact, side):
        got = lane_gather(compact, send_lane[side])
        here = jnp.where(send_tile[side] == sub, got, jnp.zeros_like(got))
        return jnp.sum(here, axis=0, keepdims=True)

    def column(density):
        weighted = density * th
        total = weighted
        for shift in (1, 2, 4):
            total = total + jnp.where(sub >= shift, pltpu.roll(total, shift, 0), 0.0)
        return BUOYANCY * (total - 0.5 * weighted)

    def copy(src, dst, sems, i, a, b):
        return pltpu.make_async_remote_copy(
            src_ref=src,
            dst_ref=dst,
            send_sem=sems.at[0, i],
            recv_sem=sems.at[1, i],
            device_id=(a, b),
            device_id_type=MESH,
        )

    def arrived(buf, sems, i):
        pltpu.make_async_copy(buf, buf, sems.at[1, i]).wait()

    def left(buf, sems, i):
        pltpu.make_async_copy(buf, buf, sems.at[0, i]).wait()

    def send_token(i):
        for d in (2**i, n_space - 2**i):
            there = (lax.rem(p + d, n_space), g)
            pl.semaphore_signal(tok.at[i], inc=1, device_id=there, device_id_type=MESH)

    def pass_token(i):
        pl.semaphore_wait(tok.at[i - 1], 2)
        send_token(i)

    def list_velocity(s):
        for side in range(2):
            for c in range(2):
                usend[s, side, c] = listed_levels([x[c, d] for d in range(TILES)], side)

    def send_velocity(s):
        copy(usend.at[s, 0], urecv.at[s, 1], usem, s, down, g).start()
        copy(usend.at[s, 1], urecv.at[s, 0], usem, s, up, g).start()

    def list_density(s, par):
        tiles = [r[par, d] for d in range(TILES)]
        for side in range(2):
            got = listed_levels(tiles, side)
            rsend[s, side] = got
            gsend[s, side, 0:1] = jnp.sum(got * th, axis=0, keepdims=True)
        for d in range(TILES):
            lsend[s, 0, d : d + 1] = jnp.sum(tiles[d] * th, axis=0, keepdims=True)

    def send_density(s):
        copy(rsend.at[s, 0], rrecv.at[s, 1], rsem, s, down, g).start()
        copy(rsend.at[s, 1], rrecv.at[s, 0], rsem, s, up, g).start()

    def send_sums(s):
        for d in far_first(n_level, 0):
            copy(gsend.at[s, 0], grecv.at[s, 1, d], gsem, s, down, level_peers[d]).start()
            copy(gsend.at[s, 1], grecv.at[s, 0, d], gsem, s, up, level_peers[d]).start()

    def send_level(s):
        for d in far_first(n_level):
            copy(lsend.at[s], lrecv.at[s, d - 1], lsem, s, p, level_peers[d]).start()

    for d in range(TILES):
        cols = slice(d * LANES, (d + 1) * LANES)
        wet = level_id < wide(bot_ref[d : d + 1])
        for c in range(2):
            x[c, d] = jnp.where(wet, vel_ref[c, :, cols], 0.0)
        r[0, d] = rho_ref[:, cols]
    list_velocity(0)
    list_density(0, 0)
    lsend[0, 1] = jnp.zeros((8, LANES), jnp.float32)
    for side in range(2):
        gsend[0, side, 1:2] = jnp.zeros((1, LANES), jnp.float32)
    loads[5].wait()
    wet_nodes = (bot_ref[...] > 0).astype(jnp.float32)
    eta[...] = eta_ref[...]
    for side in range(2):
        ssend[side, 0:1] = listed_nodes(eta_ref[...], side)
        ssend[side, 1:2] = listed_nodes(wet_nodes, side)

    pl.semaphore_wait(barrier, count)
    send_sums(0)
    send_density(0)
    send_velocity(0)
    send_level(0)
    copy(ssend.at[0], srecv.at[1], ssem, 0, down, g).start()
    copy(ssend.at[1], srecv.at[0], ssem, 0, up, g).start()
    send_token(0)

    for load in loads[6:]:
        load.wait()
    bots[0:8] = bot_ref[...]
    cors[0:8] = cor_ref[...]
    for k in range(K):
        for d in range(TILES):
            cols = slice(d * LANES, (d + 1) * LANES)
            row = slice(d, d + 1)
            nbc[k, row] = nb_ref[k : k + 1, cols]
            wts[0, k, row] = grad_ref[k, 0:1, cols]
            wts[1, k, row] = grad_ref[k, 1:2, cols]
            wts[2, k, row] = lap_ref[k : k + 1, cols]
        tile = nbc[k, 0:8] >> 7
        below = jnp.where(p > 0, 1.0, 0.0)
        above = jnp.where(p < n_space - 1, 1.0, 0.0)
        valid = jnp.where(tile == TILES, below, jnp.where(tile == TILES + 1, above, 1.0))
        nbc[k, 8:16] = jnp.zeros((8, LANES), jnp.int32)
        for j in range(3):
            wts[j, k, 0:8] = wts[j, k, 0:8] * valid
            wts[j, k, 8:16] = jnp.zeros((8, LANES), jnp.float32)
        for side in range(2):
            row = slice(8 + side, 9 + side)
            nbc[k, row] = listed_nodes(nbc[k, 0:8], side)
            for j in range(3):
                wts[j, k, row] = listed_nodes(wts[j, k, 0:8], side)
    for side in range(2):
        row = slice(8 + side, 9 + side)
        bots[row] = listed_nodes(bot_ref[...], side)
        cors[row] = listed_nodes(cor_ref[...], side)
    lists = (TILES, TILES + 1)

    def slots(k, d):
        row = wide(nbc[k, d : d + 1])
        return row & (LANES - 1), row >> 7

    def weights(k, d):
        return [wide(wts[j, k, d : d + 1]) for j in range(3)]

    def gather_own(par, dests):
        for d in dests:
            for k in range(K):
                idx, tile = slots(k, d)
                outs = [None] * 3
                for t in range(TILES):
                    hit = tile == t
                    for f, a in enumerate((x[0, t], x[1, t], r[par, t])):
                        got = lane_gather(a, idx)
                        outs[f] = jnp.where(hit, got, outs[f]) if t else got
                for f in range(3):
                    near[f, d * K + k] = outs[f]

    def with_halo(fields, halo, idx, tile, at):
        outs = [near[f, at] for f in fields]
        for side in range(2):
            hit = tile == TILES + side
            outs = [jnp.where(hit, lane_gather(a, idx), o) for a, o in zip(halo[side], outs)]
        return outs

    def velocity_of(s, d):
        if d >= TILES:
            return usend[s, d - TILES, 0], usend[s, d - TILES, 1]
        return x[0, d], x[1, d]

    def density_terms(s, par, dests):
        halo = [(rrecv[s, side],) for side in range(2)]
        for d in dests:
            own = rsend[s, d - TILES] if d >= TILES else r[par, d]
            zero = jnp.zeros((8, LANES), jnp.float32)
            lr, dxr, dyr = [zero] * 3
            for k in range(K):
                idx, tile = slots(k, d)
                (near_r,) = with_halo((2,), halo, idx, tile, d * K + k)
                dr = near_r - own
                we, wn, wl = weights(k, d)
                lr += wl * dr
                dxr += we * dr
                dyr += wn * dr
            u, v = velocity_of(s, d)
            cor = wide(cors[d : d + 1])
            drag = jnp.where(level_id == wide(bots[d : d + 1]) - 1, DRAG, 0.0)
            part[0, d] = u + DT * (cor * v - column(dxr) - drag * u)
            part[1, d] = v - DT * (cor * u + column(dyr) + drag * v)
            new = own + DT * (lr - u * dxr - v * dyr)
            if d >= TILES:
                rsend[s + 1, d - TILES] = new
                gsend[s + 1, d - TILES, 0:1] = jnp.sum(new * th, axis=0, keepdims=True)
            else:
                r[1 - par, d] = new
                lsend[s + 1, 0, d : d + 1] = jnp.sum(new * th, axis=0, keepdims=True)

    def velocity_terms(s, dests):
        halo = [[urecv[s, side, c] for c in range(2)] for side in range(2)]
        for d in dests:
            u, v = velocity_of(s, d)
            zero = jnp.zeros((8, LANES), jnp.float32)
            dxu, dyv, lu, lv = [zero] * 4
            for k in range(K):
                idx, tile = slots(k, d)
                near_u, near_v = with_halo((0, 1), halo, idx, tile, d * K + k)
                we, wn, wl = weights(k, d)
                du, dv = near_u - u, near_v - v
                dxu += we * du
                dyv += wn * dv
                lu += wl * du
                lv += wl * dv
            part[0, d] = part[0, d] + DT * lu
            part[1, d] = part[1, d] + DT * lv
            div = jnp.sum(th * (dxu + dyv), axis=0, keepdims=True)
            if d >= TILES:
                gsend[s + 1, d - TILES, 1:2] = div
            else:
                lsend[s + 1, 1, d : d + 1] = div

    def find_q(s):
        arrived(lrecv.at[s], lsem, s)
        arrived(grecv.at[s], gsem, s)
        div, mass = lsend[s, 1], jnp.zeros((8, LANES), jnp.float32)
        for d in range(1, n_level):
            mass = mass + jnp.where(g >= d, lrecv[s, d - 1, 0], 0.0)
            div = div + lrecv[s, d - 1, 1]
        new_eta = eta[...] - DT * wet_nodes * div
        eta[...] = new_eta
        q[0:8] = new_eta + BUOYANCY * mass
        for side in range(2):
            row = slice(side, side + 1)
            m = jnp.zeros((1, LANES), jnp.float32)
            h = grecv[s, side, 0, 1:2]
            for d in range(1, n_level):
                m = m + jnp.where(g >= d, grecv[s, side, d, 0:1], 0.0)
                h = h + grecv[s, side, d, 1:2]
            e = etah[row] - DT * srecv[side, 1:2] * h
            etah[row] = e
            q[8 + side : 9 + side] = e + BUOYANCY * m

    def shared_terms(dests):
        listed = dests[0] >= TILES
        rows = slice(8, 16) if listed else slice(0, 8)
        own = q[0:8]
        if listed:
            first, second = [wide(listed_nodes(own, side)) for side in range(2)]
            own = jnp.where(sub == 0, first, second)
        dx = jnp.zeros((8, LANES), jnp.float32)
        dy = dx
        source = [wide(q[t : t + 1]) for t in range(TILES + 2)]
        for k in range(K):
            slot = nbc[k, rows]
            idx, tile = slot & (LANES - 1), slot >> 7
            n = lane_gather(source[0], idx)
            for t in range(1, TILES + 2):
                n = jnp.where(tile == t, lane_gather(source[t], idx), n)
            diff = n - own
            dx = dx + wts[0, k, rows] * diff
            dy = dy + wts[1, k, rows] * diff
        dq[0, rows] = DT * dx
        dq[1, rows] = DT * dy

    def new_velocity(d, c):
        wet = level_id < wide(bots[d : d + 1])
        return jnp.where(wet, part[c, d] - wide(dq[c, d : d + 1]), 0.0)

    def drift_weights():
        area = area_ref[...] * wet_nodes
        own = [jnp.zeros((8, LANES), jnp.float32)] * 2
        for k in range(K):
            for j in range(2):
                term = area * wts[j, k, 0:8]
                own[j] = own[j] + term
                for i in range(3):
                    short = term.astype(jnp.bfloat16).astype(jnp.float32)
                    split[i, j, k] = short
                    term = term - short
        target = jnp.where(sub < 2, sub + TILES, jnp.where(sub < 4, sub + TILES - 2, -1))
        slot_lane = lax.broadcasted_iota(jnp.int32, (LANES, LANES), 0)
        total = jnp.zeros((72, LANES), jnp.float32)
        for k in range(K):
            for d in range(0, TILES, 2):
                left_side, right_side = [], []
                for e in (d, d + 1):
                    row = nbc[k, e : e + 1]
                    tile = wide(row >> 7)
                    hit, far = tile == sub, tile == target
                    pieces = []
                    for i in range(3):
                        we, wn = [wide(split[i, j, k, e : e + 1]) for j in range(2)]
                        pieces.append(jnp.where(hit, we, 0.0))
                        pieces.append(jnp.where(hit, wn, 0.0))
                        pieces.append(jnp.where(far, jnp.where(sub < 2, we, wn), 0.0))
                    left_side.append(jnp.concatenate(pieces, axis=0))
                    same = jnp.broadcast_to(row & (LANES - 1), (LANES, LANES)) == slot_lane
                    right_side.append(jnp.where(same, 1.0, 0.0))
                total = total + lax.dot_general(
                    jnp.concatenate(left_side, axis=1).astype(jnp.bfloat16),
                    jnp.concatenate(right_side, axis=1).astype(jnp.bfloat16),
                    (((1,), (1,)), ((), ())),
                    preferred_element_type=jnp.float32,
                )
        total = total[0:24] + total[24:48] + total[48:72]
        for j in range(2):
            coef[j] = total[8 * j : 8 * j + 8] - own[j]
            for side in range(2):
                bsend[side, j : j + 1] = total[16 + 2 * j + side : 17 + 2 * j + side]
        copy(bsend.at[0], brecv.at[1], bsem, 0, down, g).start()
        copy(bsend.at[1], brecv.at[0], bsem, 0, up, g).start()

    def early_drift():
        arrived(brecv, bsem, 0)
        total = jnp.zeros((8, LANES), jnp.float32)
        for j in range(2):
            for d in range(TILES):
                total = total + wide(coef[j, d : d + 1]) * x[j, d]
            for side in range(2):
                total = total + wide(brecv[side, j : j + 1]) * usend[STEPS - 1, side, j]
        return total * th

    def send_drift():
        sums = jnp.zeros((8, LANES), jnp.float32)
        terms = [vv[s] for s in range(STEPS - 1)]
        terms += [early_drift(), area_ref[...] * wet_nodes * (1.0 / n_level)]
        for j, term in enumerate(terms):
            sums = jnp.where(sub == j, wide(jnp.sum(term, axis=0, keepdims=True)), sums)
        sums = jnp.broadcast_to(jnp.sum(sums, axis=1, keepdims=True), (8, LANES))
        zsend[...] = jnp.sum(jnp.where(sub == lane, sums, 0.0), axis=0, keepdims=True)
        pl.semaphore_wait(tok.at[4], 2)
        for d in far_first(n_z):
            copy(zsend, zrecv.at[d - 1], zsem, 0, z_peer(d), g).start()

    def step(s, _):
        par = s % 2 if isinstance(s, int) else lax.rem(s, 2)
        final = s == STEPS - 2 if isinstance(s, int) else False

        if final:
            pass_token(4)
        gather_own(par, (*lists, *range(TILES)))

        @when(s == 0)
        def _():
            pass_token(1)
            drift_weights()

        @when(s == 1)
        def _():
            pass_token(3)

        arrived(rrecv.at[s], rsem, s)
        density_terms(s, par, lists)
        send_density(s + 1)
        density_terms(s, par, range(TILES))

        @when(s == 0)
        def _():
            arrived(srecv, ssem, 0)
            etah[...] = srecv[:, 0]

        arrived(urecv.at[s], usem, s)
        velocity_terms(s, lists)
        if not final:
            send_sums(s + 1)
        if final:
            velocity_terms(s, range(TILES))
        find_q(s)
        shared_terms(lists)
        for side in range(2):
            for c in range(2):
                usend[s + 1, side, c] = new_velocity(TILES + side, c)
        if not final:
            send_velocity(s + 1)
        if not final:
            velocity_terms(s, range(TILES))
            send_level(s + 1)
        vv[s] = area_ref[...] * wet_nodes * lsend[s + 1, 1]
        shared_terms(range(TILES))
        for d in range(TILES):
            for c in range(2):
                x[c, d] = new_velocity(d, c)
        @when(s == 0)
        def _():
            pass_token(2)

        if final:
            send_drift()
            send_velocity(s + 1)
            send_sums(s + 1)
            send_level(s + 1)
        return 0

    lax.fori_loop(0, STEPS - 2, step, 0)
    step(STEPS - 2, 0)
    last = STEPS - 1
    par = last % 2
    gather_own(par, range(TILES))
    arrived(rrecv.at[last], rsem, last)
    density_terms(last, par, range(TILES))
    for d in range(TILES):
        rho_out[:, d * LANES : (d + 1) * LANES] = r[1 - par, d]
    arrived(urecv.at[last], usem, last)
    velocity_terms(last, range(TILES))
    send_level(STEPS)
    find_q(last)
    shared_terms(range(TILES))
    for d in range(TILES):
        for c in range(2):
            vel_out[c, :, d * LANES : (d + 1) * LANES] = new_velocity(d, c)

    arrived(zrecv, zsem, 0)
    row = zsend[...]
    for d in range(1, n_z):
        row = row + zrecv[d - 1]
    xsend[...] = row
    for i, (a, b) in enumerate(plane):
        copy(xsend, xrecv.at[i], zsem, 1, x_peers[a], level_peers[b]).start()

    arrived(lrecv.at[STEPS], lsem, STEPS)
    div = lsend[STEPS, 1]
    for d in range(1, n_level):
        div = div + lrecv[STEPS, d - 1, 1]
    eta[...] = eta[...] - DT * wet_nodes * div

    for s in range(STEPS + 1):
        left(lrecv.at[s], lsem, s)
    for s in range(STEPS):
        left(usend.at[s], usem, s)
        left(rsend.at[s], rsem, s)
        left(grecv.at[s], gsem, s)
    left(ssend, ssem, 0)
    left(bsend, bsem, 0)
    left(zrecv, zsem, 0)

    arrived(xrecv, zsem, 1)
    for i in range(len(plane)):
        row = row + xrecv[i]
    lane_row = lane[0:1]
    total = jnp.sum(jnp.where(lane_row == STEPS, row, 0.0), axis=1, keepdims=True)
    drift_sum = jnp.sum(jnp.where(lane_row < STEPS, row, 0.0), axis=1, keepdims=True)
    drift_out[...] = jnp.where(lane_row < STEPS, row / total, 0.0)
    eta_out[...] = eta[...] + DT * (drift_sum / total)
    left(xrecv, zsem, 1)


def finish(vel, rho, eta, drift, vel_out, rho_out, eta_out, drift_out, sem):
    copies = [
        pltpu.make_async_copy(a, b, sem.at[i])
        for i, (a, b) in enumerate(((vel, vel_out), (rho, rho_out), (eta, eta_out)))
    ]
    for c in copies:
        c.start()
    drift_out[...] = drift[0, :STEPS]
    for c in copies:
        c.wait()


def solution(mesh):
    n_space, n_level = mesh.shape["space"], mesh.shape["level"]

    def local(
        velocity,
        density,
        elevation,
        grad_weights,
        lap_weights,
        coriolis,
        node_area,
        thickness,
        send_list,
        neighbours,
        bottom,
    ):
        f32, i32 = jnp.float32, jnp.int32
        compact = (TILES, LANES)
        vmem = pl.BlockSpec(memory_space=pltpu.VMEM)
        dma = pltpu.SemaphoreType.DMA
        peers = n_level - 1
        n_z = n_space // X_CHIPS
        row = (1, LANES)
        inputs = [
            pltpu.VMEM(velocity.shape, f32),
            pltpu.VMEM(density.shape, f32),
            pltpu.VMEM(compact, f32),
            pltpu.VMEM((K, 2, TILES * LANES), f32),
            pltpu.VMEM(lap_weights.shape, f32),
            pltpu.VMEM(compact, f32),
            pltpu.VMEM(compact, f32),
            pltpu.SMEM(thickness.shape, f32),
            pltpu.VMEM(send_list.shape, i32),
            pltpu.VMEM(neighbours.shape, i32),
            pltpu.VMEM(compact, i32),
            dma((11,)),
            pltpu.VMEM((K, 16, LANES), i32),
        ]
        shapes = [
            (2, 8, 8, LANES),
            (2, 8, 8, LANES),
            (2, 10, 8, LANES),
            (3, 60, 8, LANES),
            (16, LANES),
            (2, 16, LANES),
            (8, LANES),
            (2, LANES),
            (STEPS, 8, LANES),
            (STEPS + 1, 2, 8, LANES),
            (STEPS + 1, peers, 2, 8, LANES),
            (STEPS, 2, 2, 8, LANES),
            (STEPS, 2, 2, 8, LANES),
            (STEPS, 2, 8, LANES),
            (STEPS, 2, 8, LANES),
            (STEPS, 2, 2, LANES),
            (STEPS, 2, n_level, 2, LANES),
            (2, 2, LANES),
            (2, 2, LANES),
            row,
            (n_z - 1, *row),
            row,
            (X_CHIPS * n_level - 1, *row),
            (3, 2, K, 8, LANES),
            (2, 8, LANES),
            (2, 2, LANES),
            (2, 2, LANES),
        ]

        def body(*refs):
            kernel(n_space, n_level, *refs)

        vel, rho, eta, drift = pl.pallas_call(
            body,
            out_shape=(
                pltpu.VMEM(velocity.shape, f32),
                pltpu.VMEM(density.shape, f32),
                pltpu.VMEM(compact, f32),
                pltpu.VMEM((1, LANES), f32),
            ),
            in_specs=[pl.BlockSpec(memory_space=pl.ANY)] * 11,
            out_specs=(vmem,) * 4,
            scratch_shapes=inputs
            + [pltpu.VMEM((3, K, 16, LANES), f32)]
            + [pltpu.VMEM((16, LANES), i32), pltpu.VMEM((16, LANES), f32)]
            + [pltpu.VMEM(shape, f32) for shape in shapes]
            + [
                dma((2, 5)),
                dma((2, 4)),
                dma((2, 4)),
                dma((2, 4)),
                dma((2, 1)),
                dma((2, 1)),
                dma((2, 2)),
                pltpu.SemaphoreType.REGULAR((5,)),
            ],
            compiler_params=pltpu.CompilerParams(collective_id=0, has_side_effects=True),
        )(
            velocity,
            density,
            elevation.reshape(compact),
            jnp.swapaxes(grad_weights, 0, 1),
            lap_weights,
            coriolis.reshape(compact),
            node_area.reshape(compact),
            thickness,
            send_list,
            neighbours,
            bottom.reshape(compact),
        )
        results = [pltpu.with_memory_space_constraint(a, pltpu.VMEM) for a in (vel, rho, eta, drift)]
        vel, rho, eta, drift = pl.pallas_call(
            finish,
            out_shape=(
                jax.ShapeDtypeStruct(velocity.shape, f32),
                jax.ShapeDtypeStruct(density.shape, f32),
                jax.ShapeDtypeStruct(compact, f32),
                jax.ShapeDtypeStruct((STEPS,), f32),
            ),
            in_specs=[vmem] * 4,
            out_specs=(pl.BlockSpec(memory_space=pl.ANY),) * 3 + (vmem,),
            scratch_shapes=[dma((3,))],
        )(*results)
        return vel, rho, eta.reshape(elevation.shape), drift

    return jax.shard_map(
        local,
        mesh=mesh,
        in_specs=(
            P(None, "level", "space"),
            P("level", "space"),
            P("space"),
            P(None, None, "space"),
            P(None, "space"),
            P("space"),
            P("space"),
            P("level"),
            P("space", None),
            P(None, "space"),
            P("space"),
        ),
        out_specs=(P(None, "level", "space"), P("level", "space"), P("space"), P()),
        check_vma=False,
    )
```

```python
import jax
import jax.numpy as jnp
from jax import lax
from jax.experimental import pallas as pl
from jax.experimental.pallas import tpu as pltpu
from jax.sharding import PartitionSpec as P

MESH = pl.DeviceIdType.MESH
STEPS = 4
K = 6
TILES = 8
LANES = 128
X_CHIPS = 4
DT = 0.1
BUOYANCY = 0.5
DRAG = 0.5

_LANE_GATHER = lax.GatherDimensionNumbers(
    offset_dims=(),
    collapsed_slice_dims=(1,),
    start_index_map=(1,),
    operand_batching_dims=(0,),
    start_indices_batching_dims=(0,),
)


def lane_gather(x, idx):
    return lax.gather(
        x, idx[..., None], _LANE_GATHER, (1, 1), mode=lax.GatherScatterMode.PROMISE_IN_BOUNDS
    )


def far_first(count, start=1):
    return sorted(range(start, count), key=lambda d: -min(d, count - d))


def when(condition):
    if isinstance(condition, bool):
        return lambda act: act() if condition else None
    return pl.when(condition)


def tree_sum(terms):
    while len(terms) > 1:
        terms = [sum(terms[i + 1 : i + 2], terms[i]) for i in range(0, len(terms), 2)]
    return terms[0]


def wide(row):
    return jnp.broadcast_to(row, (8, LANES))


def kernel(
    n_space,
    n_level,
    vel_hbm,
    rho_hbm,
    eta_hbm,
    grad_hbm,
    lap_hbm,
    cor_hbm,
    area_hbm,
    thick_hbm,
    send_hbm,
    nb_hbm,
    bot_hbm,
    vel_out,
    rho_out,
    eta_out,
    drift_out,
    vel_ref,
    rho_ref,
    eta_ref,
    grad_ref,
    lap_ref,
    cor_ref,
    area_ref,
    thick_ref,
    send_ref,
    nb_ref,
    bot_ref,
    isem,
    nbc,
    wts,
    bots,
    cors,
    x,
    r,
    part,
    near,
    q,
    dq,
    eta,
    etah,
    vv,
    lsend,
    lrecv,
    usend,
    urecv,
    rsend,
    rrecv,
    gsend,
    grecv,
    ssend,
    srecv,
    zsend,
    zrecv,
    xsend,
    xrecv,
    split,
    coef,
    bsend,
    brecv,
    lsem,
    usem,
    rsem,
    gsem,
    ssem,
    bsem,
    zsem,
    tok,
):
    p = lax.axis_index("space")
    g = lax.axis_index("level")
    n_z = n_space // X_CHIPS
    up = lax.rem(p + 1, n_space)
    down = lax.rem(p + n_space - 1, n_space)
    level_peers = [lax.rem(g + d, n_level) for d in range(n_level)]

    def z_peer(d):
        return lax.rem(p + d * X_CHIPS, n_space)

    px = lax.rem(p, X_CHIPS)
    x_peers = [p - px + lax.rem(px + d, X_CHIPS) for d in range(X_CHIPS)]
    plane = [(a, b) for a in range(X_CHIPS) for b in range(n_level) if a or b]
    plane.sort(key=lambda ab: -2 * min(ab[0], X_CHIPS - ab[0]) - min(ab[1], n_level - ab[1]))

    barrier = pltpu.get_barrier_semaphore()
    count = 0

    def greet(a, b):
        pl.semaphore_signal(barrier, inc=1, device_id=(a, b), device_id_type=MESH)

    for d in far_first(n_level, 0):
        greet(up, level_peers[d])
        greet(down, level_peers[d])
        count += 2
        if d:
            greet(p, level_peers[d])
            count += 1

    inputs = [
        (send_hbm, send_ref),
        (vel_hbm, vel_ref),
        (bot_hbm, bot_ref),
        (rho_hbm, rho_ref),
        (thick_hbm, thick_ref),
        (eta_hbm, eta_ref),
        (nb_hbm, nb_ref),
        (grad_hbm, grad_ref),
        (lap_hbm, lap_ref),
        (cor_hbm, cor_ref),
        (area_hbm, area_ref),
    ]
    loads = [pltpu.make_async_copy(a, b, isem.at[i]) for i, (a, b) in enumerate(inputs)]
    for load in loads:
        load.start()

    sub = lax.broadcasted_iota(jnp.int32, (8, LANES), 0)
    lane = lax.broadcasted_iota(jnp.int32, (8, LANES), 1)
    level_id = sub + g * 8
    for load in loads[:5]:
        load.wait()
    th = jnp.zeros((8, LANES), jnp.float32)
    for l in range(8):
        th = jnp.where(sub == l, thick_ref[l], th)
    send_idx = [send_ref[:, side * LANES : (side + 1) * LANES] for side in range(2)]
    send_lane = [wide(i & (LANES - 1)) for i in send_idx]
    send_tile = [wide(i >> 7) for i in send_idx]

    def listed_levels(tiles, side):
        out = lane_gather(tiles[0], send_lane[side])
        for t in range(1, TILES):
            out = jnp.where(send_tile[side] == t, lane_gather(tiles[t], send_lane[side]), out)
        return out

    def listed_nodes(compact, side):
        got = lane_gather(compact, send_lane[side])
        here = jnp.where(send_tile[side] == sub, got, jnp.zeros_like(got))
        return jnp.sum(here, axis=0, keepdims=True)

    def column(density):
        weighted = density * th
        total = weighted
        for shift in (1, 2, 4):
            total = total + jnp.where(sub >= shift, pltpu.roll(total, shift, 0), 0.0)
        return BUOYANCY * (total - 0.5 * weighted)

    def copy(src, dst, sems, i, a, b):
        return pltpu.make_async_remote_copy(
            src_ref=src,
            dst_ref=dst,
            send_sem=sems.at[0, i],
            recv_sem=sems.at[1, i],
            device_id=(a, b),
            device_id_type=MESH,
        )

    def arrived(buf, sems, i):
        pltpu.make_async_copy(buf, buf, sems.at[1, i]).wait()

    def left(buf, sems, i):
        pltpu.make_async_copy(buf, buf, sems.at[0, i]).wait()

    def send_token(i):
        for d in (2**i, n_space - 2**i):
            there = (lax.rem(p + d, n_space), g)
            pl.semaphore_signal(tok.at[i], inc=1, device_id=there, device_id_type=MESH)

    def pass_token(i):
        pl.semaphore_wait(tok.at[i - 1], 2)
        send_token(i)

    def list_velocity(s):
        for side in range(2):
            for c in range(2):
                usend[s, side, c] = listed_levels([x[c, d] for d in range(TILES)], side)

    def send_velocity(s):
        copy(usend.at[s, 0], urecv.at[s, 1], usem, s, down, g).start()
        copy(usend.at[s, 1], urecv.at[s, 0], usem, s, up, g).start()

    def list_density(s, par):
        tiles = [r[par, d] for d in range(TILES)]
        for side in range(2):
            got = listed_levels(tiles, side)
            rsend[s, side] = got
            gsend[s, side, 0:1] = jnp.sum(got * th, axis=0, keepdims=True)
        for d in range(TILES):
            lsend[s, 0, d : d + 1] = jnp.sum(tiles[d] * th, axis=0, keepdims=True)

    def send_density(s):
        copy(rsend.at[s, 0], rrecv.at[s, 1], rsem, s, down, g).start()
        copy(rsend.at[s, 1], rrecv.at[s, 0], rsem, s, up, g).start()

    def send_sums(s):
        for d in far_first(n_level, 0):
            copy(gsend.at[s, 0], grecv.at[s, 1, d], gsem, s, down, level_peers[d]).start()
            copy(gsend.at[s, 1], grecv.at[s, 0, d], gsem, s, up, level_peers[d]).start()

    def send_level(s):
        for d in far_first(n_level):
            copy(lsend.at[s], lrecv.at[s, d - 1], lsem, s, p, level_peers[d]).start()

    for d in range(TILES):
        cols = slice(d * LANES, (d + 1) * LANES)
        wet = level_id < wide(bot_ref[d : d + 1])
        for c in range(2):
            x[c, d] = jnp.where(wet, vel_ref[c, :, cols], 0.0)
        r[0, d] = rho_ref[:, cols]
    list_velocity(0)
    list_density(0, 0)
    lsend[0, 1] = jnp.zeros((8, LANES), jnp.float32)
    for side in range(2):
        gsend[0, side, 1:2] = jnp.zeros((1, LANES), jnp.float32)
    loads[5].wait()
    wet_nodes = (bot_ref[...] > 0).astype(jnp.float32)
    eta[...] = eta_ref[...]
    for side in range(2):
        ssend[side, 0:1] = listed_nodes(eta_ref[...], side)
        ssend[side, 1:2] = listed_nodes(wet_nodes, side)

    pl.semaphore_wait(barrier, count)
    send_sums(0)
    send_density(0)
    send_velocity(0)
    send_level(0)
    copy(ssend.at[0], srecv.at[1], ssem, 0, down, g).start()
    copy(ssend.at[1], srecv.at[0], ssem, 0, up, g).start()
    send_token(0)

    for load in loads[6:]:
        load.wait()
    bots[0:8] = bot_ref[...]
    cors[0:8] = cor_ref[...]
    for k in range(K):
        for d in range(TILES):
            cols = slice(d * LANES, (d + 1) * LANES)
            row = slice(d, d + 1)
            nbc[k, row] = nb_ref[k : k + 1, cols]
            wts[0, k, row] = grad_ref[k, 0:1, cols]
            wts[1, k, row] = grad_ref[k, 1:2, cols]
            wts[2, k, row] = lap_ref[k : k + 1, cols]
        tile = nbc[k, 0:8] >> 7
        below = jnp.where(p > 0, 1.0, 0.0)
        above = jnp.where(p < n_space - 1, 1.0, 0.0)
        valid = jnp.where(tile == TILES, below, jnp.where(tile == TILES + 1, above, 1.0))
        nbc[k, 8:16] = jnp.zeros((8, LANES), jnp.int32)
        for j in range(3):
            wts[j, k, 0:8] = wts[j, k, 0:8] * valid
            wts[j, k, 8:16] = jnp.zeros((8, LANES), jnp.float32)
        for side in range(2):
            row = slice(8 + side, 9 + side)
            nbc[k, row] = listed_nodes(nbc[k, 0:8], side)
            for j in range(3):
                wts[j, k, row] = listed_nodes(wts[j, k, 0:8], side)
    for side in range(2):
        row = slice(8 + side, 9 + side)
        bots[row] = listed_nodes(bot_ref[...], side)
        cors[row] = listed_nodes(cor_ref[...], side)
    lists = (TILES, TILES + 1)

    def slots(k, d):
        row = wide(nbc[k, d : d + 1])
        return row & (LANES - 1), row >> 7

    def weights(k, d):
        return [wide(wts[j, k, d : d + 1]) for j in range(3)]

    def gather_own(par, dests):
        for d in dests:
            for k in range(K):
                idx, tile = slots(k, d)
                outs = [None] * 3
                for t in range(TILES):
                    hit = tile == t
                    for f, a in enumerate((x[0, t], x[1, t], r[par, t])):
                        got = lane_gather(a, idx)
                        outs[f] = jnp.where(hit, got, outs[f]) if t else got
                for f in range(3):
                    near[f, d * K + k] = outs[f]

    def with_halo(fields, halo, idx, tile, at):
        outs = [near[f, at] for f in fields]
        for side in range(2):
            hit = tile == TILES + side
            outs = [jnp.where(hit, lane_gather(a, idx), o) for a, o in zip(halo[side], outs)]
        return outs

    def velocity_of(s, d):
        if d >= TILES:
            return usend[s, d - TILES, 0], usend[s, d - TILES, 1]
        return x[0, d], x[1, d]

    def density_terms(s, par, dests):
        halo = [(rrecv[s, side],) for side in range(2)]
        for d in dests:
            own = rsend[s, d - TILES] if d >= TILES else r[par, d]
            zero = jnp.zeros((8, LANES), jnp.float32)
            lr, dxr, dyr = [zero] * 3
            for k in range(K):
                idx, tile = slots(k, d)
                (near_r,) = with_halo((2,), halo, idx, tile, d * K + k)
                dr = near_r - own
                we, wn, wl = weights(k, d)
                lr += wl * dr
                dxr += we * dr
                dyr += wn * dr
            u, v = velocity_of(s, d)
            cor = wide(cors[d : d + 1])
            drag = jnp.where(level_id == wide(bots[d : d + 1]) - 1, DRAG, 0.0)
            part[0, d] = u + DT * (cor * v - column(dxr) - drag * u)
            part[1, d] = v - DT * (cor * u + column(dyr) + drag * v)
            new = own + DT * (lr - u * dxr - v * dyr)
            if d >= TILES:
                rsend[s + 1, d - TILES] = new
                gsend[s + 1, d - TILES, 0:1] = jnp.sum(new * th, axis=0, keepdims=True)
            else:
                r[1 - par, d] = new
                lsend[s + 1, 0, d : d + 1] = jnp.sum(new * th, axis=0, keepdims=True)

    def velocity_terms(s, dests):
        halo = [[urecv[s, side, c] for c in range(2)] for side in range(2)]
        for d in dests:
            u, v = velocity_of(s, d)
            zero = jnp.zeros((8, LANES), jnp.float32)
            dxu, dyv, lu, lv = [zero] * 4
            for k in range(K):
                idx, tile = slots(k, d)
                near_u, near_v = with_halo((0, 1), halo, idx, tile, d * K + k)
                we, wn, wl = weights(k, d)
                du, dv = near_u - u, near_v - v
                dxu += we * du
                dyv += wn * dv
                lu += wl * du
                lv += wl * dv
            part[0, d] = part[0, d] + DT * lu
            part[1, d] = part[1, d] + DT * lv
            div = jnp.sum(th * (dxu + dyv), axis=0, keepdims=True)
            if d >= TILES:
                gsend[s + 1, d - TILES, 1:2] = div
            else:
                lsend[s + 1, 1, d : d + 1] = div

    def find_q(s):
        arrived(lrecv.at[s], lsem, s)
        arrived(grecv.at[s], gsem, s)
        div, mass = lsend[s, 1], jnp.zeros((8, LANES), jnp.float32)
        for d in range(1, n_level):
            mass = mass + jnp.where(g >= d, lrecv[s, d - 1, 0], 0.0)
            div = div + lrecv[s, d - 1, 1]
        new_eta = eta[...] - DT * wet_nodes * div
        eta[...] = new_eta
        q[0:8] = new_eta + BUOYANCY * mass
        for side in range(2):
            row = slice(side, side + 1)
            m = jnp.zeros((1, LANES), jnp.float32)
            h = grecv[s, side, 0, 1:2]
            for d in range(1, n_level):
                m = m + jnp.where(g >= d, grecv[s, side, d, 0:1], 0.0)
                h = h + grecv[s, side, d, 1:2]
            e = etah[row] - DT * srecv[side, 1:2] * h
            etah[row] = e
            q[8 + side : 9 + side] = e + BUOYANCY * m

    def shared_terms(dests):
        listed = dests[0] >= TILES
        rows = slice(8, 16) if listed else slice(0, 8)
        own = q[0:8]
        if listed:
            first, second = [wide(listed_nodes(own, side)) for side in range(2)]
            own = jnp.where(sub == 0, first, second)
        dx = jnp.zeros((8, LANES), jnp.float32)
        dy = dx
        source = [wide(q[t : t + 1]) for t in range(TILES + 2)]
        for k in range(K):
            slot = nbc[k, rows]
            idx, tile = slot & (LANES - 1), slot >> 7
            n = lane_gather(source[0], idx)
            for t in range(1, TILES + 2):
                n = jnp.where(tile == t, lane_gather(source[t], idx), n)
            diff = n - own
            dx = dx + wts[0, k, rows] * diff
            dy = dy + wts[1, k, rows] * diff
        dq[0, rows] = DT * dx
        dq[1, rows] = DT * dy

    def new_velocity(d, c):
        wet = level_id < wide(bots[d : d + 1])
        return jnp.where(wet, part[c, d] - wide(dq[c, d : d + 1]), 0.0)

    def drift_weights():
        area = area_ref[...] * wet_nodes
        own = [jnp.zeros((8, LANES), jnp.float32)] * 2
        for k in range(K):
            for j in range(2):
                term = area * wts[j, k, 0:8]
                own[j] = own[j] + term
                for i in range(3):
                    short = term.astype(jnp.bfloat16).astype(jnp.float32)
                    split[i, j, k] = short
                    term = term - short
        target = jnp.where(sub < 2, sub + TILES, jnp.where(sub < 4, sub + TILES - 2, -1))
        slot_lane = lax.broadcasted_iota(jnp.int32, (LANES, LANES), 0)
        total = jnp.zeros((72, LANES), jnp.float32)
        for k in range(K):
            for d in range(0, TILES, 2):
                left_side, right_side = [], []
                for e in (d, d + 1):
                    row = nbc[k, e : e + 1]
                    tile = wide(row >> 7)
                    hit, far = tile == sub, tile == target
                    pieces = []
                    for i in range(3):
                        we, wn = [wide(split[i, j, k, e : e + 1]) for j in range(2)]
                        pieces.append(jnp.where(hit, we, 0.0))
                        pieces.append(jnp.where(hit, wn, 0.0))
                        pieces.append(jnp.where(far, jnp.where(sub < 2, we, wn), 0.0))
                    left_side.append(jnp.concatenate(pieces, axis=0))
                    same = jnp.broadcast_to(row & (LANES - 1), (LANES, LANES)) == slot_lane
                    right_side.append(jnp.where(same, 1.0, 0.0))
                total = total + lax.dot_general(
                    jnp.concatenate(left_side, axis=1).astype(jnp.bfloat16),
                    jnp.concatenate(right_side, axis=1).astype(jnp.bfloat16),
                    (((1,), (1,)), ((), ())),
                    preferred_element_type=jnp.float32,
                )
        total = total[0:24] + total[24:48] + total[48:72]
        for j in range(2):
            coef[j] = total[8 * j : 8 * j + 8] - own[j]
            for side in range(2):
                bsend[side, j : j + 1] = total[16 + 2 * j + side : 17 + 2 * j + side]
        copy(bsend.at[0], brecv.at[1], bsem, 0, down, g).start()
        copy(bsend.at[1], brecv.at[0], bsem, 0, up, g).start()

    def early_drift():
        arrived(brecv, bsem, 0)
        terms = []
        for j in range(2):
            for d in range(TILES):
                terms.append(wide(coef[j, d : d + 1]) * x[j, d])
            for side in range(2):
                terms.append(wide(brecv[side, j : j + 1]) * usend[STEPS - 1, side, j])
        return tree_sum(terms) * th

    def earlier_drifts():
        sums = jnp.zeros((8, LANES), jnp.float32)
        terms = [(s, vv[s]) for s in range(STEPS - 1)]
        terms += [(STEPS, area_ref[...] * wet_nodes * (1.0 / n_level))]
        for j, term in terms:
            sums = jnp.where(sub == j, wide(jnp.sum(term, axis=0, keepdims=True)), sums)
        return sums

    def send_drift(sums):
        row = jnp.sum(early_drift(), axis=0, keepdims=True)
        sums = jnp.where(sub == STEPS - 1, wide(row), sums)
        sums = jnp.broadcast_to(jnp.sum(sums, axis=1, keepdims=True), (8, LANES))
        zsend[...] = jnp.sum(jnp.where(sub == lane, sums, 0.0), axis=0, keepdims=True)
        pl.semaphore_wait(tok.at[4], 2)
        for d in far_first(n_z):
            copy(zsend, zrecv.at[d - 1], zsem, 0, z_peer(d), g).start()

    def step(s, _):
        par = s % 2 if isinstance(s, int) else lax.rem(s, 2)
        final = s == STEPS - 2 if isinstance(s, int) else False

        if final:
            pass_token(4)
        gather_own(par, (*lists, *range(TILES)))

        @when(s == 0)
        def _():
            pass_token(1)
            drift_weights()

        @when(s == 1)
        def _():
            pass_token(3)

        arrived(rrecv.at[s], rsem, s)
        density_terms(s, par, lists)
        send_density(s + 1)
        density_terms(s, par, range(TILES))

        @when(s == 0)
        def _():
            arrived(srecv, ssem, 0)
            etah[...] = srecv[:, 0]

        arrived(urecv.at[s], usem, s)
        velocity_terms(s, lists)
        if not final:
            send_sums(s + 1)
        if final:
            velocity_terms(s, range(TILES))
            vv[s] = area_ref[...] * wet_nodes * lsend[s + 1, 1]
            sums = earlier_drifts()
        find_q(s)
        shared_terms(lists)
        for side in range(2):
            for c in range(2):
                usend[s + 1, side, c] = new_velocity(TILES + side, c)
        if not final:
            send_velocity(s + 1)
        if not final:
            velocity_terms(s, range(TILES))
            send_level(s + 1)
            vv[s] = area_ref[...] * wet_nodes * lsend[s + 1, 1]
        shared_terms(range(TILES))
        for d in range(TILES):
            for c in range(2):
                x[c, d] = new_velocity(d, c)
        @when(s == 0)
        def _():
            pass_token(2)

        if final:
            send_drift(sums)
            send_velocity(s + 1)
            send_sums(s + 1)
            send_level(s + 1)
        return 0

    lax.fori_loop(0, STEPS - 2, step, 0)
    step(STEPS - 2, 0)
    last = STEPS - 1
    par = last % 2
    gather_own(par, range(TILES))
    arrived(rrecv.at[last], rsem, last)
    density_terms(last, par, range(TILES))
    for d in range(TILES):
        rho_out[:, d * LANES : (d + 1) * LANES] = r[1 - par, d]
    arrived(urecv.at[last], usem, last)
    velocity_terms(last, range(TILES))
    send_level(STEPS)
    find_q(last)
    shared_terms(range(TILES))
    for d in range(TILES):
        for c in range(2):
            vel_out[c, :, d * LANES : (d + 1) * LANES] = new_velocity(d, c)

    arrived(zrecv, zsem, 0)
    row = tree_sum([zsend[...]] + [zrecv[d] for d in range(n_z - 1)])
    xsend[...] = row
    for i, (a, b) in enumerate(plane):
        copy(xsend, xrecv.at[i], zsem, 1, x_peers[a], level_peers[b]).start()

    arrived(lrecv.at[STEPS], lsem, STEPS)
    div = lsend[STEPS, 1]
    for d in range(1, n_level):
        div = div + lrecv[STEPS, d - 1, 1]
    eta[...] = eta[...] - DT * wet_nodes * div

    for s in range(STEPS + 1):
        left(lrecv.at[s], lsem, s)
    for s in range(STEPS):
        left(usend.at[s], usem, s)
        left(rsend.at[s], rsem, s)
        left(grecv.at[s], gsem, s)
    left(ssend, ssem, 0)
    left(bsend, bsem, 0)
    left(zrecv, zsem, 0)

    arrived(xrecv, zsem, 1)
    row = tree_sum([row] + [xrecv[i] for i in range(len(plane))])
    lane_row = lane[0:1]
    total = jnp.sum(jnp.where(lane_row == STEPS, row, 0.0), axis=1, keepdims=True)
    drift_sum = jnp.sum(jnp.where(lane_row < STEPS, row, 0.0), axis=1, keepdims=True)
    drift_out[...] = jnp.where(lane_row < STEPS, row / total, 0.0)
    eta_out[...] = eta[...] + DT * (drift_sum / total)
    left(xrecv, zsem, 1)


def finish(vel, rho, eta, drift, vel_out, rho_out, eta_out, drift_out, sem):
    copies = [
        pltpu.make_async_copy(a, b, sem.at[i])
        for i, (a, b) in enumerate(((vel, vel_out), (rho, rho_out), (eta, eta_out)))
    ]
    for c in copies:
        c.start()
    drift_out[...] = drift[0, :STEPS]
    for c in copies:
        c.wait()


def solution(mesh):
    n_space, n_level = mesh.shape["space"], mesh.shape["level"]

    def local(
        velocity,
        density,
        elevation,
        grad_weights,
        lap_weights,
        coriolis,
        node_area,
        thickness,
        send_list,
        neighbours,
        bottom,
    ):
        f32, i32 = jnp.float32, jnp.int32
        compact = (TILES, LANES)
        vmem = pl.BlockSpec(memory_space=pltpu.VMEM)
        dma = pltpu.SemaphoreType.DMA
        peers = n_level - 1
        n_z = n_space // X_CHIPS
        row = (1, LANES)
        inputs = [
            pltpu.VMEM(velocity.shape, f32),
            pltpu.VMEM(density.shape, f32),
            pltpu.VMEM(compact, f32),
            pltpu.VMEM((K, 2, TILES * LANES), f32),
            pltpu.VMEM(lap_weights.shape, f32),
            pltpu.VMEM(compact, f32),
            pltpu.VMEM(compact, f32),
            pltpu.SMEM(thickness.shape, f32),
            pltpu.VMEM(send_list.shape, i32),
            pltpu.VMEM(neighbours.shape, i32),
            pltpu.VMEM(compact, i32),
            dma((11,)),
            pltpu.VMEM((K, 16, LANES), i32),
        ]
        shapes = [
            (2, 8, 8, LANES),
            (2, 8, 8, LANES),
            (2, 10, 8, LANES),
            (3, 60, 8, LANES),
            (16, LANES),
            (2, 16, LANES),
            (8, LANES),
            (2, LANES),
            (STEPS, 8, LANES),
            (STEPS + 1, 2, 8, LANES),
            (STEPS + 1, peers, 2, 8, LANES),
            (STEPS, 2, 2, 8, LANES),
            (STEPS, 2, 2, 8, LANES),
            (STEPS, 2, 8, LANES),
            (STEPS, 2, 8, LANES),
            (STEPS, 2, 2, LANES),
            (STEPS, 2, n_level, 2, LANES),
            (2, 2, LANES),
            (2, 2, LANES),
            row,
            (n_z - 1, *row),
            row,
            (X_CHIPS * n_level - 1, *row),
            (3, 2, K, 8, LANES),
            (2, 8, LANES),
            (2, 2, LANES),
            (2, 2, LANES),
        ]

        def body(*refs):
            kernel(n_space, n_level, *refs)

        vel, rho, eta, drift = pl.pallas_call(
            body,
            out_shape=(
                pltpu.VMEM(velocity.shape, f32),
                pltpu.VMEM(density.shape, f32),
                pltpu.VMEM(compact, f32),
                pltpu.VMEM((1, LANES), f32),
            ),
            in_specs=[pl.BlockSpec(memory_space=pl.ANY)] * 11,
            out_specs=(vmem,) * 4,
            scratch_shapes=inputs
            + [pltpu.VMEM((3, K, 16, LANES), f32)]
            + [pltpu.VMEM((16, LANES), i32), pltpu.VMEM((16, LANES), f32)]
            + [pltpu.VMEM(shape, f32) for shape in shapes]
            + [
                dma((2, 5)),
                dma((2, 4)),
                dma((2, 4)),
                dma((2, 4)),
                dma((2, 1)),
                dma((2, 1)),
                dma((2, 2)),
                pltpu.SemaphoreType.REGULAR((5,)),
            ],
            compiler_params=pltpu.CompilerParams(collective_id=0, has_side_effects=True),
        )(
            velocity,
            density,
            elevation.reshape(compact),
            jnp.swapaxes(grad_weights, 0, 1),
            lap_weights,
            coriolis.reshape(compact),
            node_area.reshape(compact),
            thickness,
            send_list,
            neighbours,
            bottom.reshape(compact),
        )
        results = [pltpu.with_memory_space_constraint(a, pltpu.VMEM) for a in (vel, rho, eta, drift)]
        vel, rho, eta, drift = pl.pallas_call(
            finish,
            out_shape=(
                jax.ShapeDtypeStruct(velocity.shape, f32),
                jax.ShapeDtypeStruct(density.shape, f32),
                jax.ShapeDtypeStruct(compact, f32),
                jax.ShapeDtypeStruct((STEPS,), f32),
            ),
            in_specs=[vmem] * 4,
            out_specs=(pl.BlockSpec(memory_space=pl.ANY),) * 3 + (vmem,),
            scratch_shapes=[dma((3,))],
        )(*results)
        return vel, rho, eta.reshape(elevation.shape), drift

    return jax.shard_map(
        local,
        mesh=mesh,
        in_specs=(
            P(None, "level", "space"),
            P("level", "space"),
            P("space"),
            P(None, None, "space"),
            P(None, "space"),
            P("space"),
            P("space"),
            P("level"),
            P("space", None),
            P(None, "space"),
            P("space"),
        ),
        out_specs=(P(None, "level", "space"), P("level", "space"), P("space"), P()),
        check_vma=False,
    )
```
